128 devices in a mesh: role: 2 (over core), dev: 64 (over z, x, y).
Axes of the slice: x: 4, y: 4, z: 4, core: 2. Of those that a mesh axis runs over, the one named last changes fastest.
Arguments:
- positions: float32 [1024, 3, 512], P(('role', 'dev')), may hold values from -1 to 1
- normals: float32 [1024, 3, 512], P(('role', 'dev')), may hold values from -3.6 to 3.6
- panel_areas: float32 [1024, 512], P(('role', 'dev')), may hold values from 0.005 to 0.05
- panel_counts: int32 [1024], P(('role', 'dev')), may hold values from 128 to 512, as said below
- near_lists: int32 [1024, 6], P(('role', 'dev')), may hold values from 0 to 1023, as said below
- near_counts: int32 [1024], P(('role', 'dev')), may hold values from 1 to 6
- leaf_lists: int32 [1024, 16], P(('role', 'dev')), may hold values from 0 to 1023, as said below
- leaf_kinds: int32 [1024, 16], P(('role', 'dev')), may hold values from 0 to 7
- group_lists: int32 [128, 16], P(('role', 'dev')), may hold values from 0 to 127
- group_kinds: int32 [128, 16], P(('role', 'dev')), may hold values from 0 to 7
- block_inverse: bfloat16 [1024, 512, 512], P(('role', 'dev')), may hold values from -1 to 3
- moment_maps: bfloat16 [1024, 256, 512], P(('role', 'dev')), may hold values from -0.25 to 0.25
- up_operators: bfloat16 [8, 256, 256], replicated, may hold values from -0.125 to 0.125
- far_operators: bfloat16 [2, 8, 256, 256], replicated, may hold values from -0.09375 to 0.09375
- krylov_basis: float32 [8, 1024, 512], P(None, ('role', 'dev')), may hold values from -64 to 64, as said below
Outputs:
- next_vector: float32 [1024, 512], P(('role', 'dev'))
- hessenberg_column: float32 [9], replicated
The draws below stay inside these ranges and needn't reach their ends.
Inputs may be any that keep to these rules, and one draw needn't show every extreme that they name: `panel_counts`: some cluster has all 512 panels live. `near_lists`: ids of clusters held by the devices at most 3 places from the cluster's own device along role+dev; entries may repeat. `leaf_lists`: ids of clusters held by the devices at most 3 places from the cluster's own device along role+dev; entries may repeat. `krylov_basis`: the vectors are orthonormal under the mean over all 524288 entries, and zero on panels that are not live.
All inputs are finite; a program needn't handle non-finite values.
Results may differ from the reference program's by a relative error of at most 0.0044.
Values may be sent and summed in bfloat16 or wider, within the bound.
No kernel may reach another device: no remote copies, remote signals or barrier semaphores. Data moves between devices by JAX's collectives and lax.ppermute only.
A program may use at most 64 MiB of HBM per device.

```python
import math
import jax
import jax.numpy as jnp
from jax import lax

P_SIZE = 512
C = 256
CL_DEV = 8
NNB = 6
NIL = 16
NOP = 8
KRY = 8
RADIUS = 3
CLUSTERS = 1024
GROUPS = 128


def live_counts(key):
    counts = jax.random.randint(jax.random.fold_in(key, 101), (CLUSTERS,), P_SIZE // 4, P_SIZE + 1)
    chosen = jax.random.randint(jax.random.fold_in(key, 102), (), 0, CLUSTERS)
    return jnp.where(jnp.arange(CLUSTERS) == chosen, P_SIZE, counts).astype(jnp.int32)


def draw_panel_counts(key, part):
    return live_counts(key)


def window_lists(key, width):
    owners = jnp.arange(CLUSTERS, dtype=jnp.int32) // CL_DEV
    offsets = jax.random.randint(key, (CLUSTERS, width), 0, (2 * RADIUS + 1) * CL_DEV)
    listed = (owners[:, None] - RADIUS) * CL_DEV + offsets
    return jnp.clip(listed, 0, CLUSTERS - 1).astype(jnp.int32)


def draw_near_lists(key, part):
    return window_lists(jax.random.fold_in(key, 201), NNB)


def draw_leaf_lists(key, part):
    return window_lists(jax.random.fold_in(key, 202), NIL)


def draw_block_inverse(key, part):
    spread_key = jax.random.fold_in(key, 301)
    scale_key = jax.random.fold_in(key, 302)
    spread_part = jnp.clip(0.5 * jax.random.normal(spread_key, (CLUSTERS, P_SIZE, P_SIZE), jnp.float32), -3.0, 3.0)
    spread_part = spread_part * P_SIZE ** (-0.5)
    diagonal = jax.random.uniform(scale_key, (CLUSTERS, P_SIZE), jnp.float32, 1.0, 2.0)
    return (spread_part + diagonal[:, :, None] * jnp.eye(P_SIZE, dtype=jnp.float32)).astype(jnp.bfloat16)


def draw_krylov_basis(key, part):
    counts = live_counts(key)
    live = (jnp.arange(P_SIZE)[None, :] < counts[:, None]).astype(jnp.float32)
    drawn = jax.random.normal(jax.random.fold_in(key, 401), (KRY, CLUSTERS, P_SIZE), jnp.float32)
    drawn = drawn * live[None]
    entries = CLUSTERS * P_SIZE
    vectors = []
    for index_k in range(KRY):
        vector = drawn[index_k]
        for sweep in range(2):
            for earlier in vectors:
                vector = vector - jnp.sum(vector * earlier) / entries * earlier
        vector = vector * jnp.sqrt(entries / jnp.sum(vector * vector))
        vectors.append(vector)
    return jnp.stack(vectors)


def with_ends(values, stream_key, least, top_value):
    place = [jax.random.randint(jax.random.fold_in(stream_key, axis), (), 0, length) for axis, length in enumerate(values.shape)]
    widest = values.shape.index(max(values.shape))
    neighbour = place[:widest] + [(place[widest] + 1) % values.shape[widest]] + place[widest + 1:]
    return values.at[tuple(place)].set(least).at[tuple(neighbour)].set(top_value)


def shard_levels(key, shape, split, least, top_value):
    def one(axis_at, blocks):
        heights = jax.random.uniform(jax.random.fold_in(jax.random.fold_in(key, 6), axis_at), (blocks,), jnp.float32, least / len(split), top_value / len(split))
        return jnp.repeat(jnp.exp(heights), shape[axis_at] // blocks).reshape((-1,) + (1,) * (len(shape) - axis_at - 1))

    level = one(*split[0])
    for cut in split[1:]:
        level = level * one(*cut)
    return level


def noise(own_key, extent, scale, limit, cuts=(), held_as=jnp.bfloat16):
    result = jax.random.normal(own_key, extent, jnp.float32) * scale
    if len(cuts) > 0:
        result = shard_levels(own_key, extent, cuts, -0.22, 0.18) * result
    return jnp.clip(result, min=-limit, max=limit).astype(held_as)


def setup_inputs(seed: int = 0) -> dict:
    seeds = jax.random.split(jax.random.key(seed), 16)
    return {
        "positions": jnp.clip(jax.random.uniform(seeds[0], (CLUSTERS, 3, P_SIZE), jnp.float32, -1.0, 1.0) * shard_levels(seeds[0], (CLUSTERS, 3, P_SIZE), ((0, 128),), -0.4, 0.0), -1.0, 1.0),
        "normals": noise(seeds[1], (CLUSTERS, 3, P_SIZE), 0.6, 3.6, ((0, 128),), jnp.float32),
        "panel_areas": jnp.clip(jnp.exp(math.log(0.05) - 2.3025851 * jax.random.uniform(seeds[2], (CLUSTERS, P_SIZE), jnp.float32) ** shard_levels(seeds[2], (CLUSTERS, P_SIZE), ((0, 128),), -0.2, 0.2)), 0.005, 0.05),
        "panel_counts": draw_panel_counts(jax.random.fold_in(seeds[15], 71), 0),
        "near_lists": draw_near_lists(jax.random.fold_in(seeds[15], 71), 0),
        "near_counts": with_ends(jax.random.randint(seeds[5], (CLUSTERS,), 1, NNB + 1), jax.random.fold_in(seeds[5], 1), 1, NNB).astype(jnp.int32),
        "leaf_lists": draw_leaf_lists(jax.random.fold_in(seeds[15], 71), 0),
        "leaf_kinds": with_ends(jax.random.randint(seeds[7], (CLUSTERS, NIL), 0, NOP), jax.random.fold_in(seeds[7], 1), 0, NOP - 1).astype(jnp.int32),
        "group_lists": with_ends(jax.random.randint(seeds[8], (GROUPS, NIL), 0, GROUPS), jax.random.fold_in(seeds[8], 1), 0, GROUPS - 1).astype(jnp.int32),
        "group_kinds": with_ends(jax.random.randint(seeds[9], (GROUPS, NIL), 0, NOP), jax.random.fold_in(seeds[9], 1), 0, NOP - 1).astype(jnp.int32),
        "block_inverse": draw_block_inverse(jax.random.fold_in(seeds[15], 71), 0),
        "moment_maps": noise(seeds[11], (CLUSTERS, C, P_SIZE), P_SIZE ** -0.5, 0.25, ((0, 128),)),
        "up_operators": noise(seeds[12], (8, C, C), (8 * C) ** -0.5, 0.125),
        "far_operators": noise(seeds[13], (2, NOP, C, C), (C * NIL) ** -0.5, 0.09375),
        "krylov_basis": draw_krylov_basis(jax.random.fold_in(seeds[15], 71), 0),
    }


SOFTEN = 0.01
EPSILON = 1e-06
HIGH = lax.Precision.HIGHEST

def near_cluster(operands):
    target, sources = operands
    square = jnp.full((sources.shape[0], target.shape[1], sources.shape[2]), SOFTEN, jnp.float32)
    projected = jnp.zeros((sources.shape[0], target.shape[1], sources.shape[2]), jnp.float32)
    for component in range(3):
        offsets = target[component][None, :, None] - sources[:, component][:, None, :]
        square = square + offsets * offsets
        projected = projected + offsets * sources[:, 3 + component][:, None, :]
    inverse = lax.rsqrt(square)
    return lax.optimization_barrier(jnp.sum(projected * inverse * inverse * inverse, axis=(0, 2)))

def translate(chosen, kind_ids, operators):
    onehot = (kind_ids[:, :, None] == jnp.arange(operators.shape[0], dtype=jnp.int32)[None, None, :]).astype(jnp.float32)
    summed = jnp.einsum('gno,gnc->goc', onehot, chosen, precision=HIGH)
    return jnp.einsum('goc,oqc->gq', summed, operators, precision=HIGH)

def precond_one(operands):
    matrix, vector = operands
    return jnp.dot(matrix, vector, preferred_element_type=jnp.float32)

def back_one(operands):
    matrix, vector = operands
    return jnp.dot(vector, matrix, preferred_element_type=jnp.float32)

def reference(positions, normals, panel_areas, panel_counts, near_lists, near_counts, leaf_lists, leaf_kinds, group_lists, group_kinds, block_inverse, moment_maps, up_operators, far_operators, krylov_basis):
    live = (jnp.arange(P_SIZE, dtype=jnp.int32)[None, :] < panel_counts[:, None]).astype(jnp.float32)
    current = krylov_basis[KRY - 1].astype(jnp.bfloat16)
    density = (live * lax.map(precond_one, (block_inverse, current))).astype(jnp.bfloat16)
    density_wide = density.astype(jnp.float32)
    weighted = (panel_areas * density_wide)[:, None, :] * normals
    sources = jnp.concatenate([positions, weighted], axis=1)
    slot_ids = jnp.concatenate([jnp.arange(CLUSTERS, dtype=jnp.int32)[:, None], near_lists.astype(jnp.int32)], axis=1)
    slot_live = (jnp.arange(NNB + 1, dtype=jnp.int32)[None, :] <= near_counts[:, None]).astype(jnp.float32)

    def near_one(operands):
        target, slots, alive = operands
        return near_cluster((target, sources[slots] * alive[:, None, None]))
    near_field = lax.map(near_one, (positions, slot_ids, slot_live))
    moments = lax.map(precond_one, (moment_maps, density)).astype(jnp.bfloat16)
    up_wide = up_operators.astype(jnp.float32)
    far_wide = far_operators.astype(jnp.float32)
    children = moments.astype(jnp.float32).reshape(GROUPS, 8, C)
    group_moments = jnp.einsum('gkc,kqc->gq', children, up_wide, precision=HIGH)
    group_local = translate(group_moments[group_lists], group_kinds, far_wide[1]).astype(jnp.bfloat16)
    downward = jnp.einsum('gq,kqc->gkc', group_local.astype(jnp.float32), up_wide, precision=HIGH).reshape(CLUSTERS, C)
    leaf_local = (translate(moments[leaf_lists].astype(jnp.float32), leaf_kinds, far_wide[0]) + downward).astype(jnp.bfloat16)
    far_field = lax.map(back_one, (moment_maps, leaf_local))
    image = live * (0.5 * density_wide + near_field + far_field)
    entries = CLUSTERS * P_SIZE
    coeffs = jnp.einsum('kcp,cp->k', krylov_basis, image, precision=HIGH) / entries
    remainder = image - jnp.einsum('k,kcp->cp', coeffs, krylov_basis, precision=HIGH)
    height = jnp.sqrt(jnp.sum(remainder * remainder) / entries + EPSILON)
    return (remainder / height, jnp.concatenate([coeffs, height[None]]))
```

```python
import functools

import jax
import jax.numpy as jnp
from jax import lax
from jax.experimental import pallas as pl
from jax.experimental.pallas import tpu as pltpu
from jax.sharding import Mesh
from jax.sharding import PartitionSpec as P

RADIUS = 3
AXES = ("role", "dev_0", "dev_1", "dev_2")
SOFTEN = 0.01
EPSILON = 1e-06
HIGH = lax.Precision.HIGHEST
F32 = jnp.float32
BF16 = jnp.bfloat16
VMEM = pl.BlockSpec(memory_space=pltpu.VMEM)
SMEM = pl.BlockSpec(memory_space=pltpu.SMEM)
NT = (((1,), (1,)), ((), ()))
NN = (((1,), (0,)), ((), ()))
TILE = 256
UNROLL = 4


def dot(a, b, dims):
    return lax.dot_general(a, b, dims, preferred_element_type=F32)


def halves(value):
    top = value.astype(BF16)
    return top, (value - top.astype(F32)).astype(BF16)


def thirds(value):
    top, rest = value.astype(BF16), None
    rest = value - top.astype(F32)
    middle = rest.astype(BF16)
    return top, middle, (rest - middle.astype(F32)).astype(BF16)


def source_kernel(
    counts_ref,
    current_ref,
    inverse_ref,
    maps_ref,
    up_ref,
    position_ref,
    normal_ref,
    area_ref,
    packed_ref,
    tail_ref,
    group_ref,
    density_ref,
):
    c = pl.program_id(0)
    panels = current_ref.shape[1]
    count = counts_ref[c]
    live = lax.broadcasted_iota(jnp.int32, (1, panels), 1) < count
    current = current_ref[pl.ds(c, 1), :].astype(BF16)
    density = dot(current, inverse_ref[0], NT)
    density = jnp.where(live, density, 0.0).astype(BF16)
    wide = density.astype(F32)
    density_ref[pl.ds(c, 1), :] = wide
    moments = dot(density, maps_ref[0], NT).astype(BF16)
    tail_ref[pl.ds(c, 1), :] = jnp.concatenate(
        [moments.astype(F32), jnp.full((1, panels - moments.shape[1]), count.astype(F32))], axis=1
    )
    group = dot(moments, up_ref[0], NT)

    @pl.when(c == 0)
    def _():
        group_ref[...] = group

    @pl.when(c > 0)
    def _():
        group_ref[...] += group

    top, rest = halves(position_ref[0])
    position = top.astype(F32) + rest.astype(F32)
    weighted = (area_ref[pl.ds(c, 1), :] * wide) * normal_ref[0]
    packed_ref[0] = jnp.concatenate(
        [
            position,
            jnp.sum(position * position, axis=0, keepdims=True),
            weighted,
            jnp.sum(position * weighted, axis=0, keepdims=True),
        ],
        axis=0,
    )


def sources(counts, current, inverse, maps, up, positions, normals, areas):
    clusters, panels = current.shape
    coeffs = maps.shape[1]
    whole = lambda *shape: pl.BlockSpec(shape, lambda c: (0,) * len(shape))
    step = lambda *shape: pl.BlockSpec((1,) + shape, lambda c: (c,) + (0,) * len(shape))
    return pl.pallas_call(
        source_kernel,
        grid=(clusters,),
        in_specs=[
            SMEM,
            whole(clusters, panels),
            step(panels, panels),
            step(coeffs, panels),
            step(coeffs, coeffs),
            step(3, panels),
            step(3, panels),
            whole(clusters, panels),
        ],
        out_specs=[
            step(8, panels),
            whole(clusters, panels),
            whole(1, coeffs),
            whole(clusters, panels),
        ],
        out_shape=[
            jax.ShapeDtypeStruct((clusters, 8, panels), F32),
            jax.ShapeDtypeStruct((clusters, panels), F32),
            jax.ShapeDtypeStruct((1, coeffs), F32),
            jax.ShapeDtypeStruct((clusters, panels), F32),
        ],
        cost_estimate=pl.CostEstimate(flops=10**9, bytes_accessed=8 * 2**20, transcendentals=0),
    )(counts, current, inverse, maps, up, positions, normals, areas)


def near_kernel(
    slots_ref, nears_ref, counts_ref, source_counts_ref, window_ref, out_ref,
    target_list, source_list, features, total,
):
    clusters = out_ref.shape[0]
    panels = out_ref.shape[1]
    per_cluster = panels // TILE
    own = window_ref

    def list_cluster(c, length):
        across = (counts_ref[c] + TILE - 1) // TILE

        def list_slot(s, at):
            w = slots_ref[c, s]
            down = (source_counts_ref[w] + TILE - 1) // TILE
            for place, i, j in ((1, 0, 1), (across + 1, 1, 1), (across, 1, 0), (0, 0, 0)):
                target_list[at + place] = c * per_cluster + j
                source_list[at + place] = w * per_cluster + i
            return at + down * across

        return lax.fori_loop(0, nears_ref[c] + 1, list_slot, length)

    length = lax.fori_loop(0, clusters, list_cluster, jnp.int32(0))
    for extra in range(UNROLL - 1):
        target_list[length + extra] = clusters * per_cluster
        source_list[length + extra] = 0

    total[...] = jnp.zeros_like(total)

    def make_features(c, carry):
        rows = own[c]
        position, norm = rows[0:3], rows[3:4] + SOFTEN
        top, rest, _ = thirds(-2.0 * position)
        a, b, d = thirds(norm)
        one = jnp.ones((1, panels), F32)
        none = jnp.zeros((8, panels), F32)
        top, rest = top.astype(F32), rest.astype(F32)
        pad = none[0:4]
        rows48 = jnp.concatenate(
            [top, one, pad, rest, none[0:5], top, one, pad, rest, none[0:5],
             none[0:3], one, pad,
             a.astype(F32), b.astype(F32), d.astype(F32), none[0:5]], axis=0
        )
        turned = jnp.concatenate([rows48, jnp.zeros((80, panels), F32)], axis=0).T
        features[pl.ds(c * panels, panels), :] = turned.astype(BF16)
        return carry

    features[pl.ds(clusters * panels, TILE), :] = jnp.zeros((TILE, 128), BF16)
    lax.fori_loop(0, clusters, make_features, 0)

    def step(g, carry):
        results = []
        for u in range(UNROLL):
            t = target_list[g * UNROLL + u]
            s = source_list[g * UNROLL + u]
            w = s // per_cluster
            lane = pl.multiple_of((s % per_cluster) * TILE, TILE)
            rows = window_ref[w, :, pl.ds(lane, TILE)]
            top, middle, low = thirds(rows)
            ones = jnp.ones((8, TILE), BF16)
            right = jnp.concatenate([top, top, middle, middle, low, ones, jnp.zeros((80, TILE), BF16)], axis=0)
            left = features[pl.ds(pl.multiple_of(t * TILE, TILE), TILE), :]
            inverse = lax.rsqrt(jnp.maximum(dot(left, right, NN), SOFTEN * 0.5))
            field = (inverse * inverse * inverse).astype(BF16)
            results.append((t, dot(jnp.concatenate([top, middle], axis=0), field, NT)))
        for t, result in results:
            total[t] += result
        return carry

    lax.fori_loop(0, (length + UNROLL - 1) // UNROLL, step, 0)

    for c in range(clusters):
        for j in range(per_cluster):
            r = total[c * per_cluster + j]
            r = r[0:8] + r[8:16]
            x = window_ref[c, 0:3, j * TILE : (j + 1) * TILE]
            out_ref[c : c + 1, j * TILE : (j + 1) * TILE] = (
                jnp.sum(x * r[4:7], axis=0, keepdims=True) - r[7:8]
            )


def near_fields(slots, nears, counts, source_counts, window):
    clusters = slots.shape[0]
    panels = window.shape[2]
    per_cluster = panels // TILE
    most = clusters * slots.shape[1] * per_cluster * per_cluster + 8
    return pl.pallas_call(
        near_kernel,
        in_specs=[SMEM, SMEM, SMEM, SMEM, VMEM],
        out_specs=VMEM,
        out_shape=jax.ShapeDtypeStruct((clusters, panels), F32),
        scratch_shapes=[
            pltpu.SMEM((most,), jnp.int32),
            pltpu.SMEM((most,), jnp.int32),
            pltpu.VMEM((clusters * panels + TILE, 128), BF16),
            pltpu.VMEM((clusters * per_cluster + 1, 16, TILE), F32),
        ],
        cost_estimate=pl.CostEstimate(flops=2 * 10**9, bytes_accessed=2**20, transcendentals=10**6),
    )(slots, nears, counts, source_counts, window)


def far_kernel(
    counts_ref, leaf_pick_ref, group_pick_ref, moments_ref, groups_ref, far_ref, up_ref, maps_ref,
    density_ref, near_ref, basis_ref, image_ref, sums_ref,
):
    clusters, panels = density_ref.shape
    kinds = far_ref.shape[1]
    coeffs = far_ref.shape[2]
    group_sum = lax.dot_general(
        group_pick_ref[...], groups_ref[...], NN, precision=HIGH, preferred_element_type=F32
    )
    local = jnp.zeros((1, coeffs), F32)
    for o in range(kinds):
        parts = jnp.concatenate(
            [p.astype(F32) for p in thirds(group_sum[o : o + 1])] + [jnp.zeros((5, coeffs), F32)], axis=0
        ).astype(BF16)
        local += jnp.sum(dot(parts, far_ref[1, o], NT), axis=0, keepdims=True)
    local = local.astype(BF16)
    leaf_sum = dot(leaf_pick_ref[...].astype(BF16), moments_ref[...].astype(BF16), NN)
    leaf = jnp.zeros((2 * clusters, coeffs), F32)
    for o in range(kinds):
        top, rest = halves(leaf_sum[o * clusters : (o + 1) * clusters])
        leaf += dot(jnp.concatenate([top, rest], axis=0), far_ref[0, o], NT)
    leaf = leaf[0:clusters] + leaf[clusters:]
    total = jnp.zeros((8, 128), F32)
    rows = lax.broadcasted_iota(jnp.int32, (1, 128), 1)
    images = []
    for c in range(clusters):
        down = dot(local, up_ref[c], NN)
        leaf_local = (leaf[c : c + 1] + down).astype(BF16)
        far = dot(leaf_local, maps_ref[c], NN)
        live = lax.broadcasted_iota(jnp.int32, (1, panels), 1) < counts_ref[c]
        images.append(
            jnp.where(live, 0.5 * density_ref[c : c + 1] + near_ref[c : c + 1] + far, 0.0)
        )
    image = jnp.concatenate(images, axis=0)
    image_ref[...] = image
    sums = jnp.zeros((1, 128), F32)
    for k in range(basis_ref.shape[0] + 1):
        other = basis_ref[k] if k < basis_ref.shape[0] else image
        value = jnp.sum(jnp.sum(image * other, axis=0, keepdims=True), axis=1, keepdims=True)
        sums += jnp.where(rows == k, value, 0.0)
    sums_ref[...] = jnp.broadcast_to(sums, sums_ref.shape)


def far_fields(counts, leaf_pick, group_pick, moments, groups, far, up, maps, density, near, basis, devices):
    return pl.pallas_call(
        far_kernel,
        in_specs=[SMEM] + [VMEM] * 10,
        out_specs=[VMEM, VMEM],
        out_shape=[
            jax.ShapeDtypeStruct(density.shape, F32),
            jax.ShapeDtypeStruct((devices, 128), F32),
        ],
        cost_estimate=pl.CostEstimate(flops=10**8, bytes_accessed=2**20, transcendentals=0),
    )(counts, leaf_pick, group_pick, moments, groups, far, up, maps, density, near, basis)


def close_kernel(rows, sums_ref, image_ref, basis_ref, next_ref, column_ref):
    count = basis_ref.shape[0]
    means = jnp.sum(sums_ref[...], axis=0, keepdims=True) * (1.0 / rows)
    lane = lax.broadcasted_iota(jnp.int32, (1, 128), 1)
    coeffs = jnp.where(lane < count, means, 0.0)
    square = jnp.sum(jnp.where(lane == count, means, 0.0), axis=1, keepdims=True)
    energy = square - jnp.sum(coeffs * coeffs, axis=1, keepdims=True)
    height = jnp.sqrt(energy + EPSILON)
    column_ref[...] = jnp.where(lane == count, height, coeffs)
    remainder = image_ref[...]
    for k in range(count):
        remainder = remainder - coeffs[:, k : k + 1] * basis_ref[k]
    next_ref[...] = remainder / height


def close(sums, image, basis, rows):
    return pl.pallas_call(
        functools.partial(close_kernel, rows),
        in_specs=[VMEM] * 3,
        out_specs=[VMEM, VMEM],
        out_shape=[
            jax.ShapeDtypeStruct(image.shape, F32),
            jax.ShapeDtypeStruct((1, 128), F32),
        ],
    )(sums, image, basis)


def row_routes(rows, width):
    spot = lambda r, y: (r % rows) * width + y
    turns = {1: (1, -1, -1, -1), 2: (1, 1, -1, -1), 3: (1, 1, 1, -1)}
    return {
        k: [(spot(r, y), spot(r + turns[k][y], y)) for r in range(rows) for y in range(width)]
        for k in turns
    }


def shards(
    positions, normals, panel_areas, panel_counts, near_lists, near_counts, leaf_lists, leaf_kinds,
    group_lists, group_kinds, block_inverse, moment_maps, up_operators, far_operators, krylov_basis,
):
    clusters, _, panels = positions.shape
    coeff_count = moment_maps.shape[1]
    own = lax.axis_index(AXES)
    devices = lax.axis_size(AXES)
    width = lax.axis_size(AXES[-1])
    kinds = jnp.arange(far_operators.shape[1], dtype=jnp.int32)

    def place(ids):
        owner = ids // clusters
        shift = (own - owner) % width
        return shift + jnp.where(owner // width == own // width, 0, width - 1)

    own_ids = own * clusters + lax.broadcasted_iota(jnp.int32, (clusters, 1), 0)
    near_ids = jnp.concatenate([own_ids, near_lists], axis=1)
    slots = place(near_ids) * (clusters + 1) + near_ids % clusters
    leaf_rows = place(leaf_lists) * clusters + leaf_lists % clusters
    window_rows = jnp.arange((2 * RADIUS + 1) * clusters, dtype=jnp.int32)
    leaf_pick = jnp.sum(
        (leaf_kinds[None, :, :, None] == kinds[:, None, None, None])
        & (leaf_rows[None, :, :, None] == window_rows[None, None, None, :]),
        axis=2, dtype=F32,
    ).reshape(kinds.shape[0] * clusters, -1)
    group_pick = jnp.sum(
        (group_kinds[0][None, :, None] == kinds[:, None, None])
        & (group_lists[0][None, :, None] == jnp.arange(devices, dtype=jnp.int32)[None, None, :]),
        axis=1, dtype=F32,
    )

    packed, tail, group, density = sources(
        panel_counts, krylov_basis[-1], block_inverse, moment_maps, up_operators, positions, normals,
        panel_areas,
    )
    payload = jnp.concatenate([packed, tail[None]], axis=0)
    row = [payload] + [
        lax.ppermute(payload, AXES[-1], [(y, (y + k) % width) for y in range(width)])
        for k in range(1, width)
    ]
    routes = row_routes(devices // width, width)
    window = row + [lax.ppermute(row[k], AXES, routes[k]) for k in range(1, width)]
    groups = lax.all_to_all(
        jnp.broadcast_to(group, (devices, coeff_count)), AXES, 0, 0, tiled=True
    )
    window = jnp.concatenate(window, axis=0)
    tails = window.reshape(-1, clusters + 1, 8, panels)[:, clusters]
    source_counts = tails[:, :, coeff_count].astype(jnp.int32)
    source_counts = jnp.concatenate(
        [source_counts, jnp.zeros((source_counts.shape[0], 1), jnp.int32)], axis=1
    ).reshape(-1)
    near = near_fields(slots, near_counts, panel_counts, source_counts, window)
    moments = tails[:, :, :coeff_count].reshape(-1, coeff_count)
    image, sums = far_fields(
        panel_counts, leaf_pick, group_pick, moments, groups, far_operators, up_operators,
        moment_maps, density, near, krylov_basis, devices,
    )
    sums = lax.all_to_all(sums, AXES, 0, 0, tiled=True)
    following, column = close(sums, image, krylov_basis, devices * clusters * panels)
    return following, column[0, : krylov_basis.shape[0] + 1]


def solution(mesh):
    finer = Mesh(mesh.devices.reshape(mesh.shape["role"], 4, 4, 4), AXES)
    split = lambda rank: P(AXES, *([None] * (rank - 1)))
    return jax.shard_map(
        shards,
        mesh=finer,
        in_specs=(
            split(3), split(3), split(2), split(1), split(2), split(1), split(2), split(2), split(2),
            split(2), split(3), split(3), P(), P(), P(None, AXES, None),
        ),
        out_specs=(split(2), P()),
        check_vma=False,
    )
```

```python
import functools

import jax
import jax.numpy as jnp
from jax import lax
from jax.experimental import pallas as pl
from jax.experimental.pallas import tpu as pltpu
from jax.sharding import Mesh
from jax.sharding import PartitionSpec as P

RADIUS = 3
AXES = ("role", "dev_0", "dev_1", "dev_2")
SOFTEN = 0.01
EPSILON = 1e-06
HIGH = lax.Precision.HIGHEST
F32 = jnp.float32
BF16 = jnp.bfloat16
VMEM = pl.BlockSpec(memory_space=pltpu.VMEM)
SMEM = pl.BlockSpec(memory_space=pltpu.SMEM)
ANY = pl.BlockSpec(memory_space=pl.ANY)
HBM = pl.BlockSpec(memory_space=pltpu.HBM)
NT = (((1,), (1,)), ((), ()))
NN = (((1,), (0,)), ((), ()))
HIGHER = 128
ACROSS = 256
UNROLL = 8
MIB = 2**20


def dot(a, b, dims):
    return lax.dot_general(a, b, dims, preferred_element_type=F32)


def halves(value):
    top = value.astype(BF16)
    return top, (value - top.astype(F32)).astype(BF16)


def thirds(value):
    top, rest = value.astype(BF16), None
    rest = value - top.astype(F32)
    middle = rest.astype(BF16)
    return top, middle, (rest - middle.astype(F32)).astype(BF16)


def power(value):
    assert value & (value - 1) == 0
    return value.bit_length() - 1


def window_block(own, ids, clusters, width):
    owner = lax.shift_right_logical(ids, power(clusters))
    shift = (own - owner) & (width - 1)
    same = lax.shift_right_logical(owner, power(width)) == lax.shift_right_logical(own, power(width))
    return jnp.where(same, shift, shift + width - 1), ids & (clusters - 1)


def source_kernel(
    counts_ref, basis_ref, inverse_hbm, maps_hbm, up_hbm, position_ref, normal_ref, area_ref,
    payload_ref, group_ref, density_ref, inverse_ref, maps_ref, up_ref, sems,
):
    clusters, panels = density_ref.shape
    coeffs = maps_ref.shape[1]
    copies = [
        [pltpu.make_async_copy(a.at[c], b.at[c], sems.at[k, c]) for c in range(clusters)]
        for k, (a, b) in enumerate(((inverse_hbm, inverse_ref), (maps_hbm, maps_ref), (up_hbm, up_ref)))
    ]
    for group in copies:
        for copy in group:
            copy.start()
    lane = lax.broadcasted_iota(jnp.int32, (1, panels), 1)
    densities = []
    for c in range(clusters):
        copies[0][c].wait()
        current = basis_ref[0, c : c + 1].astype(BF16)
        density = dot(current, inverse_ref[c], NT)
        densities.append(jnp.where(lane < counts_ref[c], density, 0.0).astype(BF16))
    wide = jnp.concatenate([d.astype(F32) for d in densities], axis=0)
    density_ref[...] = wide
    total = jnp.zeros((1, coeffs), F32)
    tails = []
    for c in range(clusters):
        copies[1][c].wait()
        moments = dot(densities[c], maps_ref[c], NT).astype(BF16)
        tails.append(moments)
    for c in range(clusters):
        copies[2][c].wait()
        total += dot(tails[c], up_ref[c], NT)
        payload_ref[clusters, c : c + 1, 0:coeffs] = tails[c].astype(F32)
        payload_ref[clusters, c : c + 1, coeffs:panels] = jnp.full(
            (1, panels - coeffs), counts_ref[c].astype(F32)
        )
    lines = coeffs // 128
    row = lax.broadcasted_iota(jnp.int32, group_ref.shape, 0) & (lines - 1)
    spread = total[:, 0:128]
    for k in range(1, lines):
        spread = jnp.where(row == k, total[:, 128 * k : 128 * k + 128], spread)
    group_ref[...] = jnp.broadcast_to(spread, group_ref.shape)
    norm = jnp.zeros((clusters, panels), F32)
    across = jnp.zeros((clusters, panels), F32)
    rows = []
    scale = area_ref[...] * wide
    weights = []
    for a in range(3):
        top, rest = halves(position_ref[a])
        position = top.astype(F32) + rest.astype(F32)
        weighted = scale * normal_ref[a]
        norm += position * position
        across += position * weighted
        rows.append(position)
        weights.append(weighted)
    for k, value in enumerate(rows + [norm] + weights + [across]):
        for c in range(clusters):
            payload_ref[c, k : k + 1, :] = value[c : c + 1]


def sources(counts, basis, inverse, maps, up, positions, normals, areas, devices):
    count, clusters, panels = basis.shape
    coeffs = maps.shape[1]
    lines = devices * coeffs // 128
    whole = lambda *shape: pl.BlockSpec(shape, lambda i: (0,) * len(shape))
    return pl.pallas_call(
        source_kernel,
        grid=(1,),
        in_specs=[
            SMEM,
            pl.BlockSpec((1, clusters, panels), lambda i: (count - 1, 0, 0)),
            HBM,
            HBM,
            HBM,
            whole(3, clusters, panels),
            whole(3, clusters, panels),
            whole(clusters, panels),
        ],
        out_specs=[
            whole(clusters + 1, 8, panels),
            whole(lines, 128),
            whole(clusters, panels),
        ],
        out_shape=[
            jax.ShapeDtypeStruct((clusters + 1, 8, panels), F32),
            jax.ShapeDtypeStruct((lines, 128), F32),
            jax.ShapeDtypeStruct((clusters, panels), F32),
        ],
        scratch_shapes=[
            pltpu.VMEM(inverse.shape, BF16),
            pltpu.VMEM(maps.shape, BF16),
            pltpu.VMEM(up.shape, BF16),
            pltpu.SemaphoreType.DMA((3, clusters)),
        ],
        compiler_params=pltpu.CompilerParams(vmem_limit_bytes=14 * MIB),
        cost_estimate=pl.CostEstimate(flops=4 * 10**8, bytes_accessed=8 * MIB, transcendentals=0),
    )(counts, basis, inverse, maps, up, positions, normals, areas)


def near_tiles(
    own, blocks, first, lists_ref, nears_ref, counts_ref, tails, window, positions_of,
    target_list, source_list, features, total, squares,
):
    clusters, slots = lists_ref.shape
    panels = window.shape[2]
    highs, wides = panels // HIGHER, panels // ACROSS
    width = 4
    begin, end = blocks

    def list_cluster(c, length):
        across = (counts_ref[c] + HIGHER - 1) // HIGHER

        def entry(at, block, local):
            used = (block >= begin) & (block < end)
            held = jnp.where(used, block - begin, 0)
            live = tails[held, local, 0].astype(jnp.int32)
            down = jnp.where(used, (live + ACROSS - 1) // ACROSS, 0)
            w = held * (clusters + 1) + local
            for j in reversed(range(highs)):
                for i in reversed(range(wides)):
                    target_list[at + i * across + j] = c * highs + j
                    source_list[at + i * across + j] = w * wides + i
            return at + down * across

        def list_slot(s, at):
            return entry(at, *window_block(own, lists_ref[c, s], clusters, width))

        if first:
            length = entry(length, jnp.int32(0), c)
        return lax.fori_loop(0, nears_ref[c], list_slot, length)

    length = lax.fori_loop(0, clusters, list_cluster, jnp.int32(0))
    for extra in range(2 * UNROLL):
        target_list[length + extra] = clusters * highs
        source_list[length + extra] = 0

    total[...] = jnp.zeros_like(total)

    def make_features(c, carry):
        rows = positions_of(c)
        position, norm = rows[0:3], rows[3:4] + SOFTEN
        top, rest = [part.astype(F32) for part in halves(-2.0 * position)]
        a, b, d = [part.astype(F32) for part in thirds(norm)]
        one = jnp.ones((1, panels), F32)
        none = jnp.zeros((8, panels), F32)
        turned = jnp.concatenate(
            [top, one, none[0:4], rest, none[0:5], top, one, none[0:4], rest, none[0:5],
             none[0:3], one, none[0:4], a, b, d, none[0:5], jnp.zeros((80, panels), F32)], axis=0
        ).T
        features[pl.ds(pl.multiple_of(c * panels, panels), panels), :] = turned.astype(BF16)
        return carry

    lax.fori_loop(0, clusters, make_features, 0)
    features[pl.ds(clusters * panels, HIGHER), :] = jnp.where(
        lax.broadcasted_iota(jnp.int32, (HIGHER, 128), 1) == 40, 1.0, 0.0
    ).astype(BF16)

    def tile(s):
        lane = pl.multiple_of((s & (wides - 1)) * ACROSS, ACROSS)
        return window[lax.shift_right_logical(s, power(wides)), :, pl.ds(lane, ACROSS)]

    def square(at, u):
        top, middle, low = thirds(tile(source_list[at]))
        right = jnp.concatenate(
            [top, top, middle, middle, low, jnp.ones((8, ACROSS), BF16), jnp.zeros((80, ACROSS), BF16)],
            axis=0,
        )
        left = features[pl.ds(pl.multiple_of(target_list[at] * HIGHER, HIGHER), HIGHER), :]
        squares[u] = dot(left, right, NN)

    def apply(at, u):
        inverse = lax.rsqrt(squares[u])
        field = (inverse * inverse * inverse).astype(BF16)
        top, rest = halves(tile(source_list[at]))
        return dot(jnp.concatenate([top, rest], axis=0), field, NT)

    for u in range(UNROLL):
        square(u, u)

    def step(g, carry):
        results = []
        for u in range(UNROLL):
            results.append((target_list[g * UNROLL + u], apply(g * UNROLL + u, u)))
            square((g + 1) * UNROLL + u, u)
        for t, result in results:
            total[t] += result
        return carry

    lax.fori_loop(0, (length + UNROLL - 1) // UNROLL, step, 0)

    lines = []
    for c in range(clusters):
        parts = []
        for j in range(highs):
            r = total[c * highs + j]
            r = r[0:8] + r[8:16]
            x = positions_of(c)[0:3, j * HIGHER : (j + 1) * HIGHER]
            parts.append(jnp.sum(x * r[4:7], axis=0, keepdims=True) - r[7:8])
        lines.append(jnp.concatenate(parts, axis=1))
    return jnp.concatenate(lines, axis=0)


def near_scratch(clusters, slots, panels, blocks):
    highs, wides = panels // HIGHER, panels // ACROSS
    most = clusters * slots * highs * wides + 4 * UNROLL
    return [
        pltpu.SMEM((most,), jnp.int32),
        pltpu.SMEM((most,), jnp.int32),
        pltpu.VMEM((clusters * panels + HIGHER, 128), BF16),
        pltpu.VMEM((clusters * highs + 1, 16, HIGHER), F32),
        pltpu.VMEM((UNROLL, HIGHER, ACROSS), F32),
        pltpu.VMEM((blocks * (clusters + 1), 8, panels), F32),
        pltpu.SMEM((blocks, clusters, 128), F32),
    ]


def row_kernel(own_ref, lists_ref, nears_ref, counts_ref, a_ref, b_ref, c_ref, d_ref, out_ref,
               target_list, source_list, features, total, squares, window, tails, sems):
    clusters = lists_ref.shape[0]
    blocks = (a_ref, b_ref, c_ref, d_ref)
    coeffs = window.shape[2] // 2
    copies = []
    for k, block in enumerate(blocks):
        copies.append(pltpu.make_async_copy(
            block, window.at[pl.ds(k * (clusters + 1), clusters + 1)], sems.at[0, k]))
        copies.append(pltpu.make_async_copy(
            block.at[clusters, :, pl.ds(coeffs, 128)], tails.at[k], sems.at[1, k]))
    for copy in copies:
        copy.start()
    for copy in copies:
        copy.wait()
    out_ref[...] = near_tiles(
        own_ref[0], (0, len(blocks)), True, lists_ref, nears_ref, counts_ref, tails, window,
        lambda c: window[c], target_list, source_list, features, total, squares,
    )


def row_fields(own, lists, nears, counts, blocks):
    clusters, slots = lists.shape
    panels = blocks[0].shape[2]
    return pl.pallas_call(
        row_kernel,
        in_specs=[SMEM] * 4 + [ANY] * len(blocks),
        out_specs=VMEM,
        out_shape=jax.ShapeDtypeStruct((clusters, panels), F32),
        scratch_shapes=near_scratch(clusters, slots + 1, panels, len(blocks))
        + [pltpu.SemaphoreType.DMA((2, len(blocks)))],
        compiler_params=pltpu.CompilerParams(vmem_limit_bytes=12 * MIB),
        cost_estimate=pl.CostEstimate(flops=3 * 10**9, bytes_accessed=MIB, transcendentals=10**6),
    )(own, lists, nears, counts, *blocks)


def late_kernel(
    own_ref, lists_ref, nears_ref, counts_ref, leaf_ids_ref, leaf_kinds_ref, group_ids_ref,
    group_kinds_ref, groups_ref, density_ref, near_ref, basis_ref, far_hbm, up_hbm, maps_hbm,
    a_ref, b_ref, c_ref, d_ref, e_ref, f_ref, g_ref,
    image_ref, sums_ref,
    target_list, source_list, features, total, squares, window, tails, sems,
    far_ref, up_ref, maps_ref, own_rows, moments, weight_sems,
):
    clusters, panels = density_ref.shape
    kinds, coeffs = far_ref.shape[1], far_ref.shape[2]
    row, others = (a_ref, b_ref, c_ref, d_ref), (e_ref, f_ref, g_ref)
    copies = []
    for k, block in enumerate(others):
        copies.append(pltpu.make_async_copy(
            block, window.at[pl.ds(k * (clusters + 1), clusters + 1)], sems.at[0, k]))
        copies.append(pltpu.make_async_copy(
            block.at[clusters, :, pl.ds(coeffs, 128)], tails.at[k], sems.at[1, k]))
    copies.append(pltpu.make_async_copy(a_ref, own_rows, weight_sems.at[3]))
    for copy in copies:
        copy.start()
    later = [
        pltpu.make_async_copy(block.at[clusters, :, pl.ds(0, coeffs)],
                              moments.at[pl.ds(k * clusters, clusters)], sems.at[2, k])
        for k, block in enumerate(row + others)
    ]
    later += [
        pltpu.make_async_copy(far_hbm, far_ref, weight_sems.at[0]),
        pltpu.make_async_copy(up_hbm, up_ref, weight_sems.at[1]),
        pltpu.make_async_copy(maps_hbm, maps_ref, weight_sems.at[2]),
    ]
    for copy in later:
        copy.start()
    for copy in copies:
        copy.wait()
    own = own_ref[0]
    near = near_ref[...] + near_tiles(
        own, (4, 7), False, lists_ref, nears_ref, counts_ref, tails, window,
        lambda c: own_rows[c], target_list, source_list, features, total, squares,
    )
    for copy in later:
        copy.wait()

    lines = coeffs // 128
    spots = groups_ref.shape[0]
    kind = lax.broadcasted_iota(jnp.int32, (kinds, 1), 0)
    spot = lax.broadcasted_iota(jnp.int32, (1, spots), 1)
    pick = jnp.zeros((kinds, spots), F32)
    for n in range(group_ids_ref.shape[1]):
        hit = (kind == group_kinds_ref[0, n]) & (
            lax.shift_right_logical(spot, power(lines)) == group_ids_ref[0, n])
        pick += jnp.where(hit, 1.0, 0.0)
    local = jnp.zeros((24, coeffs), F32)
    group_sum = jnp.concatenate(
        [
            lax.dot_general(jnp.where((spot & (lines - 1)) == k, pick, 0.0), groups_ref[...], NN,
                            precision=HIGH, preferred_element_type=F32)
            for k in range(lines)
        ],
        axis=1,
    )
    group_rows = jnp.concatenate([part.astype(F32) for part in thirds(group_sum)], axis=0)
    row24 = lax.broadcasted_iota(jnp.int32, (24, 1), 0) & (kinds - 1)
    for o in range(kinds):
        local += dot(jnp.where(row24 == o, group_rows, 0.0).astype(BF16), far_ref[1, o], NT)
    local = jnp.sum(local, axis=0, keepdims=True).astype(BF16)

    block, inside = window_block(own, leaf_ids_ref[...], clusters, 4)
    spots_of = block * clusters + inside
    spot = lax.broadcasted_iota(jnp.int32, (1, moments.shape[0]), 1)
    picks = [jnp.zeros((clusters, moments.shape[0]), F32) for _ in range(kinds)]
    for n in range(leaf_ids_ref.shape[1]):
        hit = jnp.where(spots_of[:, n : n + 1] == spot, 1.0, 0.0)
        for o in range(kinds):
            picks[o] += jnp.where(leaf_kinds_ref[:, n : n + 1] == o, hit, 0.0)
    leaf_sum = dot(
        jnp.concatenate(picks, axis=0).astype(BF16), moments[...].astype(BF16), NN
    )
    leaf = jnp.zeros((2 * clusters, coeffs), F32)
    for o in range(kinds):
        top, rest = halves(leaf_sum[o * clusters : (o + 1) * clusters])
        leaf += dot(jnp.concatenate([top, rest], axis=0), far_ref[0, o], NT)
    leaf = leaf[0:clusters] + leaf[clusters:]
    leaf += jnp.concatenate([dot(local, up_ref[c], NN) for c in range(clusters)], axis=0)
    leaf = leaf.astype(BF16)
    images = []
    lane = lax.broadcasted_iota(jnp.int32, (1, panels), 1)
    for c in range(clusters):
        far = dot(leaf[c : c + 1], maps_ref[c], NN)
        value = 0.5 * density_ref[c : c + 1] + near[c : c + 1] + far
        images.append(jnp.where(lane < counts_ref[c], value, 0.0))
    image = jnp.concatenate(images, axis=0)
    image_ref[...] = image
    lane = lax.broadcasted_iota(jnp.int32, (1, 128), 1)
    sums = jnp.zeros((1, 128), F32)
    for k in range(basis_ref.shape[0] + 1):
        other = basis_ref[k] if k < basis_ref.shape[0] else image
        value = jnp.sum(jnp.sum(image * other, axis=0, keepdims=True), axis=1, keepdims=True)
        sums += jnp.where(lane == k, value, 0.0)
    sums_ref[...] = jnp.broadcast_to(sums, sums_ref.shape)


def late_fields(own, lists, nears, counts, leaf_ids, leaf_kinds, group_ids, group_kinds, groups,
                density, near, basis, far, up, maps, window, devices):
    clusters, slots = lists.shape
    panels = density.shape[1]
    return pl.pallas_call(
        late_kernel,
        in_specs=[SMEM] * 4 + [VMEM] * 2 + [SMEM] * 2 + [VMEM] * 4 + [HBM] * 3 + [ANY] * 7,
        out_specs=[VMEM, VMEM],
        out_shape=[
            jax.ShapeDtypeStruct(density.shape, F32),
            jax.ShapeDtypeStruct((devices, 128), F32),
        ],
        scratch_shapes=near_scratch(clusters, slots + 1, panels, 3)
        + [
            pltpu.SemaphoreType.DMA((3, 7)),
            pltpu.VMEM(far.shape, BF16),
            pltpu.VMEM(up.shape, BF16),
            pltpu.VMEM(maps.shape, BF16),
            pltpu.VMEM((clusters + 1, 8, panels), F32),
            pltpu.VMEM((7 * clusters, maps.shape[1]), F32),
            pltpu.SemaphoreType.DMA((4,)),
        ],
        compiler_params=pltpu.CompilerParams(vmem_limit_bytes=20 * MIB),
        cost_estimate=pl.CostEstimate(flops=3 * 10**9, bytes_accessed=MIB, transcendentals=10**6),
    )(own, lists, nears, counts, leaf_ids, leaf_kinds, group_ids, group_kinds, groups, density,
      near, basis, far, up, maps, *window)


def close_kernel(rows, sums_ref, image_ref, basis_ref, next_ref, column_ref):
    count = basis_ref.shape[0]
    means = jnp.sum(sums_ref[...], axis=0, keepdims=True) * (1.0 / rows)
    lane = lax.broadcasted_iota(jnp.int32, (1, 128), 1)
    coeffs = jnp.where(lane < count, means, 0.0)
    square = jnp.sum(jnp.where(lane == count, means, 0.0), axis=1, keepdims=True)
    energy = square - jnp.sum(coeffs * coeffs, axis=1, keepdims=True)
    height = jnp.sqrt(energy + EPSILON)
    remainder = image_ref[...]
    for k in range(count):
        remainder = remainder - coeffs[:, k : k + 1] * basis_ref[k]
        column_ref[k] = means[0, k]
    column_ref[count] = height[0, 0]
    next_ref[...] = remainder / height


def close(sums, image, basis, rows):
    return pl.pallas_call(
        functools.partial(close_kernel, rows),
        in_specs=[VMEM] * 3,
        out_specs=[VMEM, SMEM],
        out_shape=[
            jax.ShapeDtypeStruct(image.shape, F32),
            jax.ShapeDtypeStruct((basis.shape[0] + 1,), F32),
        ],
        compiler_params=pltpu.CompilerParams(vmem_limit_bytes=2 * MIB),
    )(sums, image, basis)


def row_routes(rows, width):
    spot = lambda r, y: (r % rows) * width + y
    turns = {1: (1, -1, -1, -1), 2: (1, 1, -1, -1), 3: (1, 1, 1, -1)}
    return {
        k: [(spot(r, y), spot(r + turns[k][y], y)) for r in range(rows) for y in range(width)]
        for k in turns
    }


def shards(
    positions, normals, panel_areas, panel_counts, near_lists, near_counts, leaf_lists, leaf_kinds,
    group_lists, group_kinds, block_inverse, moment_maps, up_operators, far_operators, krylov_basis,
):
    clusters, _, panels = positions.shape
    coeffs = moment_maps.shape[1]
    devices = lax.axis_size(AXES)
    width = lax.axis_size(AXES[-1])
    own = jnp.full((1,), lax.axis_index(AXES), jnp.int32)
    payload, group, density = sources(
        panel_counts, krylov_basis, block_inverse, moment_maps, up_operators,
        positions.transpose(1, 0, 2), normals.transpose(1, 0, 2), panel_areas, devices,
    )
    row = [payload] + [
        lax.ppermute(payload, AXES[-1], [(y, (y + k) % width) for y in range(width)])
        for k in range(1, width)
    ]
    routes = row_routes(devices // width, width)
    window = row + [lax.ppermute(row[k], AXES, routes[k]) for k in range(1, width)]
    groups = lax.all_to_all(group, AXES, 0, 0, tiled=True)
    near = row_fields(own, near_lists, near_counts, panel_counts, row)
    image, sums = late_fields(
        own, near_lists, near_counts, panel_counts, leaf_lists, leaf_kinds, group_lists, group_kinds,
        groups, density, near, krylov_basis, far_operators, up_operators, moment_maps, window, devices,
    )
    sums = lax.all_to_all(sums, AXES, 0, 0, tiled=True)
    return close(sums, image, krylov_basis, devices * clusters * panels)


def solution(mesh):
    finer = Mesh(mesh.devices.reshape(mesh.shape["role"], 4, 4, 4), AXES)
    split = lambda rank: P(AXES, *([None] * (rank - 1)))
    return jax.shard_map(
        shards,
        mesh=finer,
        in_specs=(
            split(3), split(3), split(2), split(1), split(2), split(1), split(2), split(2), split(2),
            split(2), split(3), split(3), P(), P(), P(None, AXES, None),
        ),
        out_specs=(split(2), P()),
        check_vma=False,
    )
```

```python
import functools

import jax
import jax.numpy as jnp
from jax import lax
from jax.experimental import pallas as pl
from jax.experimental.pallas import tpu as pltpu
from jax.sharding import Mesh
from jax.sharding import PartitionSpec as P

RADIUS = 3
AXES = ("role", "dev_0", "dev_1", "dev_2")
SOFTEN = 0.01
EPSILON = 1e-06
HIGH = lax.Precision.HIGHEST
F32 = jnp.float32
BF16 = jnp.bfloat16
VMEM = pl.BlockSpec(memory_space=pltpu.VMEM)
SMEM = pl.BlockSpec(memory_space=pltpu.SMEM)
ANY = pl.BlockSpec(memory_space=pl.ANY)
HBM = pl.BlockSpec(memory_space=pltpu.HBM)
NT = (((1,), (1,)), ((), ()))
NN = (((1,), (0,)), ((), ()))
HIGHER = 128
ACROSS = 256
UNROLL = 16
MIB = 2**20


def dot(a, b, dims):
    return lax.dot_general(a, b, dims, preferred_element_type=F32)


def halves(value):
    top = value.astype(BF16)
    return top, (value - top.astype(F32)).astype(BF16)


def thirds(value):
    top, rest = value.astype(BF16), None
    rest = value - top.astype(F32)
    middle = rest.astype(BF16)
    return top, middle, (rest - middle.astype(F32)).astype(BF16)


def power(value):
    assert value & (value - 1) == 0
    return value.bit_length() - 1


def window_block(own, ids, clusters, width):
    owner = lax.shift_right_logical(ids, power(clusters))
    shift = (own - owner) & (width - 1)
    same = lax.shift_right_logical(owner, power(width)) == lax.shift_right_logical(own, power(width))
    return jnp.where(same, shift, shift + width - 1), ids & (clusters - 1)


def source_kernel(
    counts_ref, basis_hbm, inverse_hbm, maps_hbm, up_hbm, position_hbm, normal_hbm, area_hbm,
    payload_ref, group_ref, density_ref,
    basis_ref, inverse_ref, maps_ref, up_ref, position_ref, normal_ref, area_ref, sems, small_sems,
):
    clusters, panels = density_ref.shape
    coeffs = maps_ref.shape[1]
    copies = [
        [pltpu.make_async_copy(a.at[c], b.at[c], sems.at[k, c]) for c in range(clusters)]
        for k, (a, b) in enumerate(((inverse_hbm, inverse_ref), (maps_hbm, maps_ref), (up_hbm, up_ref)))
    ]
    small = [
        pltpu.make_async_copy(a, b, small_sems.at[k])
        for k, (a, b) in enumerate((
            (basis_hbm.at[basis_hbm.shape[0] - 1], basis_ref), (position_hbm, position_ref),
            (normal_hbm, normal_ref), (area_hbm, area_ref)))
    ]
    for copy in small[0:1] + copies[0] + copies[1] + copies[2] + small[1:]:
        copy.start()
    small[0].wait()
    lane = lax.broadcasted_iota(jnp.int32, (1, panels), 1)
    densities = []
    for c in range(clusters):
        copies[0][c].wait()
        current = basis_ref[c : c + 1].astype(BF16)
        density = dot(current, inverse_ref[c], NT)
        densities.append(jnp.where(lane < counts_ref[c], density, 0.0).astype(BF16))
    wide = jnp.concatenate([d.astype(F32) for d in densities], axis=0)
    density_ref[...] = wide
    total = jnp.zeros((1, coeffs), F32)
    tails = []
    for c in range(clusters):
        copies[1][c].wait()
        moments = dot(densities[c], maps_ref[c], NT).astype(BF16)
        tails.append(moments)
    for c in range(clusters):
        copies[2][c].wait()
        total += dot(tails[c], up_ref[c], NT)
        payload_ref[clusters, c : c + 1, 0:coeffs] = tails[c].astype(F32)
        payload_ref[clusters, c : c + 1, coeffs:panels] = jnp.full(
            (1, panels - coeffs), counts_ref[c].astype(F32)
        )
    for copy in small[1:]:
        copy.wait()
    lines = coeffs // 128
    row = lax.broadcasted_iota(jnp.int32, group_ref.shape, 0) & (lines - 1)
    spread = total[:, 0:128]
    for k in range(1, lines):
        spread = jnp.where(row == k, total[:, 128 * k : 128 * k + 128], spread)
    group_ref[...] = jnp.broadcast_to(spread, group_ref.shape)
    norm = jnp.zeros((clusters, panels), F32)
    across = jnp.zeros((clusters, panels), F32)
    rows = []
    scale = area_ref[...] * wide
    weights = []
    for a in range(3):
        top, rest = halves(position_ref[a])
        position = top.astype(F32) + rest.astype(F32)
        weighted = scale * normal_ref[a]
        norm += position * position
        across += position * weighted
        rows.append(position)
        weights.append(weighted)
    for k, value in enumerate(rows + [norm] + weights + [across]):
        for c in range(clusters):
            payload_ref[c, k : k + 1, :] = value[c : c + 1]


def sources(counts, basis, inverse, maps, up, positions, normals, areas, devices):
    count, clusters, panels = basis.shape
    coeffs = maps.shape[1]
    lines = devices * coeffs // 128
    return pl.pallas_call(
        source_kernel,
        in_specs=[SMEM] + [HBM] * 7,
        out_specs=[VMEM] * 3,
        out_shape=[
            jax.ShapeDtypeStruct((clusters + 1, 8, panels), F32),
            jax.ShapeDtypeStruct((lines, 128), F32),
            jax.ShapeDtypeStruct((clusters, panels), F32),
        ],
        scratch_shapes=[
            pltpu.VMEM((clusters, panels), F32),
            pltpu.VMEM(inverse.shape, BF16),
            pltpu.VMEM(maps.shape, BF16),
            pltpu.VMEM(up.shape, BF16),
            pltpu.VMEM(positions.shape, F32),
            pltpu.VMEM(normals.shape, F32),
            pltpu.VMEM(areas.shape, F32),
            pltpu.SemaphoreType.DMA((3, clusters)),
            pltpu.SemaphoreType.DMA((4,)),
        ],
        cost_estimate=pl.CostEstimate(flops=4 * 10**8, bytes_accessed=8 * MIB, transcendentals=0),
    )(counts, basis, inverse, maps, up, positions, normals, areas)


def near_tiles(
    own, blocks, first, lists_ref, nears_ref, counts_ref, tails, window, positions_of,
    tile_list, features, total, squares, ready_list, ready,
):
    clusters, slots = lists_ref.shape
    panels = window.shape[2]
    highs, wides = panels // HIGHER, panels // ACROSS
    width = 4
    begin, end = blocks

    def list_cluster(c, length):
        across = (counts_ref[c] + HIGHER - 1) // HIGHER

        def entry(at, block, local):
            used = (block >= begin) & (block < end)
            held = jnp.where(used, block - begin, 0)
            live = tails[held, local, 0].astype(jnp.int32)
            down = jnp.where(used, (live + ACROSS - 1) // ACROSS, 0)
            base = ((held * (clusters + 1) + local) << (8 + power(wides))) + c * highs
            for j in reversed(range(highs)):
                for i in reversed(range(wides)):
                    tile_list[at + i * across + j] = base + ((i << 8) + j)
            return at + down * across

        def list_slot(s, at):
            return entry(at, *window_block(own, lists_ref[c, s], clusters, width))

        if first:
            length = entry(length, jnp.int32(0), c)
        return lax.fori_loop(0, nears_ref[c], list_slot, length)

    ready_list()
    length = lax.fori_loop(0, clusters, list_cluster, jnp.int32(0))
    for extra in range(2 * UNROLL):
        tile_list[length + extra] = clusters * highs

    total[...] = jnp.zeros_like(total)

    for c in range(clusters):
        rows = positions_of(c)
        position, norm = rows[0:3], rows[3:4] + SOFTEN
        top, rest = [part.astype(F32) for part in halves(-2.0 * position)]
        a, b, d = [part.astype(F32) for part in thirds(norm)]
        one = jnp.ones((1, panels), F32)
        none = jnp.zeros((8, panels), F32)
        turned = jnp.concatenate(
            [top, one, none[0:4], rest, none[0:5], top, one, none[0:4], rest, none[0:5],
             none[0:3], one, none[0:4], a, b, d, none[0:5], jnp.zeros((80, panels), F32)], axis=0
        ).T
        features[c * panels : (c + 1) * panels, :] = turned.astype(BF16)
    features[pl.ds(clusters * panels, HIGHER), :] = jnp.where(
        lax.broadcasted_iota(jnp.int32, (HIGHER, 128), 1) == 40, 1.0, 0.0
    ).astype(BF16)

    def tile(s):
        lane = pl.multiple_of((s & (wides - 1)) * ACROSS, ACROSS)
        return window[lax.shift_right_logical(s, power(wides)), :, pl.ds(lane, ACROSS)]

    def square(at, u):
        spot = tile_list[at]
        top, middle, low = thirds(tile(lax.shift_right_logical(spot, 8)))
        right = jnp.concatenate(
            [top, top, middle, middle, low, jnp.ones((8, ACROSS), BF16), jnp.zeros((80, ACROSS), BF16)],
            axis=0,
        )
        left = features[pl.ds(pl.multiple_of((spot & 255) * HIGHER, HIGHER), HIGHER), :]
        squares[u] = dot(left, right, NN)

    def apply(at, u):
        inverse = lax.rsqrt(squares[u])
        field = (inverse * inverse * inverse).astype(BF16)
        top, rest = halves(tile(lax.shift_right_logical(tile_list[at], 8)))
        return dot(jnp.concatenate([top, rest], axis=0), field, NT)

    ready()
    for u in range(UNROLL):
        square(u, u)

    def step(g, carry):
        results = []
        for u in range(UNROLL):
            results.append((tile_list[g * UNROLL + u] & 255, apply(g * UNROLL + u, u)))
            square((g + 1) * UNROLL + u, u)
        for t, result in results:
            total[t] += result
        return carry

    lax.fori_loop(0, (length + UNROLL - 1) // UNROLL, step, 0)

    lines = []
    for c in range(clusters):
        parts = []
        for j in range(highs):
            r = total[c * highs + j]
            r = r[0:8] + r[8:16]
            x = positions_of(c)[0:3, j * HIGHER : (j + 1) * HIGHER]
            parts.append(jnp.sum(x * r[4:7], axis=0, keepdims=True) - r[7:8])
        lines.append(jnp.concatenate(parts, axis=1))
    return jnp.concatenate(lines, axis=0)


def near_scratch(clusters, slots, panels, blocks):
    highs, wides = panels // HIGHER, panels // ACROSS
    most = clusters * slots * highs * wides + 4 * UNROLL
    return [
        pltpu.SMEM((most,), jnp.int32),
        pltpu.VMEM((clusters * panels + HIGHER, 128), BF16),
        pltpu.VMEM((clusters * highs + 1, 16, HIGHER), F32),
        pltpu.VMEM((UNROLL, HIGHER, ACROSS), F32),
        pltpu.VMEM((blocks * (clusters + 1), 8, panels), F32),
        pltpu.SMEM((blocks, clusters, 128), F32),
    ]


def row_kernel(own_ref, lists_ref, nears_ref, counts_ref, a_ref, b_ref, c_ref, d_ref, out_ref,
               tile_list, features, total, squares, window, tails, sems):
    clusters = lists_ref.shape[0]
    blocks = (a_ref, b_ref, c_ref, d_ref)
    coeffs = window.shape[2] // 2
    copies = []
    for k, block in enumerate(blocks):
        copies.append(pltpu.make_async_copy(
            block, window.at[pl.ds(k * (clusters + 1), clusters + 1)], sems.at[0, k]))
        copies.append(pltpu.make_async_copy(
            block.at[clusters, :, pl.ds(coeffs, 128)], tails.at[k], sems.at[1, k]))
    first, then = copies[0:1] + copies[1::2], copies[2::2]

    def wait(group):
        for copy in group:
            copy.wait()

    for copy in copies[1::2] + copies[0::2]:
        copy.start()
    out_ref[...] = near_tiles(
        own_ref[0], (0, len(blocks)), True, lists_ref, nears_ref, counts_ref, tails, window,
        lambda c: window[c], tile_list, features, total, squares,
        lambda: wait(first), lambda: wait(then),
    )


def row_fields(own, lists, nears, counts, blocks):
    clusters, slots = lists.shape
    panels = blocks[0].shape[2]
    return pl.pallas_call(
        row_kernel,
        in_specs=[SMEM] * 4 + [ANY] * len(blocks),
        out_specs=VMEM,
        out_shape=jax.ShapeDtypeStruct((clusters, panels), F32),
        scratch_shapes=near_scratch(clusters, slots + 1, panels, len(blocks))
        + [pltpu.SemaphoreType.DMA((2, len(blocks)))],
        cost_estimate=pl.CostEstimate(flops=3 * 10**9, bytes_accessed=MIB, transcendentals=10**6),
    )(own, lists, nears, counts, *blocks)


def late_kernel(
    own_ref, lists_ref, nears_ref, counts_ref, leaf_ids_ref, leaf_kinds_ref, group_ids_ref,
    group_kinds_ref, groups_ref, density_ref, near_ref, basis_ref, far_hbm, up_hbm, maps_hbm,
    a_ref, b_ref, c_ref, d_ref, e_ref, f_ref, g_ref,
    image_ref, sums_ref,
    tile_list, features, total, squares, window, tails, sems,
    far_ref, up_ref, maps_ref, own_rows, moments, weight_sems,
):
    clusters, panels = density_ref.shape
    kinds, coeffs = far_ref.shape[1], far_ref.shape[2]
    row, others = (a_ref, b_ref, c_ref, d_ref), (e_ref, f_ref, g_ref)
    copies = []
    for k, block in enumerate(others):
        copies.append(pltpu.make_async_copy(
            block, window.at[pl.ds(k * (clusters + 1), clusters + 1)], sems.at[0, k]))
        copies.append(pltpu.make_async_copy(
            block.at[clusters, :, pl.ds(coeffs, 128)], tails.at[k], sems.at[1, k]))
    copies.append(pltpu.make_async_copy(a_ref, own_rows, weight_sems.at[3]))
    first, then = copies[1::2] + copies[-1:], copies[0:-1:2]

    def wait(group):
        for copy in group:
            copy.wait()

    for copy in first + then:
        copy.start()
    later = [
        pltpu.make_async_copy(block.at[clusters, :, pl.ds(0, coeffs)],
                              moments.at[pl.ds(k * clusters, clusters)], sems.at[2, k])
        for k, block in enumerate(row + others)
    ]
    later += [
        pltpu.make_async_copy(far_hbm, far_ref, weight_sems.at[0]),
        pltpu.make_async_copy(up_hbm, up_ref, weight_sems.at[1]),
        pltpu.make_async_copy(maps_hbm, maps_ref, weight_sems.at[2]),
    ]
    for copy in later:
        copy.start()
    own = own_ref[0]
    near = near_ref[...] + near_tiles(
        own, (4, 7), False, lists_ref, nears_ref, counts_ref, tails, window,
        lambda c: own_rows[c], tile_list, features, total, squares,
        lambda: wait(first), lambda: wait(then),
    )
    for copy in later:
        copy.wait()

    lines = coeffs // 128
    spots = groups_ref.shape[0]
    kind = lax.broadcasted_iota(jnp.int32, (kinds, 1), 0)
    spot = lax.broadcasted_iota(jnp.int32, (1, spots), 1)
    pick = jnp.zeros((kinds, spots), F32)
    for n in range(group_ids_ref.shape[1]):
        hit = (kind == group_kinds_ref[0, n]) & (
            lax.shift_right_logical(spot, power(lines)) == group_ids_ref[0, n])
        pick += jnp.where(hit, 1.0, 0.0)
    local = jnp.zeros((24, coeffs), F32)
    group_sum = jnp.concatenate(
        [
            lax.dot_general(jnp.where((spot & (lines - 1)) == k, pick, 0.0), groups_ref[...], NN,
                            precision=HIGH, preferred_element_type=F32)
            for k in range(lines)
        ],
        axis=1,
    )
    group_rows = jnp.concatenate([part.astype(F32) for part in thirds(group_sum)], axis=0)
    row24 = lax.broadcasted_iota(jnp.int32, (24, 1), 0) & (kinds - 1)
    for o in range(kinds):
        local += dot(jnp.where(row24 == o, group_rows, 0.0).astype(BF16), far_ref[1, o], NT)
    local = jnp.sum(local, axis=0, keepdims=True).astype(BF16)

    block, inside = window_block(own, leaf_ids_ref[...], clusters, 4)
    spots_of = block * clusters + inside
    spot = lax.broadcasted_iota(jnp.int32, (1, moments.shape[0]), 1)
    picks = [jnp.zeros((clusters, moments.shape[0]), F32) for _ in range(kinds)]
    for n in range(leaf_ids_ref.shape[1]):
        hit = jnp.where(spots_of[:, n : n + 1] == spot, 1.0, 0.0)
        for o in range(kinds):
            picks[o] += jnp.where(leaf_kinds_ref[:, n : n + 1] == o, hit, 0.0)
    leaf_sum = dot(
        jnp.concatenate(picks, axis=0).astype(BF16), moments[...].astype(BF16), NN
    )
    leaf = jnp.zeros((2 * clusters, coeffs), F32)
    for o in range(kinds):
        top, rest = halves(leaf_sum[o * clusters : (o + 1) * clusters])
        leaf += dot(jnp.concatenate([top, rest], axis=0), far_ref[0, o], NT)
    leaf = leaf[0:clusters] + leaf[clusters:]
    leaf += jnp.concatenate([dot(local, up_ref[c], NN) for c in range(clusters)], axis=0)
    leaf = leaf.astype(BF16)
    images = []
    lane = lax.broadcasted_iota(jnp.int32, (1, panels), 1)
    for c in range(clusters):
        far = dot(leaf[c : c + 1], maps_ref[c], NN)
        value = 0.5 * density_ref[c : c + 1] + near[c : c + 1] + far
        images.append(jnp.where(lane < counts_ref[c], value, 0.0))
    image = jnp.concatenate(images, axis=0)
    image_ref[...] = image
    lane = lax.broadcasted_iota(jnp.int32, (1, 128), 1)
    sums = jnp.zeros((1, 128), F32)
    for k in range(basis_ref.shape[0] + 1):
        other = basis_ref[k] if k < basis_ref.shape[0] else image
        value = jnp.sum(jnp.sum(image * other, axis=0, keepdims=True), axis=1, keepdims=True)
        sums += jnp.where(lane == k, value, 0.0)
    sums_ref[...] = jnp.broadcast_to(sums, sums_ref.shape)


def late_fields(own, lists, nears, counts, leaf_ids, leaf_kinds, group_ids, group_kinds, groups,
                density, near, basis, far, up, maps, window, devices):
    clusters, slots = lists.shape
    panels = density.shape[1]
    return pl.pallas_call(
        late_kernel,
        in_specs=[SMEM] * 4 + [VMEM] * 2 + [SMEM] * 2 + [VMEM] * 4 + [HBM] * 3 + [ANY] * 7,
        out_specs=[VMEM, VMEM],
        out_shape=[
            jax.ShapeDtypeStruct(density.shape, F32),
            jax.ShapeDtypeStruct((devices, 128), F32),
        ],
        scratch_shapes=near_scratch(clusters, slots + 1, panels, 3)
        + [
            pltpu.SemaphoreType.DMA((3, 7)),
            pltpu.VMEM(far.shape, BF16),
            pltpu.VMEM(up.shape, BF16),
            pltpu.VMEM(maps.shape, BF16),
            pltpu.VMEM((clusters + 1, 8, panels), F32),
            pltpu.VMEM((7 * clusters, maps.shape[1]), F32),
            pltpu.SemaphoreType.DMA((4,)),
        ],
        cost_estimate=pl.CostEstimate(flops=3 * 10**9, bytes_accessed=MIB, transcendentals=10**6),
    )(own, lists, nears, counts, leaf_ids, leaf_kinds, group_ids, group_kinds, groups, density,
      near, basis, far, up, maps, *window)


def close_kernel(rows, sums_ref, image_ref, basis_ref, next_ref, column_ref):
    count = basis_ref.shape[0]
    means = jnp.sum(sums_ref[...], axis=0, keepdims=True) * (1.0 / rows)
    lane = lax.broadcasted_iota(jnp.int32, (1, 128), 1)
    coeffs = jnp.where(lane < count, means, 0.0)
    square = jnp.sum(jnp.where(lane == count, means, 0.0), axis=1, keepdims=True)
    energy = square - jnp.sum(coeffs * coeffs, axis=1, keepdims=True)
    height = jnp.sqrt(energy + EPSILON)
    remainder = image_ref[...]
    for k in range(count):
        remainder = remainder - coeffs[:, k : k + 1] * basis_ref[k]
        column_ref[k] = means[0, k]
    column_ref[count] = height[0, 0]
    next_ref[...] = remainder / height


def close(sums, image, basis, rows):
    return pl.pallas_call(
        functools.partial(close_kernel, rows),
        in_specs=[VMEM] * 3,
        out_specs=[VMEM, SMEM],
        out_shape=[
            jax.ShapeDtypeStruct(image.shape, F32),
            jax.ShapeDtypeStruct((basis.shape[0] + 1,), F32),
        ],
    )(sums, image, basis)


def row_routes(rows, width):
    spot = lambda r, y: (r % rows) * width + y
    turns = {1: (1, -1, -1, -1), 2: (1, 1, -1, -1), 3: (1, 1, 1, -1)}
    return {
        k: [(spot(r, y), spot(r + turns[k][y], y)) for r in range(rows) for y in range(width)]
        for k in turns
    }


def shards(
    positions, normals, panel_areas, panel_counts, near_lists, near_counts, leaf_lists, leaf_kinds,
    group_lists, group_kinds, block_inverse, moment_maps, up_operators, far_operators, krylov_basis,
):
    clusters, _, panels = positions.shape
    coeffs = moment_maps.shape[1]
    devices = lax.axis_size(AXES)
    width = lax.axis_size(AXES[-1])
    own = jnp.full((1,), lax.axis_index(AXES), jnp.int32)
    payload, group, density = sources(
        panel_counts, krylov_basis, block_inverse, moment_maps, up_operators,
        positions.transpose(1, 0, 2), normals.transpose(1, 0, 2), panel_areas, devices,
    )
    row = [payload] + [
        lax.ppermute(payload, AXES[-1], [(y, (y + k) % width) for y in range(width)])
        for k in range(1, width)
    ]
    routes = row_routes(devices // width, width)
    window = row + [lax.ppermute(row[k], AXES, routes[k]) for k in range(1, width)]
    groups = lax.all_to_all(group, AXES, 0, 0, tiled=True)
    near = row_fields(own, near_lists, near_counts, panel_counts, row)
    image, sums = late_fields(
        own, near_lists, near_counts, panel_counts, leaf_lists, leaf_kinds, group_lists, group_kinds,
        groups, density, near, krylov_basis, far_operators, up_operators, moment_maps, window, devices,
    )
    sums = lax.all_to_all(sums, AXES, 0, 0, tiled=True)
    return close(sums, image, krylov_basis, devices * clusters * panels)


def solution(mesh):
    finer = Mesh(mesh.devices.reshape(mesh.shape["role"], 4, 4, 4), AXES)
    split = lambda rank: P(AXES, *([None] * (rank - 1)))
    return jax.shard_map(
        shards,
        mesh=finer,
        in_specs=(
            split(3), split(3), split(2), split(1), split(2), split(1), split(2), split(2), split(2),
            split(2), split(3), split(3), P(), P(), P(None, AXES, None),
        ),
        out_specs=(split(2), P()),
        check_vma=False,
    )
```

```python
import functools

import jax
import jax.numpy as jnp
from jax import lax
from jax.experimental import pallas as pl
from jax.experimental.pallas import tpu as pltpu
from jax.sharding import Mesh
from jax.sharding import PartitionSpec as P

RADIUS = 3
AXES = ("role", "dev_0", "dev_1", "dev_2")
SOFTEN = 0.01
EPSILON = 1e-06
HIGH = lax.Precision.HIGHEST
F32 = jnp.float32
BF16 = jnp.bfloat16
VMEM = pl.BlockSpec(memory_space=pltpu.VMEM)
SMEM = pl.BlockSpec(memory_space=pltpu.SMEM)
ANY = pl.BlockSpec(memory_space=pl.ANY)
HBM = pl.BlockSpec(memory_space=pltpu.HBM)
NT = (((1,), (1,)), ((), ()))
NN = (((1,), (0,)), ((), ()))
HIGHER = 128
ACROSS = 256
UNROLL = 16
MIB = 2**20
PAIRS = 4
DEAD = 1 << 24


def dot(a, b, dims):
    return lax.dot_general(a, b, dims, preferred_element_type=F32)


def halves(value):
    top = value.astype(BF16)
    return top, (value - top.astype(F32)).astype(BF16)


def thirds(value):
    top, rest = value.astype(BF16), None
    rest = value - top.astype(F32)
    middle = rest.astype(BF16)
    return top, middle, (rest - middle.astype(F32)).astype(BF16)


def power(value):
    assert value & (value - 1) == 0
    return value.bit_length() - 1


def window_block(own, ids, clusters, width):
    owner = lax.shift_right_logical(ids, power(clusters))
    shift = (own - owner) & (width - 1)
    same = lax.shift_right_logical(owner, power(width)) == lax.shift_right_logical(own, power(width))
    return jnp.where(same, shift, shift + width - 1), ids & (clusters - 1)


def list_pairs(own, lists_ref, nears_ref, row_ref, off_ref, width):
    clusters = lists_ref.shape[0]

    def list_cluster(c, lengths):
        row, off = lengths
        row_ref[row] = (c << 8) + c

        def list_slot(s, lengths):
            row, off = lengths
            block, inside = window_block(own, lists_ref[c, s], clusters, width)
            pair = (block << 16) + (inside << 8) + c
            near = jnp.where(block < width, 1, 0)
            row_ref[row] = pair
            off_ref[off] = pair - (width << 16)
            return row + near, off + 1 - near

        return lax.fori_loop(0, nears_ref[c], list_slot, (row + 1, off))

    row, off = lax.fori_loop(0, clusters, list_cluster, (jnp.int32(0), jnp.int32(0)))
    for ref, length in ((row_ref, row), (off_ref, off)):
        for k in range(PAIRS):
            ref[length + k] = DEAD
        ref[ref.shape[0] - 1] = length


def source_kernel(
    own_ref, lists_ref, nears_ref, counts_ref,
    basis_hbm, inverse_hbm, maps_hbm, up_hbm, position_hbm, normal_hbm, area_hbm,
    payload_ref, group_ref, density_ref, features_ref, row_ref, off_ref,
    basis_ref, inverse_ref, maps_ref, up_ref, position_ref, normal_ref, area_ref, sems, small_sems,
):
    clusters, panels = density_ref.shape
    coeffs = maps_ref.shape[1]
    copies = [
        [pltpu.make_async_copy(a.at[c], b.at[c], sems.at[k, c]) for c in range(clusters)]
        for k, (a, b) in enumerate(((inverse_hbm, inverse_ref), (maps_hbm, maps_ref), (up_hbm, up_ref)))
    ]
    small = [
        pltpu.make_async_copy(a, b, small_sems.at[k])
        for k, (a, b) in enumerate((
            (position_hbm, position_ref), (basis_hbm.at[basis_hbm.shape[0] - 1], basis_ref),
            (normal_hbm, normal_ref), (area_hbm, area_ref)))
    ]
    for copy in small[0:2] + copies[0] + copies[1] + copies[2] + small[2:]:
        copy.start()
    list_pairs(own_ref[0], lists_ref, nears_ref, row_ref, off_ref, 4)
    small[0].wait()
    norm = jnp.zeros((clusters, panels), F32)
    positions = []
    for a in range(3):
        top, rest = halves(position_ref[a])
        positions.append((top.astype(F32), rest.astype(F32)))
        norm += (positions[a][0] + positions[a][1]) * (positions[a][0] + positions[a][1])
    softened = [part.astype(F32) for part in thirds(norm + SOFTEN)]
    one = jnp.ones((1, panels), F32)
    none = jnp.zeros((8, panels), F32)
    for c in range(clusters):
        at = slice(c, c + 1)
        top = [-2.0 * positions[a][0][at] for a in range(3)]
        rest = [-2.0 * positions[a][1][at] for a in range(3)]
        turned = jnp.concatenate(
            top + [one, none[0:4]] + rest + [none[0:5]] + top + [one, none[0:4]] + rest + [none[0:5]]
            + [none[0:3], one, none[0:4]] + [part[at] for part in softened]
            + [none[0:5], jnp.zeros((80, panels), F32)], axis=0
        ).T
        features_ref[c * panels : (c + 1) * panels, :] = turned.astype(BF16)
    features_ref[clusters * panels :, :] = jnp.where(
        lax.broadcasted_iota(jnp.int32, (HIGHER, 128), 1) == 40, 1.0, 0.0
    ).astype(BF16)
    small[1].wait()
    lane = lax.broadcasted_iota(jnp.int32, (1, panels), 1)
    densities = []
    for c in range(clusters):
        if c % 4 == 0:
            for copy in copies[0][c : c + 4]:
                copy.wait()
        current = basis_ref[c : c + 1].astype(BF16)
        density = dot(current, inverse_ref[c], NT)
        densities.append(jnp.where(lane < counts_ref[c], density, 0.0).astype(BF16))
    for copy in small[2:]:
        copy.wait()
    wide = jnp.concatenate([d.astype(F32) for d in densities], axis=0)
    density_ref[...] = wide
    scale = area_ref[...] * wide
    weights = [scale * normal_ref[a] for a in range(3)]
    whole = [top + rest for top, rest in positions]
    crossed = sum(whole[a] * weights[a] for a in range(3))
    for k, value in enumerate(whole + [norm] + weights + [crossed]):
        for c in range(clusters):
            payload_ref[c, k : k + 1, :] = value[c : c + 1]
    for copy in copies[1]:
        copy.wait()
    tails = [dot(densities[c], maps_ref[c], NT).astype(BF16) for c in range(clusters)]
    for copy in copies[2]:
        copy.wait()
    total = jnp.zeros((1, coeffs), F32)
    for c in range(clusters):
        total += dot(tails[c], up_ref[c], NT)
        payload_ref[clusters, c : c + 1, 0:coeffs] = tails[c].astype(F32)
        payload_ref[clusters, c : c + 1, coeffs:panels] = jnp.full(
            (1, panels - coeffs), counts_ref[c].astype(F32)
        )
    lines = coeffs // 128
    row = lax.broadcasted_iota(jnp.int32, group_ref.shape, 0) & (lines - 1)
    spread = total[:, 0:128]
    for k in range(1, lines):
        spread = jnp.where(row == k, total[:, 128 * k : 128 * k + 128], spread)
    group_ref[...] = jnp.broadcast_to(spread, group_ref.shape)


def sources(own, lists, nears, counts, basis, inverse, maps, up, positions, normals, areas, devices):
    count, clusters, panels = basis.shape
    coeffs = maps.shape[1]
    lines = devices * coeffs // 128
    pairs = clusters * (lists.shape[1] + 1) + PAIRS + 1
    return pl.pallas_call(
        source_kernel,
        in_specs=[SMEM] * 4 + [HBM] * 7,
        out_specs=[VMEM] * 4 + [SMEM] * 2,
        out_shape=[
            jax.ShapeDtypeStruct((clusters + 1, 8, panels), F32),
            jax.ShapeDtypeStruct((lines, 128), F32),
            jax.ShapeDtypeStruct((clusters, panels), F32),
            jax.ShapeDtypeStruct((clusters * panels + HIGHER, 128), BF16),
            jax.ShapeDtypeStruct((pairs,), jnp.int32),
            jax.ShapeDtypeStruct((pairs,), jnp.int32),
        ],
        scratch_shapes=[
            pltpu.VMEM((clusters, panels), F32),
            pltpu.VMEM(inverse.shape, BF16),
            pltpu.VMEM(maps.shape, BF16),
            pltpu.VMEM(up.shape, BF16),
            pltpu.VMEM(positions.shape, F32),
            pltpu.VMEM(normals.shape, F32),
            pltpu.VMEM(areas.shape, F32),
            pltpu.SemaphoreType.DMA((3, clusters)),
            pltpu.SemaphoreType.DMA((4,)),
        ],
        cost_estimate=pl.CostEstimate(flops=4 * 10**8, bytes_accessed=8 * MIB, transcendentals=0),
    )(own, lists, nears, counts, basis, inverse, maps, up, positions, normals, areas)


def near_tiles(
    pairs_ref, counts_ref, tails, window, position_ref,
    tile_list, features, total, squares, ready_list, ready,
):
    clusters = counts_ref.shape[0]
    panels = window.shape[2]
    highs, wides = panels // HIGHER, panels // ACROSS
    shift = lambda value, size: lax.shift_right_logical(value, power(size))
    ready_list()

    def list_some(g, length):
        for k in range(PAIRS):
            pair = pairs_ref[g * PAIRS + k]
            used = pair < DEAD
            pair = jnp.where(used, pair, 0)
            c, local, block = pair & 255, shift(pair, 256) & 255, shift(pair, 65536)
            live = tails[block, local, 0].astype(jnp.int32)
            down = jnp.where(used, shift(live + (ACROSS - 1), ACROSS), 0)
            across = shift(counts_ref[c] + (HIGHER - 1), HIGHER)
            base = ((block * (clusters + 1) + local) << (8 + power(wides))) + c * highs
            for j in reversed(range(highs)):
                for i in reversed(range(wides)):
                    tile_list[length + i * across + j] = base + ((i << 8) + j)
            length = length + down * across
        return length

    pairs = pairs_ref[pairs_ref.shape[0] - 1]
    length = lax.fori_loop(0, shift(pairs + (PAIRS - 1), PAIRS), list_some, jnp.int32(0))
    for extra in range(2 * UNROLL):
        tile_list[length + extra] = clusters * highs

    total[...] = jnp.zeros_like(total)

    def tile(s):
        lane = pl.multiple_of((s & (wides - 1)) * ACROSS, ACROSS)
        return window[lax.shift_right_logical(s, power(wides)), :, pl.ds(lane, ACROSS)]

    def square(at, u):
        spot = tile_list[at]
        top, middle, low = thirds(tile(lax.shift_right_logical(spot, 8)))
        right = jnp.concatenate(
            [top, top, middle, middle, low, jnp.ones((8, ACROSS), BF16), jnp.zeros((80, ACROSS), BF16)],
            axis=0,
        )
        left = features[pl.ds(pl.multiple_of((spot & 255) * HIGHER, HIGHER), HIGHER), :]
        squares[u] = dot(left, right, NN)

    def apply(at, u):
        inverse = lax.rsqrt(squares[u])
        field = (inverse * inverse * inverse).astype(BF16)
        top, rest = halves(tile(lax.shift_right_logical(tile_list[at], 8)))
        return dot(jnp.concatenate([top, rest], axis=0), field, NT)

    ready()
    for u in range(UNROLL):
        square(u, u)

    def step(g, carry):
        results = []
        for u in range(UNROLL):
            results.append((tile_list[g * UNROLL + u] & 255, apply(g * UNROLL + u, u)))
            square((g + 1) * UNROLL + u, u)
        for t, result in results:
            total[t] += result
        return carry

    lax.fori_loop(0, shift(length + (UNROLL - 1), UNROLL), step, 0)

    lines = []
    for c in range(clusters):
        parts = []
        for j in range(highs):
            r = total[c * highs + j]
            r = r[0:8] + r[8:16]
            x = position_ref[c, 0:3, j * HIGHER : (j + 1) * HIGHER]
            parts.append(jnp.sum(x * r[4:7], axis=0, keepdims=True) - r[7:8])
        lines.append(jnp.concatenate(parts, axis=1))
    return jnp.concatenate(lines, axis=0)


def near_scratch(clusters, slots, panels, blocks):
    highs, wides = panels // HIGHER, panels // ACROSS
    most = clusters * slots * highs * wides + 4 * UNROLL
    return [
        pltpu.SMEM((most,), jnp.int32),
        pltpu.VMEM((clusters * panels + HIGHER, 128), BF16),
        pltpu.SemaphoreType.DMA,
        pltpu.VMEM((clusters * highs + 1, 16, HIGHER), F32),
        pltpu.VMEM((UNROLL, HIGHER, ACROSS), F32),
        pltpu.VMEM((blocks * (clusters + 1), 8, panels), F32),
        pltpu.SMEM((blocks, clusters, 128), F32),
    ]


def row_kernel(pairs_ref, counts_ref, features_hbm, a_ref, b_ref, c_ref, d_ref, out_ref,
               tile_list, features, feature_sem, total, squares, window, tails, sems):
    clusters = counts_ref.shape[0]
    blocks = (a_ref, b_ref, c_ref, d_ref)
    coeffs = window.shape[2] // 2
    copies = []
    for k, block in enumerate(blocks):
        copies.append(pltpu.make_async_copy(
            block, window.at[pl.ds(k * (clusters + 1), clusters + 1)], sems.at[0, k]))
        copies.append(pltpu.make_async_copy(
            block.at[clusters, :, pl.ds(coeffs, 128)], tails.at[k], sems.at[1, k]))
    first, then = copies[1::2], copies[0::2]
    then.append(pltpu.make_async_copy(features_hbm, features, feature_sem))

    def wait(group):
        for copy in group:
            copy.wait()

    for copy in first + then:
        copy.start()
    out_ref[...] = near_tiles(
        pairs_ref, counts_ref, tails, window, window, tile_list, features, total, squares,
        lambda: wait(first), lambda: wait(then),
    )


def row_fields(pairs, counts, features, slots, blocks):
    clusters = counts.shape[0]
    panels = blocks[0].shape[2]
    return pl.pallas_call(
        row_kernel,
        in_specs=[SMEM] * 2 + [ANY] * (1 + len(blocks)),
        out_specs=VMEM,
        out_shape=jax.ShapeDtypeStruct((clusters, panels), F32),
        scratch_shapes=near_scratch(clusters, slots + 1, panels, len(blocks))
        + [pltpu.SemaphoreType.DMA((2, len(blocks)))],
        cost_estimate=pl.CostEstimate(flops=3 * 10**9, bytes_accessed=MIB, transcendentals=10**6),
    )(pairs, counts, features, *blocks)


def late_kernel(
    own_ref, pairs_ref, counts_ref, leaf_ids_ref, leaf_kinds_ref, group_ids_ref,
    group_kinds_ref, groups_ref, density_ref, near_ref, basis_ref, features_hbm, far_hbm, up_hbm, maps_hbm,
    a_ref, b_ref, c_ref, d_ref, e_ref, f_ref, g_ref,
    image_ref, sums_ref,
    tile_list, features, feature_sem, total, squares, window, tails, sems,
    far_ref, up_ref, maps_ref, own_rows, moments, weight_sems,
):
    clusters, panels = density_ref.shape
    kinds, coeffs = far_ref.shape[1], far_ref.shape[2]
    row, others = (a_ref, b_ref, c_ref, d_ref), (e_ref, f_ref, g_ref)
    copies = []
    for k, block in enumerate(others):
        copies.append(pltpu.make_async_copy(
            block, window.at[pl.ds(k * (clusters + 1), clusters + 1)], sems.at[0, k]))
        copies.append(pltpu.make_async_copy(
            block.at[clusters, :, pl.ds(coeffs, 128)], tails.at[k], sems.at[1, k]))
    copies.append(pltpu.make_async_copy(a_ref, own_rows, weight_sems.at[3]))
    first, then = copies[1::2], copies[0:-1:2] + copies[-1:]
    then.append(pltpu.make_async_copy(features_hbm, features, feature_sem))

    def wait(group):
        for copy in group:
            copy.wait()

    for copy in first + then:
        copy.start()
    later = [
        pltpu.make_async_copy(block.at[clusters, :, pl.ds(0, coeffs)],
                              moments.at[pl.ds(k * clusters, clusters)], sems.at[2, k])
        for k, block in enumerate(row + others)
    ]
    later += [
        pltpu.make_async_copy(far_hbm, far_ref, weight_sems.at[0]),
        pltpu.make_async_copy(up_hbm, up_ref, weight_sems.at[1]),
        pltpu.make_async_copy(maps_hbm, maps_ref, weight_sems.at[2]),
    ]
    for copy in later:
        copy.start()
    own = own_ref[0]
    near = near_ref[...] + near_tiles(
        pairs_ref, counts_ref, tails, window, own_rows, tile_list, features, total, squares,
        lambda: wait(first), lambda: wait(then),
    )
    for copy in later:
        copy.wait()

    lines = coeffs // 128
    spots = groups_ref.shape[0]
    kind = lax.broadcasted_iota(jnp.int32, (kinds, 1), 0)
    spot = lax.broadcasted_iota(jnp.int32, (1, spots), 1)
    pick = jnp.zeros((kinds, spots), F32)
    for n in range(group_ids_ref.shape[1]):
        hit = (kind == group_kinds_ref[0, n]) & (
            lax.shift_right_logical(spot, power(lines)) == group_ids_ref[0, n])
        pick += jnp.where(hit, 1.0, 0.0)
    local = jnp.zeros((24, coeffs), F32)
    group_sum = jnp.concatenate(
        [
            lax.dot_general(jnp.where((spot & (lines - 1)) == k, pick, 0.0), groups_ref[...], NN,
                            precision=HIGH, preferred_element_type=F32)
            for k in range(lines)
        ],
        axis=1,
    )
    group_rows = jnp.concatenate([part.astype(F32) for part in thirds(group_sum)], axis=0)
    row24 = lax.broadcasted_iota(jnp.int32, (24, 1), 0) & (kinds - 1)
    for o in range(kinds):
        local += dot(jnp.where(row24 == o, group_rows, 0.0).astype(BF16), far_ref[1, o], NT)
    local = jnp.sum(local, axis=0, keepdims=True).astype(BF16)

    block, inside = window_block(own, leaf_ids_ref[...], clusters, 4)
    spots_of = block * clusters + inside
    spot = lax.broadcasted_iota(jnp.int32, (1, moments.shape[0]), 1)
    picks = [jnp.zeros((clusters, moments.shape[0]), F32) for _ in range(kinds)]
    for n in range(leaf_ids_ref.shape[1]):
        hit = jnp.where(spots_of[:, n : n + 1] == spot, 1.0, 0.0)
        for o in range(kinds):
            picks[o] += jnp.where(leaf_kinds_ref[:, n : n + 1] == o, hit, 0.0)
    leaf_sum = dot(
        jnp.concatenate(picks, axis=0).astype(BF16), moments[...].astype(BF16), NN
    )
    leaf = jnp.zeros((2 * clusters, coeffs), F32)
    for o in range(kinds):
        top, rest = halves(leaf_sum[o * clusters : (o + 1) * clusters])
        leaf += dot(jnp.concatenate([top, rest], axis=0), far_ref[0, o], NT)
    leaf = leaf[0:clusters] + leaf[clusters:]
    leaf += jnp.concatenate([dot(local, up_ref[c], NN) for c in range(clusters)], axis=0)
    leaf = leaf.astype(BF16)
    images = []
    lane = lax.broadcasted_iota(jnp.int32, (1, panels), 1)
    for c in range(clusters):
        far = dot(leaf[c : c + 1], maps_ref[c], NN)
        value = 0.5 * density_ref[c : c + 1] + near[c : c + 1] + far
        images.append(jnp.where(lane < counts_ref[c], value, 0.0))
    image = jnp.concatenate(images, axis=0)
    image_ref[...] = image
    lane = lax.broadcasted_iota(jnp.int32, (1, 128), 1)
    sums = jnp.zeros((1, 128), F32)
    for k in range(basis_ref.shape[0] + 1):
        other = basis_ref[k] if k < basis_ref.shape[0] else image
        value = jnp.sum(jnp.sum(image * other, axis=0, keepdims=True), axis=1, keepdims=True)
        sums += jnp.where(lane == k, value, 0.0)
    sums_ref[...] = jnp.broadcast_to(sums, sums_ref.shape)


def late_fields(own, pairs, counts, slots, leaf_ids, leaf_kinds, group_ids, group_kinds, groups,
                density, near, basis, features, far, up, maps, window, devices):
    clusters, panels = density.shape
    return pl.pallas_call(
        late_kernel,
        in_specs=[SMEM] * 3 + [VMEM] * 2 + [SMEM] * 2 + [VMEM] * 4 + [ANY] + [HBM] * 3 + [ANY] * 7,
        out_specs=[VMEM, VMEM],
        out_shape=[
            jax.ShapeDtypeStruct(density.shape, F32),
            jax.ShapeDtypeStruct((devices, 128), F32),
        ],
        scratch_shapes=near_scratch(clusters, slots + 1, panels, 3)
        + [
            pltpu.SemaphoreType.DMA((3, 7)),
            pltpu.VMEM(far.shape, BF16),
            pltpu.VMEM(up.shape, BF16),
            pltpu.VMEM(maps.shape, BF16),
            pltpu.VMEM((clusters + 1, 8, panels), F32),
            pltpu.VMEM((7 * clusters, maps.shape[1]), F32),
            pltpu.SemaphoreType.DMA((4,)),
        ],
        cost_estimate=pl.CostEstimate(flops=3 * 10**9, bytes_accessed=MIB, transcendentals=10**6),
    )(own, pairs, counts, leaf_ids, leaf_kinds, group_ids, group_kinds, groups, density,
      near, basis, features, far, up, maps, *window)


def close_kernel(rows, sums_ref, image_ref, basis_ref, next_ref, column_ref):
    count = basis_ref.shape[0]
    means = jnp.sum(sums_ref[...], axis=0, keepdims=True) * (1.0 / rows)
    lane = lax.broadcasted_iota(jnp.int32, (1, 128), 1)
    coeffs = jnp.where(lane < count, means, 0.0)
    square = jnp.sum(jnp.where(lane == count, means, 0.0), axis=1, keepdims=True)
    energy = square - jnp.sum(coeffs * coeffs, axis=1, keepdims=True)
    height = jnp.sqrt(energy + EPSILON)
    remainder = image_ref[...]
    for k in range(count):
        remainder = remainder - coeffs[:, k : k + 1] * basis_ref[k]
        column_ref[k] = means[0, k]
    column_ref[count] = height[0, 0]
    next_ref[...] = remainder / height


def close(sums, image, basis, rows):
    return pl.pallas_call(
        functools.partial(close_kernel, rows),
        in_specs=[VMEM] * 3,
        out_specs=[VMEM, SMEM],
        out_shape=[
            jax.ShapeDtypeStruct(image.shape, F32),
            jax.ShapeDtypeStruct((basis.shape[0] + 1,), F32),
        ],
        compiler_params=pltpu.CompilerParams(vmem_limit_bytes=2 * MIB),
    )(sums, image, basis)


def row_routes(rows, width):
    spot = lambda r, y: (r % rows) * width + y
    turns = {1: (1, -1, -1, -1), 2: (1, 1, -1, -1), 3: (1, 1, 1, -1)}
    return {
        k: [(spot(r, y), spot(r + turns[k][y], y)) for r in range(rows) for y in range(width)]
        for k in turns
    }


def shards(
    positions, normals, panel_areas, panel_counts, near_lists, near_counts, leaf_lists, leaf_kinds,
    group_lists, group_kinds, block_inverse, moment_maps, up_operators, far_operators, krylov_basis,
):
    clusters, _, panels = positions.shape
    coeffs = moment_maps.shape[1]
    devices = lax.axis_size(AXES)
    width = lax.axis_size(AXES[-1])
    own = jnp.full((1,), lax.axis_index(AXES), jnp.int32)
    payload, group, density, features, row_pairs, off_pairs = sources(
        own, near_lists, near_counts, panel_counts, krylov_basis, block_inverse, moment_maps, up_operators,
        positions.transpose(1, 0, 2), normals.transpose(1, 0, 2), panel_areas, devices,
    )
    row = [payload] + [
        lax.ppermute(payload, AXES[-1], [(y, (y + k) % width) for y in range(width)])
        for k in range(1, width)
    ]
    routes = row_routes(devices // width, width)
    window = row + [lax.ppermute(row[k], AXES, routes[k]) for k in range(1, width)]
    groups = lax.all_to_all(group, AXES, 0, 0, tiled=True)
    slots = near_lists.shape[1]
    near = row_fields(row_pairs, panel_counts, features, slots, row)
    image, sums = late_fields(
        own, off_pairs, panel_counts, slots, leaf_lists, leaf_kinds, group_lists, group_kinds,
        groups, density, near, krylov_basis, features, far_operators, up_operators, moment_maps, window, devices,
    )
    sums = lax.all_to_all(sums, AXES, 0, 0, tiled=True)
    return close(sums, image, krylov_basis, devices * clusters * panels)


def solution(mesh):
    finer = Mesh(mesh.devices.reshape(mesh.shape["role"], 4, 4, 4), AXES)
    split = lambda rank: P(AXES, *([None] * (rank - 1)))
    return jax.shard_map(
        shards,
        mesh=finer,
        in_specs=(
            split(3), split(3), split(2), split(1), split(2), split(1), split(2), split(2), split(2),
            split(2), split(3), split(3), P(), P(), P(None, AXES, None),
        ),
        out_specs=(split(2), P()),
        check_vma=False,
    )
```

```python
import functools

import jax
import jax.numpy as jnp
from jax import lax
from jax.experimental import pallas as pl
from jax.experimental.pallas import tpu as pltpu
from jax.sharding import Mesh
from jax.sharding import PartitionSpec as P

RADIUS = 3
AXES = ("role", "dev_0", "dev_1", "dev_2")
SOFTEN = 0.01
EPSILON = 1e-06
HIGH = lax.Precision.HIGHEST
F32 = jnp.float32
BF16 = jnp.bfloat16
VMEM = pl.BlockSpec(memory_space=pltpu.VMEM)
SMEM = pl.BlockSpec(memory_space=pltpu.SMEM)
ANY = pl.BlockSpec(memory_space=pl.ANY)
HBM = pl.BlockSpec(memory_space=pltpu.HBM)
NT = (((1,), (1,)), ((), ()))
NN = (((1,), (0,)), ((), ()))
HIGHER = 128
ACROSS = 256
UNROLL = 16
MIB = 2**20
PAIRS = 4
DEAD = 1 << 24


def dot(a, b, dims):
    return lax.dot_general(a, b, dims, preferred_element_type=F32)


def halves(value):
    top = value.astype(BF16)
    return top, (value - top.astype(F32)).astype(BF16)


def thirds(value):
    top, rest = value.astype(BF16), None
    rest = value - top.astype(F32)
    middle = rest.astype(BF16)
    return top, middle, (rest - middle.astype(F32)).astype(BF16)


def power(value):
    assert value & (value - 1) == 0
    return value.bit_length() - 1


def window_block(own, ids, clusters, width):
    owner = lax.shift_right_logical(ids, power(clusters))
    shift = (own - owner) & (width - 1)
    same = lax.shift_right_logical(owner, power(width)) == lax.shift_right_logical(own, power(width))
    return jnp.where(same, shift, shift + width - 1), ids & (clusters - 1)


def list_pairs(own, lists_ref, nears_ref, row_ref, off_ref, width):
    clusters = lists_ref.shape[0]

    def list_cluster(c, lengths):
        row, off = lengths
        row_ref[row] = (c << 8) + c

        def list_slot(s, lengths):
            row, off = lengths
            block, inside = window_block(own, lists_ref[c, s], clusters, width)
            pair = (block << 16) + (inside << 8) + c
            near = jnp.where(block < width, 1, 0)
            row_ref[row] = pair
            off_ref[off] = pair - (width << 16)
            return row + near, off + 1 - near

        return lax.fori_loop(0, nears_ref[c], list_slot, (row + 1, off))

    row, off = lax.fori_loop(0, clusters, list_cluster, (jnp.int32(0), jnp.int32(0)))
    for ref, length in ((row_ref, row), (off_ref, off)):
        for k in range(PAIRS):
            ref[length + k] = DEAD
        ref[ref.shape[0] - 1] = length


def source_kernel(
    own_ref, lists_ref, nears_ref, counts_ref,
    basis_hbm, inverse_hbm, maps_hbm, up_hbm, position_hbm, normal_hbm, area_hbm,
    payload_ref, group_ref, density_ref, features_hbm, row_ref, off_ref,
    basis_ref, inverse_ref, maps_ref, up_ref, position_ref, normal_ref, area_ref,
    features_ref, sems, small_sems,
):
    clusters, panels = density_ref.shape
    coeffs = maps_ref.shape[1]
    copies = [
        [pltpu.make_async_copy(a.at[c], b.at[c], sems.at[k, c]) for c in range(clusters)]
        for k, (a, b) in enumerate(((inverse_hbm, inverse_ref), (maps_hbm, maps_ref), (up_hbm, up_ref)))
    ]
    small = [
        pltpu.make_async_copy(a, b, small_sems.at[k])
        for k, (a, b) in enumerate((
            (position_hbm, position_ref), (basis_hbm.at[basis_hbm.shape[0] - 1], basis_ref),
            (normal_hbm, normal_ref), (area_hbm, area_ref)))
    ]
    for copy in small[0:2] + copies[0] + small[2:]:
        copy.start()
    list_pairs(own_ref[0], lists_ref, nears_ref, row_ref, off_ref, 4)
    small[0].wait()
    norm = jnp.zeros((clusters, panels), F32)
    positions = []
    for a in range(3):
        top, rest = halves(position_ref[a])
        positions.append((top.astype(F32), rest.astype(F32)))
        norm += (positions[a][0] + positions[a][1]) * (positions[a][0] + positions[a][1])
    softened = [part.astype(F32) for part in thirds(norm + SOFTEN)]
    one = jnp.ones((1, panels), F32)
    none = jnp.zeros((8, panels), F32)
    for c in range(clusters):
        at = slice(c, c + 1)
        top = [-2.0 * positions[a][0][at] for a in range(3)]
        rest = [-2.0 * positions[a][1][at] for a in range(3)]
        turned = jnp.concatenate(
            top + [one, none[0:4]] + rest + [none[0:5]] + top + [one, none[0:4]] + rest + [none[0:5]]
            + [none[0:3], one, none[0:4]] + [part[at] for part in softened]
            + [none[0:5], jnp.zeros((80, panels), F32)], axis=0
        ).T
        features_ref[c * panels : (c + 1) * panels, :] = turned.astype(BF16)
    features_ref[clusters * panels :, :] = jnp.where(
        lax.broadcasted_iota(jnp.int32, (HIGHER, 128), 1) == 40, 1.0, 0.0
    ).astype(BF16)
    leaving = pltpu.make_async_copy(features_ref, features_hbm, small_sems.at[4])
    leaving.start()
    small[1].wait()
    lane = lax.broadcasted_iota(jnp.int32, (1, panels), 1)
    densities = []
    for c in range(clusters):
        if c % 4 == 0:
            for copy in copies[0][c : c + 4]:
                copy.wait()
            for copy in copies[1 + c // 4]:
                copy.start()
        current = basis_ref[c : c + 1].astype(BF16)
        density = dot(current, inverse_ref[c], NT)
        densities.append(jnp.where(lane < counts_ref[c], density, 0.0).astype(BF16))
    for copy in small[2:]:
        copy.wait()
    wide = jnp.concatenate([d.astype(F32) for d in densities], axis=0)
    density_ref[...] = wide
    scale = area_ref[...] * wide
    weights = [scale * normal_ref[a] for a in range(3)]
    whole = [top + rest for top, rest in positions]
    crossed = sum(whole[a] * weights[a] for a in range(3))
    for k, value in enumerate(whole + [norm] + weights + [crossed]):
        for c in range(clusters):
            payload_ref[c, k : k + 1, :] = value[c : c + 1]
    for copy in copies[1]:
        copy.wait()
    tails = [dot(densities[c], maps_ref[c], NT).astype(BF16) for c in range(clusters)]
    for copy in copies[2]:
        copy.wait()
    total = jnp.zeros((1, coeffs), F32)
    for c in range(clusters):
        total += dot(tails[c], up_ref[c], NT)
        payload_ref[clusters, c : c + 1, 0:coeffs] = tails[c].astype(F32)
        payload_ref[clusters, c : c + 1, coeffs:panels] = jnp.full(
            (1, panels - coeffs), counts_ref[c].astype(F32)
        )
    lines = coeffs // 128
    row = lax.broadcasted_iota(jnp.int32, group_ref.shape, 0) & (lines - 1)
    spread = total[:, 0:128]
    for k in range(1, lines):
        spread = jnp.where(row == k, total[:, 128 * k : 128 * k + 128], spread)
    group_ref[...] = jnp.broadcast_to(spread, group_ref.shape)
    leaving.wait()


def sources(own, lists, nears, counts, basis, inverse, maps, up, positions, normals, areas, devices):
    count, clusters, panels = basis.shape
    coeffs = maps.shape[1]
    lines = devices * coeffs // 128
    pairs = clusters * (lists.shape[1] + 1) + PAIRS + 1
    return pl.pallas_call(
        source_kernel,
        in_specs=[SMEM] * 4 + [HBM] * 7,
        out_specs=[VMEM] * 3 + [HBM] + [SMEM] * 2,
        out_shape=[
            jax.ShapeDtypeStruct((clusters + 1, 8, panels), F32),
            jax.ShapeDtypeStruct((lines, 128), F32),
            jax.ShapeDtypeStruct((clusters, panels), F32),
            jax.ShapeDtypeStruct((clusters * panels + HIGHER, 128), BF16),
            jax.ShapeDtypeStruct((pairs,), jnp.int32),
            jax.ShapeDtypeStruct((pairs,), jnp.int32),
        ],
        scratch_shapes=[
            pltpu.VMEM((clusters, panels), F32),
            pltpu.VMEM(inverse.shape, BF16),
            pltpu.VMEM(maps.shape, BF16),
            pltpu.VMEM(up.shape, BF16),
            pltpu.VMEM(positions.shape, F32),
            pltpu.VMEM(normals.shape, F32),
            pltpu.VMEM(areas.shape, F32),
            pltpu.VMEM((clusters * panels + HIGHER, 128), BF16),
            pltpu.SemaphoreType.DMA((3, clusters)),
            pltpu.SemaphoreType.DMA((5,)),
        ],
        cost_estimate=pl.CostEstimate(flops=4 * 10**8, bytes_accessed=8 * MIB, transcendentals=0),
    )(own, lists, nears, counts, basis, inverse, maps, up, positions, normals, areas)


def near_tiles(
    pairs_ref, counts_ref, tails, window, position_ref,
    tile_list, features, total, squares, ready_list, ready,
):
    clusters = counts_ref.shape[0]
    panels = window.shape[2]
    highs, wides = panels // HIGHER, panels // ACROSS
    shift = lambda value, size: lax.shift_right_logical(value, power(size))
    ready_list()

    def list_some(g, length):
        for k in range(PAIRS):
            pair = pairs_ref[g * PAIRS + k]
            used = pair < DEAD
            pair = jnp.where(used, pair, 0)
            c, local, block = pair & 255, shift(pair, 256) & 255, shift(pair, 65536)
            live = tails[block, local, 0].astype(jnp.int32)
            down = jnp.where(used, shift(live + (ACROSS - 1), ACROSS), 0)
            across = shift(counts_ref[c] + (HIGHER - 1), HIGHER)
            base = ((block * (clusters + 1) + local) << (8 + power(wides))) + c * highs
            for j in reversed(range(highs)):
                for i in reversed(range(wides)):
                    tile_list[length + i * across + j] = base + ((i << 8) + j)
            length = length + down * across
        return length

    pairs = pairs_ref[pairs_ref.shape[0] - 1]
    length = lax.fori_loop(0, shift(pairs + (PAIRS - 1), PAIRS), list_some, jnp.int32(0))
    for extra in range(2 * UNROLL):
        tile_list[length + extra] = clusters * highs

    total[...] = jnp.zeros_like(total)

    def tile(s):
        lane = pl.multiple_of((s & (wides - 1)) * ACROSS, ACROSS)
        return window[lax.shift_right_logical(s, power(wides)), :, pl.ds(lane, ACROSS)]

    def square(at, u):
        spot = tile_list[at]
        top, middle, low = thirds(tile(lax.shift_right_logical(spot, 8)))
        right = jnp.concatenate(
            [top, top, middle, middle, low, jnp.ones((8, ACROSS), BF16), jnp.zeros((80, ACROSS), BF16)],
            axis=0,
        )
        left = features[pl.ds(pl.multiple_of((spot & 255) * HIGHER, HIGHER), HIGHER), :]
        squares[u] = dot(left, right, NN)

    def apply(at, u):
        inverse = lax.rsqrt(squares[u])
        field = (inverse * inverse * inverse).astype(BF16)
        top, rest = halves(tile(lax.shift_right_logical(tile_list[at], 8)))
        return dot(jnp.concatenate([top, rest], axis=0), field, NT)

    ready()
    for u in range(UNROLL):
        square(u, u)

    def step(g, carry):
        results = []
        for u in range(UNROLL):
            results.append((tile_list[g * UNROLL + u] & 255, apply(g * UNROLL + u, u)))
            square((g + 1) * UNROLL + u, u)
        for t, result in results:
            total[t] += result
        return carry

    lax.fori_loop(0, shift(length + (UNROLL - 1), UNROLL), step, 0)

    lines = []
    for c in range(clusters):
        parts = []
        for j in range(highs):
            r = total[c * highs + j]
            r = r[0:8] + r[8:16]
            x = position_ref[c, 0:3, j * HIGHER : (j + 1) * HIGHER]
            parts.append(jnp.sum(x * r[4:7], axis=0, keepdims=True) - r[7:8])
        lines.append(jnp.concatenate(parts, axis=1))
    return jnp.concatenate(lines, axis=0)


def near_scratch(clusters, slots, panels, blocks):
    highs, wides = panels // HIGHER, panels // ACROSS
    most = clusters * slots * highs * wides + 4 * UNROLL
    return [
        pltpu.SMEM((most,), jnp.int32),
        pltpu.VMEM((clusters * panels + HIGHER, 128), BF16),
        pltpu.SemaphoreType.DMA,
        pltpu.VMEM((clusters * highs + 1, 16, HIGHER), F32),
        pltpu.VMEM((UNROLL, HIGHER, ACROSS), F32),
        pltpu.VMEM((blocks * (clusters + 1), 8, panels), F32),
        pltpu.SMEM((blocks, clusters, 128), F32),
    ]


def row_kernel(pairs_ref, counts_ref, features_hbm, a_ref, b_ref, c_ref, d_ref, out_ref,
               tile_list, features, feature_sem, total, squares, window, tails, sems):
    clusters = counts_ref.shape[0]
    blocks = (a_ref, b_ref, c_ref, d_ref)
    coeffs = window.shape[2] // 2
    copies = []
    for k, block in enumerate(blocks):
        copies.append(pltpu.make_async_copy(
            block, window.at[pl.ds(k * (clusters + 1), clusters + 1)], sems.at[0, k]))
        copies.append(pltpu.make_async_copy(
            block.at[clusters, :, pl.ds(coeffs, 128)], tails.at[k], sems.at[1, k]))
    first, then = copies[1::2], copies[0::2]
    then.append(pltpu.make_async_copy(features_hbm, features, feature_sem))

    def wait(group):
        for copy in group:
            copy.wait()

    for copy in first + then:
        copy.start()
    out_ref[...] = near_tiles(
        pairs_ref, counts_ref, tails, window, window, tile_list, features, total, squares,
        lambda: wait(first), lambda: wait(then),
    )


def row_fields(pairs, counts, features, slots, blocks):
    clusters = counts.shape[0]
    panels = blocks[0].shape[2]
    return pl.pallas_call(
        row_kernel,
        in_specs=[SMEM] * 2 + [ANY] * (1 + len(blocks)),
        out_specs=VMEM,
        out_shape=jax.ShapeDtypeStruct((clusters, panels), F32),
        scratch_shapes=near_scratch(clusters, slots + 1, panels, len(blocks))
        + [pltpu.SemaphoreType.DMA((2, len(blocks)))],
        cost_estimate=pl.CostEstimate(flops=3 * 10**9, bytes_accessed=MIB, transcendentals=10**6),
    )(pairs, counts, features, *blocks)


def late_kernel(
    own_ref, pairs_ref, counts_ref, leaf_ids_ref, leaf_kinds_ref, group_ids_ref,
    group_kinds_ref, groups_ref, density_ref, near_ref, basis_ref, features_hbm, far_hbm, up_hbm, maps_hbm,
    a_ref, b_ref, c_ref, d_ref, e_ref, f_ref, g_ref,
    image_ref, sums_ref,
    tile_list, features, feature_sem, total, squares, window, tails, sems,
    far_ref, up_ref, maps_ref, own_rows, moments, weight_sems,
):
    clusters, panels = density_ref.shape
    kinds, coeffs = far_ref.shape[1], far_ref.shape[2]
    row, others = (a_ref, b_ref, c_ref, d_ref), (e_ref, f_ref, g_ref)
    copies = []
    for k, block in enumerate(others):
        copies.append(pltpu.make_async_copy(
            block, window.at[pl.ds(k * (clusters + 1), clusters + 1)], sems.at[0, k]))
        copies.append(pltpu.make_async_copy(
            block.at[clusters, :, pl.ds(coeffs, 128)], tails.at[k], sems.at[1, k]))
    copies.append(pltpu.make_async_copy(a_ref, own_rows, weight_sems.at[3]))
    first, then = copies[1::2], copies[0:-1:2] + copies[-1:]
    then.append(pltpu.make_async_copy(features_hbm, features, feature_sem))

    def wait(group):
        for copy in group:
            copy.wait()

    for copy in first + then:
        copy.start()
    later = [
        pltpu.make_async_copy(block.at[clusters, :, pl.ds(0, coeffs)],
                              moments.at[pl.ds(k * clusters, clusters)], sems.at[2, k])
        for k, block in enumerate(row + others)
    ]
    later += [
        pltpu.make_async_copy(far_hbm, far_ref, weight_sems.at[0]),
        pltpu.make_async_copy(up_hbm, up_ref, weight_sems.at[1]),
        pltpu.make_async_copy(maps_hbm, maps_ref, weight_sems.at[2]),
    ]
    own = own_ref[0]

    def arrived():
        wait(then)
        for copy in later:
            copy.start()

    near = near_ref[...] + near_tiles(
        pairs_ref, counts_ref, tails, window, own_rows, tile_list, features, total, squares,
        lambda: wait(first), arrived,
    )
    for copy in later:
        copy.wait()

    lines = coeffs // 128
    spots = groups_ref.shape[0]
    kind = lax.broadcasted_iota(jnp.int32, (kinds, 1), 0)
    spot = lax.broadcasted_iota(jnp.int32, (1, spots), 1)
    pick = jnp.zeros((kinds, spots), F32)
    for n in range(group_ids_ref.shape[1]):
        hit = (kind == group_kinds_ref[0, n]) & (
            lax.shift_right_logical(spot, power(lines)) == group_ids_ref[0, n])
        pick += jnp.where(hit, 1.0, 0.0)
    local = jnp.zeros((24, coeffs), F32)
    group_sum = jnp.concatenate(
        [
            lax.dot_general(jnp.where((spot & (lines - 1)) == k, pick, 0.0), groups_ref[...], NN,
                            precision=HIGH, preferred_element_type=F32)
            for k in range(lines)
        ],
        axis=1,
    )
    group_rows = jnp.concatenate([part.astype(F32) for part in thirds(group_sum)], axis=0)
    row24 = lax.broadcasted_iota(jnp.int32, (24, 1), 0) & (kinds - 1)
    for o in range(kinds):
        local += dot(jnp.where(row24 == o, group_rows, 0.0).astype(BF16), far_ref[1, o], NT)
    local = jnp.sum(local, axis=0, keepdims=True).astype(BF16)

    block, inside = window_block(own, leaf_ids_ref[...], clusters, 4)
    spots_of = block * clusters + inside
    spot = lax.broadcasted_iota(jnp.int32, (1, moments.shape[0]), 1)
    picks = [jnp.zeros((clusters, moments.shape[0]), F32) for _ in range(kinds)]
    for n in range(leaf_ids_ref.shape[1]):
        hit = jnp.where(spots_of[:, n : n + 1] == spot, 1.0, 0.0)
        for o in range(kinds):
            picks[o] += jnp.where(leaf_kinds_ref[:, n : n + 1] == o, hit, 0.0)
    leaf_sum = dot(
        jnp.concatenate(picks, axis=0).astype(BF16), moments[...].astype(BF16), NN
    )
    leaf = jnp.zeros((2 * clusters, coeffs), F32)
    for o in range(kinds):
        top, rest = halves(leaf_sum[o * clusters : (o + 1) * clusters])
        leaf += dot(jnp.concatenate([top, rest], axis=0), far_ref[0, o], NT)
    leaf = leaf[0:clusters] + leaf[clusters:]
    leaf += jnp.concatenate([dot(local, up_ref[c], NN) for c in range(clusters)], axis=0)
    leaf = leaf.astype(BF16)
    images = []
    lane = lax.broadcasted_iota(jnp.int32, (1, panels), 1)
    for c in range(clusters):
        far = dot(leaf[c : c + 1], maps_ref[c], NN)
        value = 0.5 * density_ref[c : c + 1] + near[c : c + 1] + far
        images.append(jnp.where(lane < counts_ref[c], value, 0.0))
    image = jnp.concatenate(images, axis=0)
    image_ref[...] = image
    lane = lax.broadcasted_iota(jnp.int32, (1, 128), 1)
    sums = jnp.zeros((1, 128), F32)
    for k in range(basis_ref.shape[0] + 1):
        other = basis_ref[k] if k < basis_ref.shape[0] else image
        value = jnp.sum(jnp.sum(image * other, axis=0, keepdims=True), axis=1, keepdims=True)
        sums += jnp.where(lane == k, value, 0.0)
    sums_ref[...] = jnp.broadcast_to(sums, sums_ref.shape)


def late_fields(own, pairs, counts, slots, leaf_ids, leaf_kinds, group_ids, group_kinds, groups,
                density, near, basis, features, far, up, maps, window, devices):
    clusters, panels = density.shape
    return pl.pallas_call(
        late_kernel,
        in_specs=[SMEM] * 3 + [VMEM] * 2 + [SMEM] * 2 + [VMEM] * 4 + [ANY] + [HBM] * 3 + [ANY] * 7,
        out_specs=[VMEM, VMEM],
        out_shape=[
            jax.ShapeDtypeStruct(density.shape, F32),
            jax.ShapeDtypeStruct((devices, 128), F32),
        ],
        scratch_shapes=near_scratch(clusters, slots + 1, panels, 3)
        + [
            pltpu.SemaphoreType.DMA((3, 7)),
            pltpu.VMEM(far.shape, BF16),
            pltpu.VMEM(up.shape, BF16),
            pltpu.VMEM(maps.shape, BF16),
            pltpu.VMEM((clusters + 1, 8, panels), F32),
            pltpu.VMEM((7 * clusters, maps.shape[1]), F32),
            pltpu.SemaphoreType.DMA((4,)),
        ],
        cost_estimate=pl.CostEstimate(flops=3 * 10**9, bytes_accessed=MIB, transcendentals=10**6),
    )(own, pairs, counts, leaf_ids, leaf_kinds, group_ids, group_kinds, groups, density,
      near, basis, features, far, up, maps, *window)


def close_kernel(rows, sums_ref, image_hbm, basis_ref, next_ref, column_ref, image_ref, sem):
    copy = pltpu.make_async_copy(image_hbm, image_ref, sem)
    copy.start()
    count = basis_ref.shape[0]
    means = jnp.sum(sums_ref[...], axis=0, keepdims=True) * (1.0 / rows)
    lane = lax.broadcasted_iota(jnp.int32, (1, 128), 1)
    coeffs = jnp.where(lane < count, means, 0.0)
    square = jnp.sum(jnp.where(lane == count, means, 0.0), axis=1, keepdims=True)
    energy = square - jnp.sum(coeffs * coeffs, axis=1, keepdims=True)
    height = jnp.sqrt(energy + EPSILON)
    copy.wait()
    remainder = image_ref[...]
    for k in range(count):
        remainder = remainder - coeffs[:, k : k + 1] * basis_ref[k]
        column_ref[k] = means[0, k]
    column_ref[count] = height[0, 0]
    next_ref[...] = remainder / height


def close(sums, image, basis, rows):
    return pl.pallas_call(
        functools.partial(close_kernel, rows),
        in_specs=[VMEM, HBM, VMEM],
        out_specs=[VMEM, SMEM],
        out_shape=[
            jax.ShapeDtypeStruct(image.shape, F32),
            jax.ShapeDtypeStruct((basis.shape[0] + 1,), F32),
        ],
        scratch_shapes=[pltpu.VMEM(image.shape, F32), pltpu.SemaphoreType.DMA],
        compiler_params=pltpu.CompilerParams(vmem_limit_bytes=2 * MIB),
    )(sums, image, basis)


def row_routes(rows, width):
    spot = lambda r, y: (r % rows) * width + y
    turns = {1: (1, -1, -1, -1), 2: (1, 1, -1, -1), 3: (1, 1, 1, -1)}
    return {
        k: [(spot(r, y), spot(r + turns[k][y], y)) for r in range(rows) for y in range(width)]
        for k in turns
    }


def shards(
    positions, normals, panel_areas, panel_counts, near_lists, near_counts, leaf_lists, leaf_kinds,
    group_lists, group_kinds, block_inverse, moment_maps, up_operators, far_operators, krylov_basis,
):
    clusters, _, panels = positions.shape
    coeffs = moment_maps.shape[1]
    devices = lax.axis_size(AXES)
    width = lax.axis_size(AXES[-1])
    own = jnp.full((1,), lax.axis_index(AXES), jnp.int32)
    payload, group, density, features, row_pairs, off_pairs = sources(
        own, near_lists, near_counts, panel_counts, krylov_basis, block_inverse, moment_maps, up_operators,
        positions.transpose(1, 0, 2), normals.transpose(1, 0, 2), panel_areas, devices,
    )
    row = [payload] + [
        lax.ppermute(payload, AXES[-1], [(y, (y + k) % width) for y in range(width)])
        for k in range(1, width)
    ]
    routes = row_routes(devices // width, width)
    window = row + [lax.ppermute(row[k], AXES, routes[k]) for k in range(1, width)]
    groups = lax.all_to_all(group, AXES, 0, 0, tiled=True)
    slots = near_lists.shape[1]
    near = row_fields(row_pairs, panel_counts, features, slots, row)
    image, sums = late_fields(
        own, off_pairs, panel_counts, slots, leaf_lists, leaf_kinds, group_lists, group_kinds,
        groups, density, near, krylov_basis, features, far_operators, up_operators, moment_maps, window, devices,
    )
    sums = lax.all_to_all(sums, AXES, 0, 0, tiled=True)
    return close(sums, image, krylov_basis, devices * clusters * panels)


def solution(mesh):
    finer = Mesh(mesh.devices.reshape(mesh.shape["role"], 4, 4, 4), AXES)
    split = lambda rank: P(AXES, *([None] * (rank - 1)))
    return jax.shard_map(
        shards,
        mesh=finer,
        in_specs=(
            split(3), split(3), split(2), split(1), split(2), split(1), split(2), split(2), split(2),
            split(2), split(3), split(3), P(), P(), P(None, AXES, None),
        ),
        out_specs=(split(2), P()),
        check_vma=False,
    )
```

```python
import functools

import jax
import jax.numpy as jnp
from jax import lax
from jax.experimental import pallas as pl
from jax.experimental.pallas import tpu as pltpu
from jax.sharding import Mesh
from jax.sharding import PartitionSpec as P

RADIUS = 3
AXES = ("role", "dev_0", "dev_1", "dev_2")
SOFTEN = 0.01
EPSILON = 1e-06
HIGH = lax.Precision.HIGHEST
F32 = jnp.float32
BF16 = jnp.bfloat16
VMEM = pl.BlockSpec(memory_space=pltpu.VMEM)
SMEM = pl.BlockSpec(memory_space=pltpu.SMEM)
ANY = pl.BlockSpec(memory_space=pl.ANY)
HBM = pl.BlockSpec(memory_space=pltpu.HBM)
NT = (((1,), (1,)), ((), ()))
NN = (((1,), (0,)), ((), ()))
HIGHER = 128
ACROSS = 256
UNROLL = 16
MIB = 2**20
PAIRS = 4
DEAD = 1 << 24


def dot(a, b, dims):
    return lax.dot_general(a, b, dims, preferred_element_type=F32)


def halves(value):
    top = value.astype(BF16)
    return top, (value - top.astype(F32)).astype(BF16)


def thirds(value):
    top, rest = value.astype(BF16), None
    rest = value - top.astype(F32)
    middle = rest.astype(BF16)
    return top, middle, (rest - middle.astype(F32)).astype(BF16)


def power(value):
    assert value & (value - 1) == 0
    return value.bit_length() - 1


def window_block(own, ids, clusters, width):
    owner = lax.shift_right_logical(ids, power(clusters))
    shift = (own - owner) & (width - 1)
    same = lax.shift_right_logical(owner, power(width)) == lax.shift_right_logical(own, power(width))
    return jnp.where(same, shift, shift + width - 1), ids & (clusters - 1)


def list_pairs(own, lists_ref, nears_ref, row_ref, off_ref, width):
    clusters = lists_ref.shape[0]

    def list_cluster(c, lengths):
        row, off = lengths
        row_ref[row] = (c << 8) + c

        def list_slot(s, lengths):
            row, off = lengths
            block, inside = window_block(own, lists_ref[c, s], clusters, width)
            pair = (block << 16) + (inside << 8) + c
            near = jnp.where(block < width, 1, 0)
            row_ref[row] = pair
            off_ref[off] = pair - (width << 16)
            return row + near, off + 1 - near

        return lax.fori_loop(0, nears_ref[c], list_slot, (row + 1, off))

    row, off = lax.fori_loop(0, clusters, list_cluster, (jnp.int32(0), jnp.int32(0)))
    for ref, length in ((row_ref, row), (off_ref, off)):
        for k in range(PAIRS):
            ref[length + k] = DEAD
        ref[ref.shape[0] - 1] = length


def source_kernel(
    own_ref, lists_ref, nears_ref, counts_ref,
    basis_hbm, inverse_hbm, maps_hbm, up_hbm, position_hbm, normal_hbm, area_hbm,
    payload_ref, group_ref, density_ref, features_hbm, row_ref, off_ref,
    basis_ref, inverse_ref, maps_ref, up_ref, position_ref, normal_ref, area_ref,
    features_ref, sems, small_sems,
):
    clusters, panels = density_ref.shape
    coeffs = maps_ref.shape[1]
    copies = [
        [pltpu.make_async_copy(a.at[c], b.at[c], sems.at[k, c]) for c in range(clusters)]
        for k, (a, b) in enumerate(((inverse_hbm, inverse_ref), (maps_hbm, maps_ref), (up_hbm, up_ref)))
    ]
    small = [
        pltpu.make_async_copy(a, b, small_sems.at[k])
        for k, (a, b) in enumerate((
            (position_hbm, position_ref), (basis_hbm.at[basis_hbm.shape[0] - 1], basis_ref),
            (normal_hbm, normal_ref), (area_hbm, area_ref)))
    ]
    for copy in small[0:2] + copies[0] + small[2:]:
        copy.start()
    list_pairs(own_ref[0], lists_ref, nears_ref, row_ref, off_ref, 4)
    small[0].wait()
    norm = jnp.zeros((clusters, panels), F32)
    positions = []
    for a in range(3):
        top, rest = halves(position_ref[a])
        positions.append((top.astype(F32), rest.astype(F32)))
        norm += (positions[a][0] + positions[a][1]) * (positions[a][0] + positions[a][1])
    softened = [part.astype(F32) for part in thirds(norm + SOFTEN)]
    one = jnp.ones((1, panels), F32)
    none = jnp.zeros((8, panels), F32)
    for c in range(clusters):
        at = slice(c, c + 1)
        top = [-2.0 * positions[a][0][at] for a in range(3)]
        rest = [-2.0 * positions[a][1][at] for a in range(3)]
        turned = jnp.concatenate(
            top + [one, none[0:4]] + rest + [none[0:5]] + top + [one, none[0:4]] + rest + [none[0:5]]
            + [none[0:3], one, none[0:4]] + [part[at] for part in softened]
            + [none[0:5], jnp.zeros((80, panels), F32)], axis=0
        ).T
        features_ref[c * panels : (c + 1) * panels, :] = turned.astype(BF16)
    features_ref[clusters * panels :, :] = jnp.where(
        lax.broadcasted_iota(jnp.int32, (HIGHER, 128), 1) == 40, 1.0, 0.0
    ).astype(BF16)
    leaving = pltpu.make_async_copy(features_ref, features_hbm, small_sems.at[4])
    leaving.start()
    small[1].wait()
    lane = lax.broadcasted_iota(jnp.int32, (1, panels), 1)
    densities = []
    for c in range(clusters):
        if c % 4 == 0:
            for copy in copies[0][c : c + 4]:
                copy.wait()
            for copy in copies[1 + c // 4]:
                copy.start()
        current = basis_ref[c : c + 1].astype(BF16)
        density = dot(current, inverse_ref[c], NT)
        densities.append(jnp.where(lane < counts_ref[c], density, 0.0).astype(BF16))
    for copy in small[2:]:
        copy.wait()
    wide = jnp.concatenate([d.astype(F32) for d in densities], axis=0)
    density_ref[...] = wide
    scale = area_ref[...] * wide
    weights = [scale * normal_ref[a] for a in range(3)]
    whole = [top + rest for top, rest in positions]
    crossed = sum(whole[a] * weights[a] for a in range(3))
    for k, value in enumerate(whole + [norm] + weights + [crossed]):
        for c in range(clusters):
            payload_ref[c, k : k + 1, :] = value[c : c + 1]
    for copy in copies[1]:
        copy.wait()
    tails = [dot(densities[c], maps_ref[c], NT).astype(BF16) for c in range(clusters)]
    for copy in copies[2]:
        copy.wait()
    total = jnp.zeros((1, coeffs), F32)
    for c in range(clusters):
        total += dot(tails[c], up_ref[c], NT)
        payload_ref[clusters, c : c + 1, 0:coeffs] = tails[c].astype(F32)
        payload_ref[clusters, c : c + 1, coeffs:panels] = jnp.full(
            (1, panels - coeffs), counts_ref[c].astype(F32)
        )
    lines = coeffs // 128
    row = lax.broadcasted_iota(jnp.int32, group_ref.shape, 0) & (lines - 1)
    spread = total[:, 0:128]
    for k in range(1, lines):
        spread = jnp.where(row == k, total[:, 128 * k : 128 * k + 128], spread)
    group_ref[...] = jnp.broadcast_to(spread, group_ref.shape)
    leaving.wait()


def sources(own, lists, nears, counts, basis, inverse, maps, up, positions, normals, areas, devices):
    count, clusters, panels = basis.shape
    coeffs = maps.shape[1]
    lines = devices * coeffs // 128
    pairs = clusters * (lists.shape[1] + 1) + PAIRS + 1
    return pl.pallas_call(
        source_kernel,
        in_specs=[SMEM] * 4 + [HBM] * 7,
        out_specs=[VMEM] * 3 + [HBM] + [SMEM] * 2,
        out_shape=[
            jax.ShapeDtypeStruct((clusters + 1, 8, panels), F32),
            jax.ShapeDtypeStruct((lines, 128), F32),
            jax.ShapeDtypeStruct((clusters, panels), F32),
            jax.ShapeDtypeStruct((clusters * panels + HIGHER, 128), BF16),
            jax.ShapeDtypeStruct((pairs,), jnp.int32),
            jax.ShapeDtypeStruct((pairs,), jnp.int32),
        ],
        scratch_shapes=[
            pltpu.VMEM((clusters, panels), F32),
            pltpu.VMEM(inverse.shape, BF16),
            pltpu.VMEM(maps.shape, BF16),
            pltpu.VMEM(up.shape, BF16),
            pltpu.VMEM(positions.shape, F32),
            pltpu.VMEM(normals.shape, F32),
            pltpu.VMEM(areas.shape, F32),
            pltpu.VMEM((clusters * panels + HIGHER, 128), BF16),
            pltpu.SemaphoreType.DMA((3, clusters)),
            pltpu.SemaphoreType.DMA((5,)),
        ],
        cost_estimate=pl.CostEstimate(flops=4 * 10**8, bytes_accessed=8 * MIB, transcendentals=0),
    )(own, lists, nears, counts, basis, inverse, maps, up, positions, normals, areas)


def near_tiles(
    pairs_ref, counts_ref, tails, window, position_ref,
    tile_list, features, total, squares, ready_list, ready,
):
    clusters = counts_ref.shape[0]
    panels = window.shape[2]
    highs, wides = panels // HIGHER, panels // ACROSS
    shift = lambda value, size: lax.shift_right_logical(value, power(size))
    ready_list()

    def list_some(g, length):
        for k in range(PAIRS):
            pair = pairs_ref[g * PAIRS + k]
            used = pair < DEAD
            pair = jnp.where(used, pair, 0)
            c, local, block = pair & 255, shift(pair, 256) & 255, shift(pair, 65536)
            live = tails[block, local, 0].astype(jnp.int32)
            down = jnp.where(used, shift(live + (ACROSS - 1), ACROSS), 0)
            across = shift(counts_ref[c] + (HIGHER - 1), HIGHER)
            base = ((block * (clusters + 1) + local) << (8 + power(wides))) + c * highs
            for j in reversed(range(highs)):
                for i in reversed(range(wides)):
                    tile_list[length + i * across + j] = base + ((i << 8) + j)
            length = length + down * across
        return length

    pairs = pairs_ref[pairs_ref.shape[0] - 1]
    length = lax.fori_loop(0, shift(pairs + (PAIRS - 1), PAIRS), list_some, jnp.int32(0))
    for extra in range(2 * UNROLL):
        tile_list[length + extra] = clusters * highs

    total[...] = jnp.zeros_like(total)

    def tile(s):
        lane = pl.multiple_of((s & (wides - 1)) * ACROSS, ACROSS)
        return window[lax.shift_right_logical(s, power(wides)), :, pl.ds(lane, ACROSS)]

    def square(at, u):
        spot = tile_list[at]
        top, middle, low = thirds(tile(lax.shift_right_logical(spot, 8)))
        right = jnp.concatenate(
            [top, top, middle, middle, low, jnp.ones((8, ACROSS), BF16), jnp.zeros((80, ACROSS), BF16)],
            axis=0,
        )
        left = features[pl.ds(pl.multiple_of((spot & 255) * HIGHER, HIGHER), HIGHER), :]
        squares[u] = dot(left, right, NN)

    def apply(at, u):
        inverse = lax.rsqrt(squares[u])
        field = (inverse * inverse * inverse).astype(BF16)
        top, rest = halves(tile(lax.shift_right_logical(tile_list[at], 8)))
        return dot(jnp.concatenate([top, rest], axis=0), field, NT)

    ready()
    for u in range(UNROLL):
        square(u, u)

    def step(g, carry):
        results = []
        for u in range(UNROLL):
            results.append((tile_list[g * UNROLL + u] & 255, apply(g * UNROLL + u, u)))
            square((g + 1) * UNROLL + u, u)
        for t, result in results:
            total[t] += result
        return carry

    lax.fori_loop(0, shift(length + (UNROLL - 1), UNROLL), step, 0)

    lines = []
    for c in range(clusters):
        parts = []
        for j in range(highs):
            r = total[c * highs + j]
            r = r[0:8] + r[8:16]
            x = position_ref[c, 0:3, j * HIGHER : (j + 1) * HIGHER]
            parts.append(jnp.sum(x * r[4:7], axis=0, keepdims=True) - r[7:8])
        lines.append(jnp.concatenate(parts, axis=1))
    return jnp.concatenate(lines, axis=0)


def near_scratch(clusters, slots, panels, blocks):
    highs, wides = panels // HIGHER, panels // ACROSS
    most = clusters * slots * highs * wides + 4 * UNROLL
    return [
        pltpu.SMEM((most,), jnp.int32),
        pltpu.VMEM((clusters * panels + HIGHER, 128), BF16),
        pltpu.SemaphoreType.DMA,
        pltpu.VMEM((clusters * highs + 1, 16, HIGHER), F32),
        pltpu.VMEM((UNROLL, HIGHER, ACROSS), F32),
        pltpu.VMEM((blocks * (clusters + 1), 8, panels), F32),
        pltpu.SMEM((blocks, clusters, 128), F32),
    ]


def row_kernel(pairs_ref, counts_ref, features_hbm, a_ref, b_ref, c_ref, d_ref, out_ref,
               tile_list, features, feature_sem, total, squares, window, tails, sems):
    clusters = counts_ref.shape[0]
    blocks = (a_ref, b_ref, c_ref, d_ref)
    coeffs = window.shape[2] // 2
    copies = []
    for k, block in enumerate(blocks):
        copies.append(pltpu.make_async_copy(
            block, window.at[pl.ds(k * (clusters + 1), clusters + 1)], sems.at[0, k]))
        copies.append(pltpu.make_async_copy(
            block.at[clusters, :, pl.ds(coeffs, 128)], tails.at[k], sems.at[1, k]))
    first, then = copies[1::2], copies[0::2]
    then.append(pltpu.make_async_copy(features_hbm, features, feature_sem))

    def wait(group):
        for copy in group:
            copy.wait()

    for copy in first + then:
        copy.start()
    out_ref[...] = near_tiles(
        pairs_ref, counts_ref, tails, window, window, tile_list, features, total, squares,
        lambda: wait(first), lambda: wait(then),
    )


def row_fields(pairs, counts, features, slots, blocks):
    clusters = counts.shape[0]
    panels = blocks[0].shape[2]
    return pl.pallas_call(
        row_kernel,
        in_specs=[SMEM] * 2 + [ANY] * (1 + len(blocks)),
        out_specs=VMEM,
        out_shape=jax.ShapeDtypeStruct((clusters, panels), F32),
        scratch_shapes=near_scratch(clusters, slots + 1, panels, len(blocks))
        + [pltpu.SemaphoreType.DMA((2, len(blocks)))],
        cost_estimate=pl.CostEstimate(flops=3 * 10**9, bytes_accessed=MIB, transcendentals=10**6),
    )(pairs, counts, features, *blocks)


def late_kernel(
    own_ref, pairs_ref, counts_ref, leaf_ids_ref, leaf_kinds_ref, group_ids_ref,
    group_kinds_ref, groups_ref, density_ref, near_ref, basis_ref, features_hbm, far_hbm, up_hbm, maps_hbm,
    a_ref, b_ref, c_ref, d_ref, e_ref, f_ref, g_ref,
    image_ref, sums_ref,
    tile_list, features, feature_sem, total, squares, window, tails, sems,
    far_ref, up_ref, maps_ref, own_rows, moments, weight_sems,
):
    clusters, panels = density_ref.shape
    kinds, coeffs = far_ref.shape[1], far_ref.shape[2]
    row, others = (a_ref, b_ref, c_ref, d_ref), (e_ref, f_ref, g_ref)
    copies = []
    for k, block in enumerate(others):
        copies.append(pltpu.make_async_copy(
            block, window.at[pl.ds(k * (clusters + 1), clusters + 1)], sems.at[0, k]))
        copies.append(pltpu.make_async_copy(
            block.at[clusters, :, pl.ds(coeffs, 128)], tails.at[k], sems.at[1, k]))
    copies.append(pltpu.make_async_copy(a_ref, own_rows, weight_sems.at[3]))
    first, then = copies[1::2], copies[0:-1:2] + copies[-1:]
    then.append(pltpu.make_async_copy(features_hbm, features, feature_sem))

    def wait(group):
        for copy in group:
            copy.wait()

    for copy in first + then:
        copy.start()
    later = [
        pltpu.make_async_copy(block.at[clusters, :, pl.ds(0, coeffs)],
                              moments.at[pl.ds(k * clusters, clusters)], sems.at[2, k])
        for k, block in enumerate(row + others)
    ]
    weights = [
        pltpu.make_async_copy(far_hbm, far_ref, weight_sems.at[0]),
        pltpu.make_async_copy(up_hbm, up_ref, weight_sems.at[1]),
        pltpu.make_async_copy(maps_hbm, maps_ref, weight_sems.at[2]),
    ]
    weights[0].start()
    own = own_ref[0]

    def arrived():
        wait(then)
        for copy in later + weights[1:]:
            copy.start()

    near = near_ref[...] + near_tiles(
        pairs_ref, counts_ref, tails, window, own_rows, tile_list, features, total, squares,
        lambda: wait(first), arrived,
    )
    for copy in later:
        copy.wait()

    lines = coeffs // 128
    spots = groups_ref.shape[0]
    kind = lax.broadcasted_iota(jnp.int32, (kinds, 1), 0)
    spot = lax.broadcasted_iota(jnp.int32, (1, spots), 1)
    pick = jnp.zeros((kinds, spots), F32)
    for n in range(group_ids_ref.shape[1]):
        hit = (kind == group_kinds_ref[0, n]) & (
            lax.shift_right_logical(spot, power(lines)) == group_ids_ref[0, n])
        pick += jnp.where(hit, 1.0, 0.0)
    pick = jnp.concatenate(
        [jnp.where((spot & (lines - 1)) == k, pick, 0.0) for k in range(lines)], axis=0
    ).astype(BF16)
    group_sum = sum(dot(pick, part, NN) for part in thirds(groups_ref[...]))
    group_sum = jnp.concatenate(
        [group_sum[k * kinds : (k + 1) * kinds] for k in range(lines)], axis=1
    )
    local = jnp.zeros((24, coeffs), F32)
    weights[0].wait()
    group_rows = jnp.concatenate([part.astype(F32) for part in thirds(group_sum)], axis=0)
    row24 = lax.broadcasted_iota(jnp.int32, (24, 1), 0) & (kinds - 1)
    for o in range(kinds):
        local += dot(jnp.where(row24 == o, group_rows, 0.0).astype(BF16), far_ref[1, o], NT)
    local = jnp.sum(local, axis=0, keepdims=True).astype(BF16)

    block, inside = window_block(own, leaf_ids_ref[...], clusters, 4)
    spots_of = block * clusters + inside
    spot = lax.broadcasted_iota(jnp.int32, (1, moments.shape[0]), 1)
    picks = [jnp.zeros((clusters, moments.shape[0]), F32) for _ in range(kinds)]
    for n in range(leaf_ids_ref.shape[1]):
        hit = jnp.where(spots_of[:, n : n + 1] == spot, 1.0, 0.0)
        for o in range(kinds):
            picks[o] += jnp.where(leaf_kinds_ref[:, n : n + 1] == o, hit, 0.0)
    leaf_sum = dot(
        jnp.concatenate(picks, axis=0).astype(BF16), moments[...].astype(BF16), NN
    )
    leaf = jnp.zeros((2 * clusters, coeffs), F32)
    for o in range(kinds):
        top, rest = halves(leaf_sum[o * clusters : (o + 1) * clusters])
        leaf += dot(jnp.concatenate([top, rest], axis=0), far_ref[0, o], NT)
    leaf = leaf[0:clusters] + leaf[clusters:]
    weights[1].wait()
    leaf += jnp.concatenate([dot(local, up_ref[c], NN) for c in range(clusters)], axis=0)
    leaf = leaf.astype(BF16)
    weights[2].wait()
    images = []
    lane = lax.broadcasted_iota(jnp.int32, (1, panels), 1)
    for c in range(clusters):
        far = dot(leaf[c : c + 1], maps_ref[c], NN)
        value = 0.5 * density_ref[c : c + 1] + near[c : c + 1] + far
        images.append(jnp.where(lane < counts_ref[c], value, 0.0))
    image = jnp.concatenate(images, axis=0)
    image_ref[...] = image
    lane = lax.broadcasted_iota(jnp.int32, (1, 128), 1)
    sums = jnp.zeros((1, 128), F32)
    for k in range(basis_ref.shape[0] + 1):
        other = basis_ref[k] if k < basis_ref.shape[0] else image
        value = jnp.sum(jnp.sum(image * other, axis=0, keepdims=True), axis=1, keepdims=True)
        sums += jnp.where(lane == k, value, 0.0)
    sums_ref[...] = jnp.broadcast_to(sums, sums_ref.shape)


def late_fields(own, pairs, counts, slots, leaf_ids, leaf_kinds, group_ids, group_kinds, groups,
                density, near, basis, features, far, up, maps, window, devices):
    clusters, panels = density.shape
    return pl.pallas_call(
        late_kernel,
        in_specs=[SMEM] * 3 + [VMEM] * 2 + [SMEM] * 2 + [VMEM] * 4 + [ANY] + [HBM] * 3 + [ANY] * 7,
        out_specs=[VMEM, VMEM],
        out_shape=[
            jax.ShapeDtypeStruct(density.shape, F32),
            jax.ShapeDtypeStruct((devices, 128), F32),
        ],
        scratch_shapes=near_scratch(clusters, slots + 1, panels, 3)
        + [
            pltpu.SemaphoreType.DMA((3, 7)),
            pltpu.VMEM(far.shape, BF16),
            pltpu.VMEM(up.shape, BF16),
            pltpu.VMEM(maps.shape, BF16),
            pltpu.VMEM((clusters + 1, 8, panels), F32),
            pltpu.VMEM((7 * clusters, maps.shape[1]), F32),
            pltpu.SemaphoreType.DMA((4,)),
        ],
        cost_estimate=pl.CostEstimate(flops=3 * 10**9, bytes_accessed=MIB, transcendentals=10**6),
    )(own, pairs, counts, leaf_ids, leaf_kinds, group_ids, group_kinds, groups, density,
      near, basis, features, far, up, maps, *window)


def close_kernel(rows, sums_ref, image_hbm, basis_ref, next_ref, column_ref, image_ref, sem):
    copy = pltpu.make_async_copy(image_hbm, image_ref, sem)
    copy.start()
    count = basis_ref.shape[0]
    means = jnp.sum(sums_ref[...], axis=0, keepdims=True) * (1.0 / rows)
    lane = lax.broadcasted_iota(jnp.int32, (1, 128), 1)
    coeffs = jnp.where(lane < count, means, 0.0)
    square = jnp.sum(jnp.where(lane == count, means, 0.0), axis=1, keepdims=True)
    energy = square - jnp.sum(coeffs * coeffs, axis=1, keepdims=True)
    height = jnp.sqrt(energy + EPSILON)
    copy.wait()
    remainder = image_ref[...]
    for k in range(count):
        remainder = remainder - coeffs[:, k : k + 1] * basis_ref[k]
        column_ref[k] = means[0, k]
    column_ref[count] = height[0, 0]
    next_ref[...] = remainder / height


def close(sums, image, basis, rows):
    return pl.pallas_call(
        functools.partial(close_kernel, rows),
        in_specs=[VMEM, HBM, VMEM],
        out_specs=[VMEM, SMEM],
        out_shape=[
            jax.ShapeDtypeStruct(image.shape, F32),
            jax.ShapeDtypeStruct((basis.shape[0] + 1,), F32),
        ],
        scratch_shapes=[pltpu.VMEM(image.shape, F32), pltpu.SemaphoreType.DMA],
    )(sums, image, basis)


def row_routes(rows, width):
    spot = lambda r, y: (r % rows) * width + y
    turns = {1: (1, -1, -1, -1), 2: (1, 1, -1, -1), 3: (1, 1, 1, -1)}
    return {
        k: [(spot(r, y), spot(r + turns[k][y], y)) for r in range(rows) for y in range(width)]
        for k in turns
    }


def shards(
    positions, normals, panel_areas, panel_counts, near_lists, near_counts, leaf_lists, leaf_kinds,
    group_lists, group_kinds, block_inverse, moment_maps, up_operators, far_operators, krylov_basis,
):
    clusters, _, panels = positions.shape
    coeffs = moment_maps.shape[1]
    devices = lax.axis_size(AXES)
    width = lax.axis_size(AXES[-1])
    own = jnp.full((1,), lax.axis_index(AXES), jnp.int32)
    payload, group, density, features, row_pairs, off_pairs = sources(
        own, near_lists, near_counts, panel_counts, krylov_basis, block_inverse, moment_maps, up_operators,
        positions.transpose(1, 0, 2), normals.transpose(1, 0, 2), panel_areas, devices,
    )
    row = [payload] + [
        lax.ppermute(payload, AXES[-1], [(y, (y + k) % width) for y in range(width)])
        for k in range(1, width)
    ]
    routes = row_routes(devices // width, width)
    window = row + [lax.ppermute(row[k], AXES, routes[k]) for k in range(1, width)]
    groups = lax.all_to_all(group, AXES, 0, 0, tiled=True)
    slots = near_lists.shape[1]
    near = row_fields(row_pairs, panel_counts, features, slots, row)
    image, sums = late_fields(
        own, off_pairs, panel_counts, slots, leaf_lists, leaf_kinds, group_lists, group_kinds,
        groups, density, near, krylov_basis, features, far_operators, up_operators, moment_maps, window, devices,
    )
    sums = lax.all_to_all(sums, AXES, 0, 0, tiled=True)
    return close(sums, image, krylov_basis, devices * clusters * panels)


def solution(mesh):
    finer = Mesh(mesh.devices.reshape(mesh.shape["role"], 4, 4, 4), AXES)
    split = lambda rank: P(AXES, *([None] * (rank - 1)))
    return jax.shard_map(
        shards,
        mesh=finer,
        in_specs=(
            split(3), split(3), split(2), split(1), split(2), split(1), split(2), split(2), split(2),
            split(2), split(3), split(3), P(), P(), P(None, AXES, None),
        ),
        out_specs=(split(2), P()),
        check_vma=False,
    )
```

```python
import functools

import jax
import jax.numpy as jnp
from jax import lax
from jax.experimental import pallas as pl
from jax.experimental.pallas import tpu as pltpu
from jax.sharding import Mesh
from jax.sharding import PartitionSpec as P

RADIUS = 3
AXES = ("role", "dev_0", "dev_1", "dev_2")
SOFTEN = 0.01
EPSILON = 1e-06
HIGH = lax.Precision.HIGHEST
F32 = jnp.float32
BF16 = jnp.bfloat16
VMEM = pl.BlockSpec(memory_space=pltpu.VMEM)
SMEM = pl.BlockSpec(memory_space=pltpu.SMEM)
ANY = pl.BlockSpec(memory_space=pl.ANY)
HBM = pl.BlockSpec(memory_space=pltpu.HBM)
NT = (((1,), (1,)), ((), ()))
NN = (((1,), (0,)), ((), ()))
HIGHER = 128
ACROSS = 256
UNROLL = 16
MIB = 2**20
PAIRS = 4
DEAD = 1 << 24


def dot(a, b, dims):
    return lax.dot_general(a, b, dims, preferred_element_type=F32)


def halves(value):
    top = value.astype(BF16)
    return top, (value - top.astype(F32)).astype(BF16)


def thirds(value):
    top, rest = value.astype(BF16), None
    rest = value - top.astype(F32)
    middle = rest.astype(BF16)
    return top, middle, (rest - middle.astype(F32)).astype(BF16)


def power(value):
    assert value & (value - 1) == 0
    return value.bit_length() - 1


def window_block(own, ids, clusters, width):
    owner = lax.shift_right_logical(ids, power(clusters))
    shift = (own - owner) & (width - 1)
    same = lax.shift_right_logical(owner, power(width)) == lax.shift_right_logical(own, power(width))
    return jnp.where(same, shift, shift + width - 1), ids & (clusters - 1)


def list_pairs(own, lists_ref, nears_ref, row_ref, off_ref, width):
    clusters = lists_ref.shape[0]

    def list_cluster(c, lengths):
        row, off = lengths
        row_ref[row] = (c << 8) + c

        def list_slot(s, lengths):
            row, off = lengths
            block, inside = window_block(own, lists_ref[c, s], clusters, width)
            pair = (block << 16) + (inside << 8) + c
            near = jnp.where(block < width, 1, 0)
            row_ref[row] = pair
            off_ref[off] = pair - (width << 16)
            return row + near, off + 1 - near

        return lax.fori_loop(0, nears_ref[c], list_slot, (row + 1, off))

    row, off = lax.fori_loop(0, clusters, list_cluster, (jnp.int32(0), jnp.int32(0)))
    for ref, length in ((row_ref, row), (off_ref, off)):
        for k in range(PAIRS):
            ref[length + k] = DEAD
        ref[ref.shape[0] - 1] = length


def source_kernel(
    own_ref, lists_ref, nears_ref, counts_ref,
    basis_hbm, inverse_hbm, maps_hbm, up_hbm, position_hbm, normal_hbm, area_hbm,
    payload_ref, group_ref, density_ref, features_hbm, row_ref, off_ref,
    basis_ref, inverse_ref, maps_ref, up_ref, position_ref, normal_ref, area_ref,
    features_ref, sems, small_sems,
):
    clusters, panels = density_ref.shape
    coeffs = maps_ref.shape[1]
    copies = [
        [pltpu.make_async_copy(a.at[c], b.at[c], sems.at[k, c]) for c in range(clusters)]
        for k, (a, b) in enumerate(((inverse_hbm, inverse_ref), (maps_hbm, maps_ref), (up_hbm, up_ref)))
    ]
    small = [
        pltpu.make_async_copy(a, b, small_sems.at[k])
        for k, (a, b) in enumerate((
            (position_hbm, position_ref), (basis_hbm.at[basis_hbm.shape[0] - 1], basis_ref),
            (normal_hbm, normal_ref), (area_hbm, area_ref)))
    ]
    for copy in small[0:2] + copies[0] + small[2:]:
        copy.start()
    list_pairs(own_ref[0], lists_ref, nears_ref, row_ref, off_ref, 4)
    small[0].wait()
    norm = jnp.zeros((clusters, panels), F32)
    positions = []
    for a in range(3):
        top, rest = halves(position_ref[a])
        positions.append((top.astype(F32), rest.astype(F32)))
        norm += (positions[a][0] + positions[a][1]) * (positions[a][0] + positions[a][1])
    softened = [part.astype(F32) for part in thirds(norm + SOFTEN)]
    one = jnp.ones((1, panels), F32)
    none = jnp.zeros((8, panels), F32)
    for c in range(clusters):
        at = slice(c, c + 1)
        top = [-2.0 * positions[a][0][at] for a in range(3)]
        rest = [-2.0 * positions[a][1][at] for a in range(3)]
        turned = jnp.concatenate(
            top + [one, none[0:4]] + rest + [none[0:5]] + top + [one, none[0:4]] + rest + [none[0:5]]
            + [none[0:3], one, none[0:4]] + [part[at] for part in softened]
            + [none[0:5], jnp.zeros((80, panels), F32)], axis=0
        ).T
        features_ref[c * panels : (c + 1) * panels, :] = turned.astype(BF16)
    features_ref[clusters * panels :, :] = jnp.where(
        lax.broadcasted_iota(jnp.int32, (HIGHER, 128), 1) == 40, 1.0, 0.0
    ).astype(BF16)
    leaving = pltpu.make_async_copy(features_ref, features_hbm, small_sems.at[4])
    leaving.start()
    small[1].wait()
    lane = lax.broadcasted_iota(jnp.int32, (1, panels), 1)
    densities = []
    for c in range(clusters):
        if c % 4 == 0:
            for copy in copies[0][c : c + 4]:
                copy.wait()
            for copy in copies[1 + c // 4]:
                copy.start()
        current = basis_ref[c : c + 1].astype(BF16)
        density = dot(current, inverse_ref[c], NT)
        densities.append(jnp.where(lane < counts_ref[c], density, 0.0).astype(BF16))
    for copy in small[2:]:
        copy.wait()
    wide = jnp.concatenate([d.astype(F32) for d in densities], axis=0)
    density_ref[...] = wide
    scale = area_ref[...] * wide
    weights = [scale * normal_ref[a] for a in range(3)]
    whole = [top + rest for top, rest in positions]
    crossed = sum(whole[a] * weights[a] for a in range(3))
    for k, value in enumerate(whole + [norm] + weights + [crossed]):
        for c in range(clusters):
            payload_ref[c, k : k + 1, :] = value[c : c + 1]
    tails = []
    for c in range(clusters):
        if c % 4 == 0:
            for copy in copies[1][c : c + 4]:
                copy.wait()
        tails.append(dot(densities[c], maps_ref[c], NT).astype(BF16))
    for copy in copies[2]:
        copy.wait()
    total = jnp.zeros((1, coeffs), F32)
    for c in range(clusters):
        total += dot(tails[c], up_ref[c], NT)
        payload_ref[clusters, c : c + 1, 0:coeffs] = tails[c].astype(F32)
        payload_ref[clusters, c : c + 1, coeffs:panels] = jnp.full(
            (1, panels - coeffs), counts_ref[c].astype(F32)
        )
    lines = coeffs // 128
    row = lax.broadcasted_iota(jnp.int32, group_ref.shape, 0) & (lines - 1)
    spread = total[:, 0:128]
    for k in range(1, lines):
        spread = jnp.where(row == k, total[:, 128 * k : 128 * k + 128], spread)
    group_ref[...] = jnp.broadcast_to(spread, group_ref.shape)
    leaving.wait()


def sources(own, lists, nears, counts, basis, inverse, maps, up, positions, normals, areas, devices):
    count, clusters, panels = basis.shape
    coeffs = maps.shape[1]
    lines = devices * coeffs // 128
    pairs = clusters * (lists.shape[1] + 1) + PAIRS + 1
    return pl.pallas_call(
        source_kernel,
        in_specs=[SMEM] * 4 + [HBM] * 7,
        out_specs=[VMEM] * 3 + [HBM] + [SMEM] * 2,
        out_shape=[
            jax.ShapeDtypeStruct((clusters + 1, 8, panels), F32),
            jax.ShapeDtypeStruct((lines, 128), F32),
            jax.ShapeDtypeStruct((clusters, panels), F32),
            jax.ShapeDtypeStruct((clusters * panels + HIGHER, 128), BF16),
            jax.ShapeDtypeStruct((pairs,), jnp.int32),
            jax.ShapeDtypeStruct((pairs,), jnp.int32),
        ],
        scratch_shapes=[
            pltpu.VMEM((clusters, panels), F32),
            pltpu.VMEM(inverse.shape, BF16),
            pltpu.VMEM(maps.shape, BF16),
            pltpu.VMEM(up.shape, BF16),
            pltpu.VMEM(positions.shape, F32),
            pltpu.VMEM(normals.shape, F32),
            pltpu.VMEM(areas.shape, F32),
            pltpu.VMEM((clusters * panels + HIGHER, 128), BF16),
            pltpu.SemaphoreType.DMA((3, clusters)),
            pltpu.SemaphoreType.DMA((5,)),
        ],
        cost_estimate=pl.CostEstimate(flops=4 * 10**8, bytes_accessed=8 * MIB, transcendentals=0),
    )(own, lists, nears, counts, basis, inverse, maps, up, positions, normals, areas)


def near_tiles(
    pairs_ref, counts_ref, tails, window, position_ref,
    tile_list, features, total, squares, ready_list, ready,
):
    clusters = counts_ref.shape[0]
    panels = window.shape[2]
    highs, wides = panels // HIGHER, panels // ACROSS
    shift = lambda value, size: lax.shift_right_logical(value, power(size))
    ready_list()

    def list_some(g, length):
        for k in range(PAIRS):
            pair = pairs_ref[g * PAIRS + k]
            used = pair < DEAD
            pair = jnp.where(used, pair, 0)
            c, local, block = pair & 255, shift(pair, 256) & 255, shift(pair, 65536)
            live = tails[block, local, 0].astype(jnp.int32)
            down = jnp.where(used, shift(live + (ACROSS - 1), ACROSS), 0)
            across = shift(counts_ref[c] + (HIGHER - 1), HIGHER)
            base = ((block * (clusters + 1) + local) << (8 + power(wides))) + c * highs
            for j in reversed(range(highs)):
                for i in reversed(range(wides)):
                    tile_list[length + i * across + j] = base + ((i << 8) + j)
            length = length + down * across
        return length

    pairs = pairs_ref[pairs_ref.shape[0] - 1]
    length = lax.fori_loop(0, shift(pairs + (PAIRS - 1), PAIRS), list_some, jnp.int32(0))
    for extra in range(2 * UNROLL):
        tile_list[length + extra] = clusters * highs

    total[...] = jnp.zeros_like(total)

    def tile(s):
        lane = pl.multiple_of((s & (wides - 1)) * ACROSS, ACROSS)
        return window[lax.shift_right_logical(s, power(wides)), :, pl.ds(lane, ACROSS)]

    def square(at, u):
        spot = tile_list[at]
        top, middle, low = thirds(tile(lax.shift_right_logical(spot, 8)))
        right = jnp.concatenate(
            [top, top, middle, middle, low, jnp.ones((8, ACROSS), BF16), jnp.zeros((80, ACROSS), BF16)],
            axis=0,
        )
        left = features[pl.ds(pl.multiple_of((spot & 255) * HIGHER, HIGHER), HIGHER), :]
        squares[u] = dot(left, right, NN)

    def apply(at, u):
        inverse = lax.rsqrt(squares[u])
        field = (inverse * inverse * inverse).astype(BF16)
        top, rest = halves(tile(lax.shift_right_logical(tile_list[at], 8)))
        return dot(jnp.concatenate([top, rest], axis=0), field, NT)

    ready()
    for u in range(UNROLL):
        square(u, u)

    def step(g, carry):
        results = []
        for u in range(UNROLL):
            results.append((tile_list[g * UNROLL + u] & 255, apply(g * UNROLL + u, u)))
            square((g + 1) * UNROLL + u, u)
        for t, result in results:
            total[t] += result
        return carry

    lax.fori_loop(0, shift(length + (UNROLL - 1), UNROLL), step, 0)

    lines = []
    for c in range(clusters):
        parts = []
        for j in range(highs):
            r = total[c * highs + j]
            r = r[0:8] + r[8:16]
            x = position_ref[c, 0:3, j * HIGHER : (j + 1) * HIGHER]
            parts.append(jnp.sum(x * r[4:7], axis=0, keepdims=True) - r[7:8])
        lines.append(jnp.concatenate(parts, axis=1))
    return jnp.concatenate(lines, axis=0)


def near_scratch(clusters, slots, panels, blocks):
    highs, wides = panels // HIGHER, panels // ACROSS
    most = clusters * slots * highs * wides + 4 * UNROLL
    return [
        pltpu.SMEM((most,), jnp.int32),
        pltpu.VMEM((clusters * panels + HIGHER, 128), BF16),
        pltpu.SemaphoreType.DMA,
        pltpu.VMEM((clusters * highs + 1, 16, HIGHER), F32),
        pltpu.VMEM((UNROLL, HIGHER, ACROSS), F32),
        pltpu.VMEM((blocks * (clusters + 1), 8, panels), F32),
        pltpu.SMEM((blocks, clusters, 128), F32),
    ]


def row_kernel(pairs_ref, counts_ref, features_hbm, a_ref, b_ref, c_ref, d_ref, out_ref,
               tile_list, features, feature_sem, total, squares, window, tails, sems):
    clusters = counts_ref.shape[0]
    blocks = (a_ref, b_ref, c_ref, d_ref)
    coeffs = window.shape[2] // 2
    copies = []
    for k, block in enumerate(blocks):
        copies.append(pltpu.make_async_copy(
            block, window.at[pl.ds(k * (clusters + 1), clusters + 1)], sems.at[0, k]))
        copies.append(pltpu.make_async_copy(
            block.at[clusters, :, pl.ds(coeffs, 128)], tails.at[k], sems.at[1, k]))
    first, then = copies[1::2], copies[0::2]
    then.append(pltpu.make_async_copy(features_hbm, features, feature_sem))

    def wait(group):
        for copy in group:
            copy.wait()

    for copy in first + then:
        copy.start()
    out_ref[...] = near_tiles(
        pairs_ref, counts_ref, tails, window, window, tile_list, features, total, squares,
        lambda: wait(first), lambda: wait(then),
    )


def row_fields(pairs, counts, features, slots, blocks):
    clusters = counts.shape[0]
    panels = blocks[0].shape[2]
    return pl.pallas_call(
        row_kernel,
        in_specs=[SMEM] * 2 + [ANY] * (1 + len(blocks)),
        out_specs=VMEM,
        out_shape=jax.ShapeDtypeStruct((clusters, panels), F32),
        scratch_shapes=near_scratch(clusters, slots + 1, panels, len(blocks))
        + [pltpu.SemaphoreType.DMA((2, len(blocks)))],
        cost_estimate=pl.CostEstimate(flops=3 * 10**9, bytes_accessed=MIB, transcendentals=10**6),
    )(pairs, counts, features, *blocks)


def late_kernel(
    own_ref, pairs_ref, counts_ref, leaf_ids_ref, leaf_kinds_ref, group_ids_ref,
    group_kinds_ref, groups_ref, density_ref, near_ref, basis_ref, features_hbm, far_hbm, up_hbm, maps_hbm,
    a_ref, b_ref, c_ref, d_ref, e_ref, f_ref, g_ref,
    image_ref, sums_ref,
    tile_list, features, feature_sem, total, squares, window, tails, sems,
    far_ref, up_ref, maps_ref, own_rows, moments, weight_sems,
):
    clusters, panels = density_ref.shape
    kinds, coeffs = far_ref.shape[1], far_ref.shape[2]
    row, others = (a_ref, b_ref, c_ref, d_ref), (e_ref, f_ref, g_ref)
    copies = []
    for k, block in enumerate(others):
        copies.append(pltpu.make_async_copy(
            block, window.at[pl.ds(k * (clusters + 1), clusters + 1)], sems.at[0, k]))
        copies.append(pltpu.make_async_copy(
            block.at[clusters, :, pl.ds(coeffs, 128)], tails.at[k], sems.at[1, k]))
    copies.append(pltpu.make_async_copy(a_ref, own_rows, weight_sems.at[3]))
    first, then = copies[1::2], copies[0:-1:2] + copies[-1:]
    then.append(pltpu.make_async_copy(features_hbm, features, feature_sem))

    def wait(group):
        for copy in group:
            copy.wait()

    for copy in first + then:
        copy.start()
    later = [
        pltpu.make_async_copy(block.at[clusters, :, pl.ds(0, coeffs)],
                              moments.at[pl.ds(k * clusters, clusters)], sems.at[2, k])
        for k, block in enumerate(row + others)
    ]
    weights = [
        pltpu.make_async_copy(far_hbm, far_ref, weight_sems.at[0]),
        pltpu.make_async_copy(up_hbm, up_ref, weight_sems.at[1]),
        pltpu.make_async_copy(maps_hbm, maps_ref, weight_sems.at[2]),
    ]
    weights[0].start()
    own = own_ref[0]

    def arrived():
        wait(then)
        for copy in later + weights[1:]:
            copy.start()

    near = near_ref[...] + near_tiles(
        pairs_ref, counts_ref, tails, window, own_rows, tile_list, features, total, squares,
        lambda: wait(first), arrived,
    )
    for copy in later:
        copy.wait()

    lines = coeffs // 128
    spots = groups_ref.shape[0]
    kind = lax.broadcasted_iota(jnp.int32, (kinds, 1), 0)
    spot = lax.broadcasted_iota(jnp.int32, (1, spots), 1)
    pick = jnp.zeros((kinds, spots), F32)
    for n in range(group_ids_ref.shape[1]):
        hit = (kind == group_kinds_ref[0, n]) & (
            lax.shift_right_logical(spot, power(lines)) == group_ids_ref[0, n])
        pick += jnp.where(hit, 1.0, 0.0)
    pick = jnp.concatenate(
        [jnp.where((spot & (lines - 1)) == k, pick, 0.0) for k in range(lines)], axis=0
    ).astype(BF16)
    group_sum = sum(dot(pick, part, NN) for part in thirds(groups_ref[...]))
    group_sum = jnp.concatenate(
        [group_sum[k * kinds : (k + 1) * kinds] for k in range(lines)], axis=1
    )
    local = jnp.zeros((24, coeffs), F32)
    weights[0].wait()
    group_rows = jnp.concatenate([part.astype(F32) for part in thirds(group_sum)], axis=0)
    row24 = lax.broadcasted_iota(jnp.int32, (24, 1), 0) & (kinds - 1)
    for o in range(kinds):
        local += dot(jnp.where(row24 == o, group_rows, 0.0).astype(BF16), far_ref[1, o], NT)
    local = jnp.sum(local, axis=0, keepdims=True).astype(BF16)

    block, inside = window_block(own, leaf_ids_ref[...], clusters, 4)
    spots_of = block * clusters + inside
    spot = lax.broadcasted_iota(jnp.int32, (1, moments.shape[0]), 1)
    picks = [jnp.zeros((clusters, moments.shape[0]), F32) for _ in range(kinds)]
    for n in range(leaf_ids_ref.shape[1]):
        hit = jnp.where(spots_of[:, n : n + 1] == spot, 1.0, 0.0)
        for o in range(kinds):
            picks[o] += jnp.where(leaf_kinds_ref[:, n : n + 1] == o, hit, 0.0)
    leaf_sum = dot(
        jnp.concatenate(picks, axis=0).astype(BF16), moments[...].astype(BF16), NN
    )
    leaf = jnp.zeros((2 * clusters, coeffs), F32)
    for o in range(kinds):
        top, rest = halves(leaf_sum[o * clusters : (o + 1) * clusters])
        leaf += dot(jnp.concatenate([top, rest], axis=0), far_ref[0, o], NT)
    leaf = leaf[0:clusters] + leaf[clusters:]
    weights[1].wait()
    leaf += jnp.concatenate([dot(local, up_ref[c], NN) for c in range(clusters)], axis=0)
    leaf = leaf.astype(BF16)
    weights[2].wait()
    images = []
    lane = lax.broadcasted_iota(jnp.int32, (1, panels), 1)
    for c in range(clusters):
        far = dot(leaf[c : c + 1], maps_ref[c], NN)
        value = 0.5 * density_ref[c : c + 1] + near[c : c + 1] + far
        images.append(jnp.where(lane < counts_ref[c], value, 0.0))
    image = jnp.concatenate(images, axis=0)
    image_ref[...] = image
    lane = lax.broadcasted_iota(jnp.int32, (1, 128), 1)
    sums = jnp.zeros((1, 128), F32)
    for k in range(basis_ref.shape[0] + 1):
        other = basis_ref[k] if k < basis_ref.shape[0] else image
        value = jnp.sum(jnp.sum(image * other, axis=0, keepdims=True), axis=1, keepdims=True)
        sums += jnp.where(lane == k, value, 0.0)
    sums_ref[...] = jnp.broadcast_to(sums, sums_ref.shape)


def late_fields(own, pairs, counts, slots, leaf_ids, leaf_kinds, group_ids, group_kinds, groups,
                density, near, basis, features, far, up, maps, window, devices):
    clusters, panels = density.shape
    return pl.pallas_call(
        late_kernel,
        in_specs=[SMEM] * 3 + [VMEM] * 2 + [SMEM] * 2 + [VMEM] * 4 + [ANY] + [HBM] * 3 + [ANY] * 7,
        out_specs=[VMEM, VMEM],
        out_shape=[
            jax.ShapeDtypeStruct(density.shape, F32),
            jax.ShapeDtypeStruct((devices, 128), F32),
        ],
        scratch_shapes=near_scratch(clusters, slots + 1, panels, 3)
        + [
            pltpu.SemaphoreType.DMA((3, 7)),
            pltpu.VMEM(far.shape, BF16),
            pltpu.VMEM(up.shape, BF16),
            pltpu.VMEM(maps.shape, BF16),
            pltpu.VMEM((clusters + 1, 8, panels), F32),
            pltpu.VMEM((7 * clusters, maps.shape[1]), F32),
            pltpu.SemaphoreType.DMA((4,)),
        ],
        cost_estimate=pl.CostEstimate(flops=3 * 10**9, bytes_accessed=MIB, transcendentals=10**6),
    )(own, pairs, counts, leaf_ids, leaf_kinds, group_ids, group_kinds, groups, density,
      near, basis, features, far, up, maps, *window)


def close_kernel(rows, sums_ref, image_hbm, basis_ref, next_ref, column_ref, image_ref, sem):
    copy = pltpu.make_async_copy(image_hbm, image_ref, sem)
    copy.start()
    count = basis_ref.shape[0]
    means = jnp.sum(sums_ref[...], axis=0, keepdims=True) * (1.0 / rows)
    lane = lax.broadcasted_iota(jnp.int32, (1, 128), 1)
    coeffs = jnp.where(lane < count, means, 0.0)
    square = jnp.sum(jnp.where(lane == count, means, 0.0), axis=1, keepdims=True)
    energy = square - jnp.sum(coeffs * coeffs, axis=1, keepdims=True)
    height = jnp.sqrt(energy + EPSILON)
    copy.wait()
    remainder = image_ref[...]
    for k in range(count):
        remainder = remainder - coeffs[:, k : k + 1] * basis_ref[k]
        column_ref[k] = means[0, k]
    column_ref[count] = height[0, 0]
    next_ref[...] = remainder / height


def close(sums, image, basis, rows):
    return pl.pallas_call(
        functools.partial(close_kernel, rows),
        in_specs=[VMEM, HBM, VMEM],
        out_specs=[VMEM, SMEM],
        out_shape=[
            jax.ShapeDtypeStruct(image.shape, F32),
            jax.ShapeDtypeStruct((basis.shape[0] + 1,), F32),
        ],
        scratch_shapes=[pltpu.VMEM(image.shape, F32), pltpu.SemaphoreType.DMA],
        compiler_params=pltpu.CompilerParams(vmem_limit_bytes=2 * MIB),
    )(sums, image, basis)


def row_routes(rows, width):
    spot = lambda r, y: (r % rows) * width + y
    turns = {1: (1, -1, -1, -1), 2: (1, 1, -1, -1), 3: (1, 1, 1, -1)}
    return {
        k: [(spot(r, y), spot(r + turns[k][y], y)) for r in range(rows) for y in range(width)]
        for k in turns
    }


def shards(
    positions, normals, panel_areas, panel_counts, near_lists, near_counts, leaf_lists, leaf_kinds,
    group_lists, group_kinds, block_inverse, moment_maps, up_operators, far_operators, krylov_basis,
):
    clusters, _, panels = positions.shape
    coeffs = moment_maps.shape[1]
    devices = lax.axis_size(AXES)
    width = lax.axis_size(AXES[-1])
    own = jnp.full((1,), lax.axis_index(AXES), jnp.int32)
    payload, group, density, features, row_pairs, off_pairs = sources(
        own, near_lists, near_counts, panel_counts, krylov_basis, block_inverse, moment_maps, up_operators,
        positions.transpose(1, 0, 2), normals.transpose(1, 0, 2), panel_areas, devices,
    )
    row = [payload] + [
        lax.ppermute(payload, AXES[-1], [(y, (y + k) % width) for y in range(width)])
        for k in range(1, width)
    ]
    routes = row_routes(devices // width, width)
    window = row + [lax.ppermute(row[k], AXES, routes[k]) for k in range(1, width)]
    groups = lax.all_to_all(group, AXES, 0, 0, tiled=True)
    slots = near_lists.shape[1]
    near = row_fields(row_pairs, panel_counts, features, slots, row)
    image, sums = late_fields(
        own, off_pairs, panel_counts, slots, leaf_lists, leaf_kinds, group_lists, group_kinds,
        groups, density, near, krylov_basis, features, far_operators, up_operators, moment_maps, window, devices,
    )
    sums = lax.all_to_all(sums, AXES, 0, 0, tiled=True)
    return close(sums, image, krylov_basis, devices * clusters * panels)


def solution(mesh):
    finer = Mesh(mesh.devices.reshape(mesh.shape["role"], 4, 4, 4), AXES)
    split = lambda rank: P(AXES, *([None] * (rank - 1)))
    return jax.shard_map(
        shards,
        mesh=finer,
        in_specs=(
            split(3), split(3), split(2), split(1), split(2), split(1), split(2), split(2), split(2),
            split(2), split(3), split(3), P(), P(), P(None, AXES, None),
        ),
        out_specs=(split(2), P()),
        check_vma=False,
    )
```

```python
import functools

import jax
import jax.numpy as jnp
from jax import lax
from jax.experimental import pallas as pl
from jax.experimental.pallas import tpu as pltpu
from jax.sharding import Mesh
from jax.sharding import PartitionSpec as P

RADIUS = 3
AXES = ("role", "dev_0", "dev_1", "dev_2")
SOFTEN = 0.01
EPSILON = 1e-06
HIGH = lax.Precision.HIGHEST
F32 = jnp.float32
BF16 = jnp.bfloat16
VMEM = pl.BlockSpec(memory_space=pltpu.VMEM)
SMEM = pl.BlockSpec(memory_space=pltpu.SMEM)
ANY = pl.BlockSpec(memory_space=pl.ANY)
HBM = pl.BlockSpec(memory_space=pltpu.HBM)
NT = (((1,), (1,)), ((), ()))
NN = (((1,), (0,)), ((), ()))
HIGHER = 128
ACROSS = 256
UNROLL = 16
MIB = 2**20
PAIRS = 4
DEAD = 1 << 24


def dot(a, b, dims):
    return lax.dot_general(a, b, dims, preferred_element_type=F32)


def halves(value):
    top = value.astype(BF16)
    return top, (value - top.astype(F32)).astype(BF16)


def thirds(value):
    top, rest = value.astype(BF16), None
    rest = value - top.astype(F32)
    middle = rest.astype(BF16)
    return top, middle, (rest - middle.astype(F32)).astype(BF16)


def power(value):
    assert value & (value - 1) == 0
    return value.bit_length() - 1


def window_block(own, ids, clusters, width):
    owner = lax.shift_right_logical(ids, power(clusters))
    shift = (own - owner) & (width - 1)
    same = lax.shift_right_logical(owner, power(width)) == lax.shift_right_logical(own, power(width))
    return jnp.where(same, shift, shift + width - 1), ids & (clusters - 1)


def list_pairs(own, lists_ref, nears_ref, row_ref, off_ref, width):
    clusters = lists_ref.shape[0]

    def list_cluster(c, lengths):
        row, off = lengths
        row_ref[row] = (c << 8) + c

        def list_slot(s, lengths):
            row, off = lengths
            block, inside = window_block(own, lists_ref[c, s], clusters, width)
            pair = (block << 16) + (inside << 8) + c
            near = jnp.where(block < width, 1, 0)
            row_ref[row] = pair
            off_ref[off] = pair - (width << 16)
            return row + near, off + 1 - near

        return lax.fori_loop(0, nears_ref[c], list_slot, (row + 1, off))

    row, off = lax.fori_loop(0, clusters, list_cluster, (jnp.int32(0), jnp.int32(0)))
    for ref, length in ((row_ref, row), (off_ref, off)):
        for k in range(PAIRS):
            ref[length + k] = DEAD
        ref[ref.shape[0] - 1] = length


def source_kernel(
    own_ref, lists_ref, nears_ref, counts_ref,
    basis_hbm, inverse_hbm, maps_hbm, up_hbm, position_hbm, normal_hbm, area_hbm,
    payload_ref, group_ref, density_ref, features_hbm, row_ref, off_ref,
    basis_ref, inverse_ref, maps_ref, up_ref, position_ref, normal_ref, area_ref,
    features_ref, sems, small_sems,
):
    clusters, panels = density_ref.shape
    coeffs = maps_ref.shape[1]
    copies = [
        [pltpu.make_async_copy(a.at[c], b.at[c], sems.at[k, c]) for c in range(clusters)]
        for k, (a, b) in enumerate(((inverse_hbm, inverse_ref), (maps_hbm, maps_ref), (up_hbm, up_ref)))
    ]
    small = [
        pltpu.make_async_copy(a, b, small_sems.at[k])
        for k, (a, b) in enumerate((
            (position_hbm, position_ref), (basis_hbm.at[basis_hbm.shape[0] - 1], basis_ref),
            (normal_hbm, normal_ref), (area_hbm, area_ref)))
    ]
    for copy in small[0:2] + copies[0] + small[2:]:
        copy.start()
    list_pairs(own_ref[0], lists_ref, nears_ref, row_ref, off_ref, 4)
    small[0].wait()
    norm = jnp.zeros((clusters, panels), F32)
    positions = []
    for a in range(3):
        top, rest = halves(position_ref[a])
        positions.append((top.astype(F32), rest.astype(F32)))
        norm += (positions[a][0] + positions[a][1]) * (positions[a][0] + positions[a][1])
    softened = [part.astype(F32) for part in thirds(norm + SOFTEN)]
    one = jnp.ones((1, panels), F32)
    none = jnp.zeros((8, panels), F32)
    for c in range(clusters):
        at = slice(c, c + 1)
        top = [-2.0 * positions[a][0][at] for a in range(3)]
        rest = [-2.0 * positions[a][1][at] for a in range(3)]
        turned = jnp.concatenate(
            top + [one, none[0:4]] + rest + [none[0:5]] + top + [one, none[0:4]] + rest + [none[0:5]]
            + [none[0:3], one, none[0:4]] + [part[at] for part in softened]
            + [none[0:5], jnp.zeros((80, panels), F32)], axis=0
        ).T
        features_ref[c * panels : (c + 1) * panels, :] = turned.astype(BF16)
    features_ref[clusters * panels :, :] = jnp.where(
        lax.broadcasted_iota(jnp.int32, (HIGHER, 128), 1) == 40, 1.0, 0.0
    ).astype(BF16)
    leaving = pltpu.make_async_copy(features_ref, features_hbm, small_sems.at[4])
    leaving.start()
    small[1].wait()
    lane = lax.broadcasted_iota(jnp.int32, (1, panels), 1)
    densities = []
    for c in range(clusters):
        if c % 4 == 0:
            for copy in copies[0][c : c + 4]:
                copy.wait()
            for copy in copies[1 + c // 4]:
                copy.start()
        current = basis_ref[c : c + 1].astype(BF16)
        density = dot(current, inverse_ref[c], NT)
        densities.append(jnp.where(lane < counts_ref[c], density, 0.0).astype(BF16))
    for copy in small[2:]:
        copy.wait()
    wide = jnp.concatenate([d.astype(F32) for d in densities], axis=0)
    density_ref[...] = wide
    scale = area_ref[...] * wide
    weights = [scale * normal_ref[a] for a in range(3)]
    whole = [top + rest for top, rest in positions]
    crossed = sum(whole[a] * weights[a] for a in range(3))
    for k, value in enumerate(whole + [norm] + weights + [crossed]):
        for c in range(clusters):
            payload_ref[c, k : k + 1, :] = value[c : c + 1]
    tails = []
    for c in range(clusters):
        if c % 4 == 0:
            for copy in copies[1][c : c + 4]:
                copy.wait()
        tails.append(dot(densities[c], maps_ref[c], NT).astype(BF16))
    for copy in copies[2]:
        copy.wait()
    total = jnp.zeros((1, coeffs), F32)
    for c in range(clusters):
        total += dot(tails[c], up_ref[c], NT)
        payload_ref[clusters, c : c + 1, 0:coeffs] = tails[c].astype(F32)
        payload_ref[clusters, c : c + 1, coeffs:panels] = jnp.full(
            (1, panels - coeffs), counts_ref[c].astype(F32)
        )
    lines = coeffs // 128
    row = lax.broadcasted_iota(jnp.int32, group_ref.shape, 0) & (lines - 1)
    spread = total[:, 0:128]
    for k in range(1, lines):
        spread = jnp.where(row == k, total[:, 128 * k : 128 * k + 128], spread)
    group_ref[...] = jnp.broadcast_to(spread, group_ref.shape)
    leaving.wait()


def sources(own, lists, nears, counts, basis, inverse, maps, up, positions, normals, areas, devices):
    count, clusters, panels = basis.shape
    coeffs = maps.shape[1]
    lines = devices * coeffs // 128
    pairs = clusters * (lists.shape[1] + 1) + PAIRS + 1
    return pl.pallas_call(
        source_kernel,
        in_specs=[SMEM] * 4 + [HBM] * 7,
        out_specs=[VMEM] * 3 + [HBM] + [SMEM] * 2,
        out_shape=[
            jax.ShapeDtypeStruct((clusters + 1, 8, panels), F32),
            jax.ShapeDtypeStruct((lines, 128), F32),
            jax.ShapeDtypeStruct((clusters, panels), F32),
            jax.ShapeDtypeStruct((clusters * panels + HIGHER, 128), BF16),
            jax.ShapeDtypeStruct((pairs,), jnp.int32),
            jax.ShapeDtypeStruct((pairs,), jnp.int32),
        ],
        scratch_shapes=[
            pltpu.VMEM((clusters, panels), F32),
            pltpu.VMEM(inverse.shape, BF16),
            pltpu.VMEM(maps.shape, BF16),
            pltpu.VMEM(up.shape, BF16),
            pltpu.VMEM(positions.shape, F32),
            pltpu.VMEM(normals.shape, F32),
            pltpu.VMEM(areas.shape, F32),
            pltpu.VMEM((clusters * panels + HIGHER, 128), BF16),
            pltpu.SemaphoreType.DMA((3, clusters)),
            pltpu.SemaphoreType.DMA((5,)),
        ],
        cost_estimate=pl.CostEstimate(flops=4 * 10**8, bytes_accessed=8 * MIB, transcendentals=0),
    )(own, lists, nears, counts, basis, inverse, maps, up, positions, normals, areas)


def near_tiles(
    pairs_ref, counts_ref, tails, window, position_ref,
    tile_list, features, total, squares, ready_list, ready,
):
    clusters = counts_ref.shape[0]
    panels = window.shape[2]
    highs, wides = panels // HIGHER, panels // ACROSS
    shift = lambda value, size: lax.shift_right_logical(value, power(size))
    ready_list()

    def list_some(g, length):
        for k in range(PAIRS):
            pair = pairs_ref[g * PAIRS + k]
            used = pair < DEAD
            pair = jnp.where(used, pair, 0)
            c, local, block = pair & 255, shift(pair, 256) & 255, shift(pair, 65536)
            live = tails[block, local, 0].astype(jnp.int32)
            down = jnp.where(used, shift(live + (ACROSS - 1), ACROSS), 0)
            across = shift(counts_ref[c] + (HIGHER - 1), HIGHER)
            base = ((block * (clusters + 1) + local) << (8 + power(wides))) + c * highs
            for j in reversed(range(highs)):
                for i in reversed(range(wides)):
                    tile_list[length + i * across + j] = base + ((i << 8) + j)
            length = length + down * across
        return length

    pairs = pairs_ref[pairs_ref.shape[0] - 1]
    length = lax.fori_loop(0, shift(pairs + (PAIRS - 1), PAIRS), list_some, jnp.int32(0))
    for extra in range(2 * UNROLL):
        tile_list[length + extra] = clusters * highs

    total[...] = jnp.zeros_like(total)

    def tile(s):
        lane = pl.multiple_of((s & (wides - 1)) * ACROSS, ACROSS)
        return window[lax.shift_right_logical(s, power(wides)), :, pl.ds(lane, ACROSS)]

    def square(at, u):
        spot = tile_list[at]
        top, middle, low = thirds(tile(lax.shift_right_logical(spot, 8)))
        right = jnp.concatenate(
            [top, top, middle, middle, low, jnp.ones((8, ACROSS), BF16), jnp.zeros((80, ACROSS), BF16)],
            axis=0,
        )
        left = features[pl.ds(pl.multiple_of((spot & 255) * HIGHER, HIGHER), HIGHER), :]
        squares[u] = dot(left, right, NN)

    def apply(at, u):
        inverse = lax.rsqrt(squares[u])
        field = (inverse * inverse * inverse).astype(BF16)
        top, rest = halves(tile(lax.shift_right_logical(tile_list[at], 8)))
        return dot(jnp.concatenate([top, rest], axis=0), field, NT)

    ready()
    for u in range(UNROLL):
        square(u, u)

    def step(g, carry):
        results = []
        for u in range(UNROLL):
            results.append((tile_list[g * UNROLL + u] & 255, apply(g * UNROLL + u, u)))
            square((g + 1) * UNROLL + u, u)
        for t, result in results:
            total[t] += result
        return carry

    lax.fori_loop(0, shift(length + (UNROLL - 1), UNROLL), step, 0)

    lines = []
    for c in range(clusters):
        parts = []
        for j in range(highs):
            r = total[c * highs + j]
            r = r[0:8] + r[8:16]
            x = position_ref[c, 0:3, j * HIGHER : (j + 1) * HIGHER]
            parts.append(jnp.sum(x * r[4:7], axis=0, keepdims=True) - r[7:8])
        lines.append(jnp.concatenate(parts, axis=1))
    return jnp.concatenate(lines, axis=0)


def near_scratch(clusters, slots, panels, blocks):
    highs, wides = panels // HIGHER, panels // ACROSS
    most = clusters * slots * highs * wides + 4 * UNROLL
    return [
        pltpu.SMEM((most,), jnp.int32),
        pltpu.VMEM((clusters * panels + HIGHER, 128), BF16),
        pltpu.SemaphoreType.DMA,
        pltpu.VMEM((clusters * highs + 1, 16, HIGHER), F32),
        pltpu.VMEM((UNROLL, HIGHER, ACROSS), F32),
        pltpu.VMEM((blocks * (clusters + 1), 8, panels), F32),
        pltpu.SMEM((blocks, clusters, 128), F32),
    ]


def row_kernel(pairs_ref, counts_ref, features_hbm, a_ref, b_ref, c_ref, d_ref, out_ref,
               tile_list, features, feature_sem, total, squares, window, tails, sems):
    clusters = counts_ref.shape[0]
    blocks = (a_ref, b_ref, c_ref, d_ref)
    coeffs = window.shape[2] // 2
    copies = []
    for k, block in enumerate(blocks):
        copies.append(pltpu.make_async_copy(
            block, window.at[pl.ds(k * (clusters + 1), clusters + 1)], sems.at[0, k]))
        copies.append(pltpu.make_async_copy(
            block.at[clusters, :, pl.ds(coeffs, 128)], tails.at[k], sems.at[1, k]))
    first, then = copies[1::2], copies[0::2]
    then.append(pltpu.make_async_copy(features_hbm, features, feature_sem))

    def wait(group):
        for copy in group:
            copy.wait()

    for copy in first + then:
        copy.start()
    out_ref[...] = near_tiles(
        pairs_ref, counts_ref, tails, window, window, tile_list, features, total, squares,
        lambda: wait(first), lambda: wait(then),
    )


def row_fields(pairs, counts, features, slots, blocks):
    clusters = counts.shape[0]
    panels = blocks[0].shape[2]
    return pl.pallas_call(
        row_kernel,
        in_specs=[SMEM] * 2 + [ANY] * (1 + len(blocks)),
        out_specs=VMEM,
        out_shape=jax.ShapeDtypeStruct((clusters, panels), F32),
        scratch_shapes=near_scratch(clusters, slots + 1, panels, len(blocks))
        + [pltpu.SemaphoreType.DMA((2, len(blocks)))],
        cost_estimate=pl.CostEstimate(flops=3 * 10**9, bytes_accessed=MIB, transcendentals=10**6),
    )(pairs, counts, features, *blocks)


def late_kernel(
    own_ref, pairs_ref, counts_ref, leaf_ids_ref, leaf_kinds_ref, group_ids_ref,
    group_kinds_ref, groups_ref, density_ref, near_ref, basis_ref, features_hbm, far_hbm, up_hbm, maps_hbm,
    a_ref, b_ref, c_ref, d_ref, e_ref, f_ref, g_ref,
    image_ref, sums_ref,
    tile_list, features, feature_sem, total, squares, window, tails, sems,
    far_ref, up_ref, maps_ref, own_rows, moments, weight_sems,
):
    clusters, panels = density_ref.shape
    kinds, coeffs = far_ref.shape[1], far_ref.shape[2]
    row, others = (a_ref, b_ref, c_ref, d_ref), (e_ref, f_ref, g_ref)
    copies = []
    for k, block in enumerate(others):
        copies.append(pltpu.make_async_copy(
            block, window.at[pl.ds(k * (clusters + 1), clusters + 1)], sems.at[0, k]))
        copies.append(pltpu.make_async_copy(
            block.at[clusters, :, pl.ds(coeffs, 128)], tails.at[k], sems.at[1, k]))
    copies.append(pltpu.make_async_copy(a_ref, own_rows, weight_sems.at[3]))
    first, then = copies[1::2], copies[0:-1:2] + copies[-1:]
    then.append(pltpu.make_async_copy(features_hbm, features, feature_sem))

    def wait(group):
        for copy in group:
            copy.wait()

    for copy in first + then:
        copy.start()
    later = [
        pltpu.make_async_copy(block.at[clusters, :, pl.ds(0, coeffs)],
                              moments.at[pl.ds(k * clusters, clusters)], sems.at[2, k])
        for k, block in enumerate(row + others)
    ]
    weights = [
        pltpu.make_async_copy(far_hbm, far_ref, weight_sems.at[0]),
        pltpu.make_async_copy(up_hbm, up_ref, weight_sems.at[1]),
        pltpu.make_async_copy(maps_hbm, maps_ref, weight_sems.at[2]),
    ]
    weights[0].start()
    own = own_ref[0]

    def arrived():
        wait(then)
        for copy in later + weights[1:]:
            copy.start()

    near = near_ref[...] + near_tiles(
        pairs_ref, counts_ref, tails, window, own_rows, tile_list, features, total, squares,
        lambda: wait(first), arrived,
    )
    for copy in later:
        copy.wait()

    lines = coeffs // 128
    spots = groups_ref.shape[0]
    kind = lax.broadcasted_iota(jnp.int32, (kinds, 1), 0)
    spot = lax.broadcasted_iota(jnp.int32, (1, spots), 1)
    pick = jnp.zeros((kinds, spots), F32)
    for n in range(group_ids_ref.shape[1]):
        hit = (kind == group_kinds_ref[0, n]) & (
            lax.shift_right_logical(spot, power(lines)) == group_ids_ref[0, n])
        pick += jnp.where(hit, 1.0, 0.0)
    pick = jnp.concatenate(
        [jnp.where((spot & (lines - 1)) == k, pick, 0.0) for k in range(lines)], axis=0
    ).astype(BF16)
    group_sum = sum(dot(pick, part, NN) for part in thirds(groups_ref[...]))
    group_sum = jnp.concatenate(
        [group_sum[k * kinds : (k + 1) * kinds] for k in range(lines)], axis=1
    )
    local = jnp.zeros((24, coeffs), F32)
    weights[0].wait()
    group_rows = jnp.concatenate([part.astype(F32) for part in thirds(group_sum)], axis=0)
    row24 = lax.broadcasted_iota(jnp.int32, (24, 1), 0) & (kinds - 1)
    for o in range(kinds):
        local += dot(jnp.where(row24 == o, group_rows, 0.0).astype(BF16), far_ref[1, o], NT)
    local = jnp.sum(local, axis=0, keepdims=True).astype(BF16)

    block, inside = window_block(own, leaf_ids_ref[...], clusters, 4)
    spots_of = block * clusters + inside
    spot = lax.broadcasted_iota(jnp.int32, (1, moments.shape[0]), 1)
    picks = [jnp.zeros((clusters, moments.shape[0]), F32) for _ in range(kinds)]
    for n in range(leaf_ids_ref.shape[1]):
        hit = jnp.where(spots_of[:, n : n + 1] == spot, 1.0, 0.0)
        for o in range(kinds):
            picks[o] += jnp.where(leaf_kinds_ref[:, n : n + 1] == o, hit, 0.0)
    leaf_sum = dot(
        jnp.concatenate(picks, axis=0).astype(BF16), moments[...].astype(BF16), NN
    )
    leaf = jnp.zeros((2 * clusters, coeffs), F32)
    for o in range(kinds):
        top, rest = halves(leaf_sum[o * clusters : (o + 1) * clusters])
        leaf += dot(jnp.concatenate([top, rest], axis=0), far_ref[0, o], NT)
    leaf = leaf[0:clusters] + leaf[clusters:]
    weights[1].wait()
    leaf += jnp.concatenate([dot(local, up_ref[c], NN) for c in range(clusters)], axis=0)
    leaf = leaf.astype(BF16)
    weights[2].wait()
    images = []
    lane = lax.broadcasted_iota(jnp.int32, (1, panels), 1)
    for c in range(clusters):
        far = dot(leaf[c : c + 1], maps_ref[c], NN)
        value = 0.5 * density_ref[c : c + 1] + near[c : c + 1] + far
        images.append(jnp.where(lane < counts_ref[c], value, 0.0))
    image = jnp.concatenate(images, axis=0)
    image_ref[...] = image
    lane = lax.broadcasted_iota(jnp.int32, (1, 128), 1)
    sums = jnp.zeros((1, 128), F32)
    for k in range(basis_ref.shape[0] + 1):
        other = basis_ref[k] if k < basis_ref.shape[0] else image
        value = jnp.sum(jnp.sum(image * other, axis=0, keepdims=True), axis=1, keepdims=True)
        sums += jnp.where(lane == k, value, 0.0)
    sums_ref[...] = jnp.broadcast_to(sums, sums_ref.shape)


def late_fields(own, pairs, counts, slots, leaf_ids, leaf_kinds, group_ids, group_kinds, groups,
                density, near, basis, features, far, up, maps, window, devices):
    clusters, panels = density.shape
    return pl.pallas_call(
        late_kernel,
        in_specs=[SMEM] * 3 + [VMEM] * 2 + [SMEM] * 2 + [VMEM] * 4 + [ANY] + [HBM] * 3 + [ANY] * 7,
        out_specs=[VMEM, VMEM],
        out_shape=[
            jax.ShapeDtypeStruct(density.shape, F32),
            jax.ShapeDtypeStruct((devices, 128), F32),
        ],
        scratch_shapes=near_scratch(clusters, slots + 1, panels, 3)
        + [
            pltpu.SemaphoreType.DMA((3, 7)),
            pltpu.VMEM(far.shape, BF16),
            pltpu.VMEM(up.shape, BF16),
            pltpu.VMEM(maps.shape, BF16),
            pltpu.VMEM((clusters + 1, 8, panels), F32),
            pltpu.VMEM((7 * clusters, maps.shape[1]), F32),
            pltpu.SemaphoreType.DMA((4,)),
        ],
        compiler_params=pltpu.CompilerParams(vmem_limit_bytes=56 * 10**6),
        cost_estimate=pl.CostEstimate(flops=3 * 10**9, bytes_accessed=MIB, transcendentals=10**6),
    )(own, pairs, counts, leaf_ids, leaf_kinds, group_ids, group_kinds, groups, density,
      near, basis, features, far, up, maps, *window)


def close_kernel(rows, sums_ref, image_hbm, basis_ref, next_ref, column_ref, image_ref, sem):
    copy = pltpu.make_async_copy(image_hbm, image_ref, sem)
    copy.start()
    count = basis_ref.shape[0]
    means = jnp.sum(sums_ref[...], axis=0, keepdims=True) * (1.0 / rows)
    lane = lax.broadcasted_iota(jnp.int32, (1, 128), 1)
    coeffs = jnp.where(lane < count, means, 0.0)
    square = jnp.sum(jnp.where(lane == count, means, 0.0), axis=1, keepdims=True)
    energy = square - jnp.sum(coeffs * coeffs, axis=1, keepdims=True)
    height = jnp.sqrt(energy + EPSILON)
    copy.wait()
    remainder = image_ref[...]
    for k in range(count):
        remainder = remainder - coeffs[:, k : k + 1] * basis_ref[k]
        column_ref[k] = means[0, k]
    column_ref[count] = height[0, 0]
    next_ref[...] = remainder / height


def close(sums, image, basis, rows):
    return pl.pallas_call(
        functools.partial(close_kernel, rows),
        in_specs=[VMEM, HBM, VMEM],
        out_specs=[VMEM, SMEM],
        out_shape=[
            jax.ShapeDtypeStruct(image.shape, F32),
            jax.ShapeDtypeStruct((basis.shape[0] + 1,), F32),
        ],
        scratch_shapes=[pltpu.VMEM(image.shape, F32), pltpu.SemaphoreType.DMA],
        compiler_params=pltpu.CompilerParams(vmem_limit_bytes=2 * MIB),
    )(sums, image, basis)


def row_routes(rows, width):
    spot = lambda r, y: (r % rows) * width + y
    turns = {1: (1, -1, -1, -1), 2: (1, 1, -1, -1), 3: (1, 1, 1, -1)}
    return {
        k: [(spot(r, y), spot(r + turns[k][y], y)) for r in range(rows) for y in range(width)]
        for k in turns
    }


def shards(
    positions, normals, panel_areas, panel_counts, near_lists, near_counts, leaf_lists, leaf_kinds,
    group_lists, group_kinds, block_inverse, moment_maps, up_operators, far_operators, krylov_basis,
):
    clusters, _, panels = positions.shape
    coeffs = moment_maps.shape[1]
    devices = lax.axis_size(AXES)
    width = lax.axis_size(AXES[-1])
    own = jnp.full((1,), lax.axis_index(AXES), jnp.int32)
    payload, group, density, features, row_pairs, off_pairs = sources(
        own, near_lists, near_counts, panel_counts, krylov_basis, block_inverse, moment_maps, up_operators,
        positions.transpose(1, 0, 2), normals.transpose(1, 0, 2), panel_areas, devices,
    )
    row = [payload] + [
        lax.ppermute(payload, AXES[-1], [(y, (y + k) % width) for y in range(width)])
        for k in range(1, width)
    ]
    routes = row_routes(devices // width, width)
    window = row + [lax.ppermute(row[k], AXES, routes[k]) for k in range(1, width)]
    groups = lax.all_to_all(group, AXES, 0, 0, tiled=True)
    slots = near_lists.shape[1]
    near = row_fields(row_pairs, panel_counts, features, slots, row)
    image, sums = late_fields(
        own, off_pairs, panel_counts, slots, leaf_lists, leaf_kinds, group_lists, group_kinds,
        groups, density, near, krylov_basis, features, far_operators, up_operators, moment_maps, window, devices,
    )
    sums = lax.all_to_all(sums, AXES, 0, 0, tiled=True)
    return close(sums, image, krylov_basis, devices * clusters * panels)


def solution(mesh):
    finer = Mesh(mesh.devices.reshape(mesh.shape["role"], 4, 4, 4), AXES)
    split = lambda rank: P(AXES, *([None] * (rank - 1)))
    return jax.shard_map(
        shards,
        mesh=finer,
        in_specs=(
            split(3), split(3), split(2), split(1), split(2), split(1), split(2), split(2), split(2),
            split(2), split(3), split(3), P(), P(), P(None, AXES, None),
        ),
        out_specs=(split(2), P()),
        check_vma=False,
    )
```

```python
import functools

import jax
import jax.numpy as jnp
from jax import lax
from jax.experimental import pallas as pl
from jax.experimental.pallas import tpu as pltpu
from jax.sharding import Mesh
from jax.sharding import PartitionSpec as P

RADIUS = 3
AXES = ("role", "dev_0", "dev_1", "dev_2")
SOFTEN = 0.01
EPSILON = 1e-06
HIGH = lax.Precision.HIGHEST
F32 = jnp.float32
BF16 = jnp.bfloat16
VMEM = pl.BlockSpec(memory_space=pltpu.VMEM)
SMEM = pl.BlockSpec(memory_space=pltpu.SMEM)
ANY = pl.BlockSpec(memory_space=pl.ANY)
HBM = pl.BlockSpec(memory_space=pltpu.HBM)
NT = (((1,), (1,)), ((), ()))
NN = (((1,), (0,)), ((), ()))
HIGHER = 128
ACROSS = 256
UNROLL = 16
MIB = 2**20
PAIRS = 4
DEAD = 1 << 24


def dot(a, b, dims):
    return lax.dot_general(a, b, dims, preferred_element_type=F32)


def halves(value):
    top = value.astype(BF16)
    return top, (value - top.astype(F32)).astype(BF16)


def thirds(value):
    top, rest = value.astype(BF16), None
    rest = value - top.astype(F32)
    middle = rest.astype(BF16)
    return top, middle, (rest - middle.astype(F32)).astype(BF16)


def power(value):
    assert value & (value - 1) == 0
    return value.bit_length() - 1


def window_block(own, ids, clusters, width):
    owner = lax.shift_right_logical(ids, power(clusters))
    shift = (own - owner) & (width - 1)
    same = lax.shift_right_logical(owner, power(width)) == lax.shift_right_logical(own, power(width))
    return jnp.where(same, shift, shift + width - 1), ids & (clusters - 1)


def list_pairs(own, lists_ref, nears_ref, row_ref, off_ref, width):
    clusters = lists_ref.shape[0]

    def list_cluster(c, lengths):
        row, off = lengths
        row_ref[row] = (c << 8) + c

        def list_slot(s, lengths):
            row, off = lengths
            block, inside = window_block(own, lists_ref[c, s], clusters, width)
            pair = (block << 16) + (inside << 8) + c
            near = jnp.where(block < width, 1, 0)
            row_ref[row] = pair
            off_ref[off] = pair - (width << 16)
            return row + near, off + 1 - near

        return lax.fori_loop(0, nears_ref[c], list_slot, (row + 1, off))

    row, off = lax.fori_loop(0, clusters, list_cluster, (jnp.int32(0), jnp.int32(0)))
    for ref, length in ((row_ref, row), (off_ref, off)):
        for k in range(PAIRS):
            ref[length + k] = DEAD
        ref[ref.shape[0] - 1] = length


def source_kernel(
    own_ref, lists_ref, nears_ref, counts_ref,
    basis_hbm, inverse_hbm, maps_hbm, up_hbm, position_hbm, normal_hbm, area_hbm,
    payload_ref, group_ref, density_ref, features_hbm, row_ref, off_ref,
    basis_ref, inverse_ref, maps_ref, up_ref, position_ref, normal_ref, area_ref,
    features_ref, sems, small_sems,
):
    clusters, panels = density_ref.shape
    coeffs = maps_ref.shape[1]
    copies = [
        [pltpu.make_async_copy(a.at[c], b.at[c], sems.at[k, c]) for c in range(clusters)]
        for k, (a, b) in enumerate(((inverse_hbm, inverse_ref), (maps_hbm, maps_ref), (up_hbm, up_ref)))
    ]
    small = [
        pltpu.make_async_copy(a, b, small_sems.at[k])
        for k, (a, b) in enumerate((
            (position_hbm, position_ref), (basis_hbm.at[basis_hbm.shape[0] - 1], basis_ref),
            (normal_hbm, normal_ref), (area_hbm, area_ref)))
    ]
    for copy in small[0:2] + copies[0] + small[2:]:
        copy.start()
    list_pairs(own_ref[0], lists_ref, nears_ref, row_ref, off_ref, 4)
    small[0].wait()
    norm = jnp.zeros((clusters, panels), F32)
    positions = []
    for a in range(3):
        top, rest = halves(position_ref[a])
        positions.append((top.astype(F32), rest.astype(F32)))
        norm += (positions[a][0] + positions[a][1]) * (positions[a][0] + positions[a][1])
    softened = [part.astype(F32) for part in thirds(norm + SOFTEN)]
    one = jnp.ones((1, panels), F32)
    none = jnp.zeros((8, panels), F32)
    for c in range(clusters):
        at = slice(c, c + 1)
        top = [-2.0 * positions[a][0][at] for a in range(3)]
        rest = [-2.0 * positions[a][1][at] for a in range(3)]
        turned = jnp.concatenate(
            top + [one, none[0:4]] + rest + [none[0:5]] + top + [one, none[0:4]] + rest + [none[0:5]]
            + [none[0:3], one, none[0:4]] + [part[at] for part in softened]
            + [none[0:5], jnp.zeros((80, panels), F32)], axis=0
        ).T
        features_ref[c * panels : (c + 1) * panels, :] = turned.astype(BF16)
    features_ref[clusters * panels :, :] = jnp.where(
        lax.broadcasted_iota(jnp.int32, (HIGHER, 128), 1) == 40, 1.0, 0.0
    ).astype(BF16)
    leaving = pltpu.make_async_copy(features_ref, features_hbm, small_sems.at[4])
    leaving.start()
    small[1].wait()
    lane = lax.broadcasted_iota(jnp.int32, (1, panels), 1)
    densities = []
    for c in range(clusters):
        if c % 4 == 0:
            for copy in copies[0][c : c + 4]:
                copy.wait()
            for copy in copies[1 + c // 4]:
                copy.start()
        current = basis_ref[c : c + 1].astype(BF16)
        density = dot(current, inverse_ref[c], NT)
        densities.append(jnp.where(lane < counts_ref[c], density, 0.0).astype(BF16))
    for copy in small[2:]:
        copy.wait()
    wide = jnp.concatenate([d.astype(F32) for d in densities], axis=0)
    density_ref[...] = wide
    scale = area_ref[...] * wide
    weights = [scale * normal_ref[a] for a in range(3)]
    whole = [top + rest for top, rest in positions]
    crossed = sum(whole[a] * weights[a] for a in range(3))
    for k, value in enumerate(whole + [norm] + weights + [crossed]):
        for c in range(clusters):
            payload_ref[c, k : k + 1, :] = value[c : c + 1]
    tails = []
    for c in range(clusters):
        if c % 4 == 0:
            for copy in copies[1][c : c + 4]:
                copy.wait()
        tails.append(dot(densities[c], maps_ref[c], NT).astype(BF16))
    for copy in copies[2]:
        copy.wait()
    total = jnp.zeros((1, coeffs), F32)
    for c in range(clusters):
        total += dot(tails[c], up_ref[c], NT)
        payload_ref[clusters, c : c + 1, 0:coeffs] = tails[c].astype(F32)
        payload_ref[clusters, c : c + 1, coeffs:panels] = jnp.full(
            (1, panels - coeffs), counts_ref[c].astype(F32)
        )
    lines = coeffs // 128
    row = lax.broadcasted_iota(jnp.int32, group_ref.shape, 0) & (lines - 1)
    spread = total[:, 0:128]
    for k in range(1, lines):
        spread = jnp.where(row == k, total[:, 128 * k : 128 * k + 128], spread)
    group_ref[...] = jnp.broadcast_to(spread, group_ref.shape)
    leaving.wait()


def sources(own, lists, nears, counts, basis, inverse, maps, up, positions, normals, areas, devices):
    count, clusters, panels = basis.shape
    coeffs = maps.shape[1]
    lines = devices * coeffs // 128
    pairs = clusters * (lists.shape[1] + 1) + PAIRS + 1
    return pl.pallas_call(
        source_kernel,
        in_specs=[SMEM] * 4 + [HBM] * 7,
        out_specs=[VMEM] * 3 + [HBM] + [SMEM] * 2,
        out_shape=[
            jax.ShapeDtypeStruct((clusters + 1, 8, panels), F32),
            jax.ShapeDtypeStruct((lines, 128), F32),
            jax.ShapeDtypeStruct((clusters, panels), F32),
            jax.ShapeDtypeStruct((clusters * panels + HIGHER, 128), BF16),
            jax.ShapeDtypeStruct((pairs,), jnp.int32),
            jax.ShapeDtypeStruct((pairs,), jnp.int32),
        ],
        scratch_shapes=[
            pltpu.VMEM((clusters, panels), F32),
            pltpu.VMEM(inverse.shape, BF16),
            pltpu.VMEM(maps.shape, BF16),
            pltpu.VMEM(up.shape, BF16),
            pltpu.VMEM(positions.shape, F32),
            pltpu.VMEM(normals.shape, F32),
            pltpu.VMEM(areas.shape, F32),
            pltpu.VMEM((clusters * panels + HIGHER, 128), BF16),
            pltpu.SemaphoreType.DMA((3, clusters)),
            pltpu.SemaphoreType.DMA((5,)),
        ],
        cost_estimate=pl.CostEstimate(flops=4 * 10**8, bytes_accessed=8 * MIB, transcendentals=0),
    )(own, lists, nears, counts, basis, inverse, maps, up, positions, normals, areas)


def near_tiles(
    pairs_ref, counts_ref, tails, window, position_ref,
    tile_list, features, total, squares, ready_list, ready,
):
    clusters = counts_ref.shape[0]
    panels = window.shape[2]
    highs, wides = panels // HIGHER, panels // ACROSS
    shift = lambda value, size: lax.shift_right_logical(value, power(size))
    ready_list()

    def list_some(g, length):
        for k in range(PAIRS):
            pair = pairs_ref[g * PAIRS + k]
            used = pair < DEAD
            pair = jnp.where(used, pair, 0)
            c, local, block = pair & 255, shift(pair, 256) & 255, shift(pair, 65536)
            live = tails[block, local, 0].astype(jnp.int32)
            down = jnp.where(used, shift(live + (ACROSS - 1), ACROSS), 0)
            across = shift(counts_ref[c] + (HIGHER - 1), HIGHER)
            base = ((block * (clusters + 1) + local) << (8 + power(wides))) + c * highs
            for j in reversed(range(highs)):
                for i in reversed(range(wides)):
                    tile_list[length + i * across + j] = base + ((i << 8) + j)
            length = length + down * across
        return length

    pairs = pairs_ref[pairs_ref.shape[0] - 1]
    length = lax.fori_loop(0, shift(pairs + (PAIRS - 1), PAIRS), list_some, jnp.int32(0))
    for extra in range(2 * UNROLL):
        tile_list[length + extra] = clusters * highs

    total[...] = jnp.zeros_like(total)

    def tile(s):
        lane = pl.multiple_of((s & (wides - 1)) * ACROSS, ACROSS)
        return window[lax.shift_right_logical(s, power(wides)), :, pl.ds(lane, ACROSS)]

    def square(at, u):
        spot = tile_list[at]
        top, middle, low = thirds(tile(lax.shift_right_logical(spot, 8)))
        right = jnp.concatenate(
            [top, top, middle, middle, low, jnp.ones((8, ACROSS), BF16), jnp.zeros((80, ACROSS), BF16)],
            axis=0,
        )
        left = features[pl.ds(pl.multiple_of((spot & 255) * HIGHER, HIGHER), HIGHER), :]
        squares[u] = dot(left, right, NN)

    def apply(at, u):
        inverse = lax.rsqrt(squares[u])
        field = (inverse * inverse * inverse).astype(BF16)
        top, rest = halves(tile(lax.shift_right_logical(tile_list[at], 8)))
        return dot(jnp.concatenate([top, rest], axis=0), field, NT)

    ready()
    for u in range(UNROLL):
        square(u, u)

    def step(g, carry):
        results = []
        for u in range(UNROLL):
            results.append((tile_list[g * UNROLL + u] & 255, apply(g * UNROLL + u, u)))
            square((g + 1) * UNROLL + u, u)
        for t, result in results:
            total[t] += result
        return carry

    lax.fori_loop(0, shift(length + (UNROLL - 1), UNROLL), step, 0)

    lines = []
    for c in range(clusters):
        parts = []
        for j in range(highs):
            r = total[c * highs + j]
            r = r[0:8] + r[8:16]
            x = position_ref[c, 0:3, j * HIGHER : (j + 1) * HIGHER]
            parts.append(jnp.sum(x * r[4:7], axis=0, keepdims=True) - r[7:8])
        lines.append(jnp.concatenate(parts, axis=1))
    return jnp.concatenate(lines, axis=0)


def near_scratch(clusters, slots, panels, blocks):
    highs, wides = panels // HIGHER, panels // ACROSS
    most = clusters * slots * highs * wides + 4 * UNROLL
    return [
        pltpu.SMEM((most,), jnp.int32),
        pltpu.VMEM((clusters * panels + HIGHER, 128), BF16),
        pltpu.SemaphoreType.DMA,
        pltpu.VMEM((clusters * highs + 1, 16, HIGHER), F32),
        pltpu.VMEM((UNROLL, HIGHER, ACROSS), F32),
        pltpu.VMEM((blocks * (clusters + 1), 8, panels), F32),
        pltpu.SMEM((blocks, clusters, 128), F32),
    ]


def row_kernel(pairs_ref, counts_ref, features_hbm, a_ref, b_ref, c_ref, d_ref, out_ref,
               tile_list, features, feature_sem, total, squares, window, tails, sems):
    clusters = counts_ref.shape[0]
    blocks = (a_ref, b_ref, c_ref, d_ref)
    coeffs = window.shape[2] // 2
    copies = []
    for k, block in enumerate(blocks):
        copies.append(pltpu.make_async_copy(
            block, window.at[pl.ds(k * (clusters + 1), clusters + 1)], sems.at[0, k]))
        copies.append(pltpu.make_async_copy(
            block.at[clusters, :, pl.ds(coeffs, 128)], tails.at[k], sems.at[1, k]))
    first, then = copies[1::2], copies[0::2]
    then.append(pltpu.make_async_copy(features_hbm, features, feature_sem))

    def wait(group):
        for copy in group:
            copy.wait()

    for copy in first + then:
        copy.start()
    out_ref[...] = near_tiles(
        pairs_ref, counts_ref, tails, window, window, tile_list, features, total, squares,
        lambda: wait(first), lambda: wait(then),
    )


def row_fields(pairs, counts, features, slots, blocks):
    clusters = counts.shape[0]
    panels = blocks[0].shape[2]
    return pl.pallas_call(
        row_kernel,
        in_specs=[SMEM] * 2 + [ANY] * (1 + len(blocks)),
        out_specs=VMEM,
        out_shape=jax.ShapeDtypeStruct((clusters, panels), F32),
        scratch_shapes=near_scratch(clusters, slots + 1, panels, len(blocks))
        + [pltpu.SemaphoreType.DMA((2, len(blocks)))],
        compiler_params=pltpu.CompilerParams(vmem_limit_bytes=56_450_000),
        cost_estimate=pl.CostEstimate(flops=3 * 10**9, bytes_accessed=MIB, transcendentals=10**6),
    )(pairs, counts, features, *blocks)


def late_kernel(
    own_ref, pairs_ref, counts_ref, leaf_ids_ref, leaf_kinds_ref, group_ids_ref,
    group_kinds_ref, groups_ref, density_ref, near_ref, basis_ref, features_hbm, far_hbm, up_hbm, maps_hbm,
    a_ref, b_ref, c_ref, d_ref, e_ref, f_ref, g_ref,
    image_ref, sums_ref,
    tile_list, features, feature_sem, total, squares, window, tails, sems,
    far_ref, up_ref, maps_ref, own_rows, moments, weight_sems,
):
    clusters, panels = density_ref.shape
    kinds, coeffs = far_ref.shape[1], far_ref.shape[2]
    row, others = (a_ref, b_ref, c_ref, d_ref), (e_ref, f_ref, g_ref)
    copies = []
    for k, block in enumerate(others):
        copies.append(pltpu.make_async_copy(
            block, window.at[pl.ds(k * (clusters + 1), clusters + 1)], sems.at[0, k]))
        copies.append(pltpu.make_async_copy(
            block.at[clusters, :, pl.ds(coeffs, 128)], tails.at[k], sems.at[1, k]))
    copies.append(pltpu.make_async_copy(a_ref, own_rows, weight_sems.at[3]))
    first, then = copies[1::2], copies[0:-1:2] + copies[-1:]
    then.append(pltpu.make_async_copy(features_hbm, features, feature_sem))

    def wait(group):
        for copy in group:
            copy.wait()

    for copy in first + then:
        copy.start()
    later = [
        pltpu.make_async_copy(block.at[clusters, :, pl.ds(0, coeffs)],
                              moments.at[pl.ds(k * clusters, clusters)], sems.at[2, k])
        for k, block in enumerate(row + others)
    ]
    weights = [
        pltpu.make_async_copy(far_hbm, far_ref, weight_sems.at[0]),
        pltpu.make_async_copy(up_hbm, up_ref, weight_sems.at[1]),
        pltpu.make_async_copy(maps_hbm, maps_ref, weight_sems.at[2]),
    ]
    weights[0].start()
    own = own_ref[0]

    def arrived():
        wait(then)
        for copy in later + weights[1:]:
            copy.start()

    near = near_ref[...] + near_tiles(
        pairs_ref, counts_ref, tails, window, own_rows, tile_list, features, total, squares,
        lambda: wait(first), arrived,
    )
    for copy in later:
        copy.wait()

    lines = coeffs // 128
    spots = groups_ref.shape[0]
    kind = lax.broadcasted_iota(jnp.int32, (kinds, 1), 0)
    spot = lax.broadcasted_iota(jnp.int32, (1, spots), 1)
    pick = jnp.zeros((kinds, spots), F32)
    for n in range(group_ids_ref.shape[1]):
        hit = (kind == group_kinds_ref[0, n]) & (
            lax.shift_right_logical(spot, power(lines)) == group_ids_ref[0, n])
        pick += jnp.where(hit, 1.0, 0.0)
    pick = jnp.concatenate(
        [jnp.where((spot & (lines - 1)) == k, pick, 0.0) for k in range(lines)], axis=0
    ).astype(BF16)
    group_sum = sum(dot(pick, part, NN) for part in thirds(groups_ref[...]))
    group_sum = jnp.concatenate(
        [group_sum[k * kinds : (k + 1) * kinds] for k in range(lines)], axis=1
    )
    local = jnp.zeros((24, coeffs), F32)
    weights[0].wait()
    group_rows = jnp.concatenate([part.astype(F32) for part in thirds(group_sum)], axis=0)
    row24 = lax.broadcasted_iota(jnp.int32, (24, 1), 0) & (kinds - 1)
    for o in range(kinds):
        local += dot(jnp.where(row24 == o, group_rows, 0.0).astype(BF16), far_ref[1, o], NT)
    local = jnp.sum(local, axis=0, keepdims=True).astype(BF16)

    block, inside = window_block(own, leaf_ids_ref[...], clusters, 4)
    spots_of = block * clusters + inside
    spot = lax.broadcasted_iota(jnp.int32, (1, moments.shape[0]), 1)
    picks = [jnp.zeros((clusters, moments.shape[0]), F32) for _ in range(kinds)]
    for n in range(leaf_ids_ref.shape[1]):
        hit = jnp.where(spots_of[:, n : n + 1] == spot, 1.0, 0.0)
        for o in range(kinds):
            picks[o] += jnp.where(leaf_kinds_ref[:, n : n + 1] == o, hit, 0.0)
    leaf_sum = dot(
        jnp.concatenate(picks, axis=0).astype(BF16), moments[...].astype(BF16), NN
    )
    leaf = jnp.zeros((2 * clusters, coeffs), F32)
    for o in range(kinds):
        top, rest = halves(leaf_sum[o * clusters : (o + 1) * clusters])
        leaf += dot(jnp.concatenate([top, rest], axis=0), far_ref[0, o], NT)
    leaf = leaf[0:clusters] + leaf[clusters:]
    weights[1].wait()
    leaf += jnp.concatenate([dot(local, up_ref[c], NN) for c in range(clusters)], axis=0)
    leaf = leaf.astype(BF16)
    weights[2].wait()
    images = []
    lane = lax.broadcasted_iota(jnp.int32, (1, panels), 1)
    for c in range(clusters):
        far = dot(leaf[c : c + 1], maps_ref[c], NN)
        value = 0.5 * density_ref[c : c + 1] + near[c : c + 1] + far
        images.append(jnp.where(lane < counts_ref[c], value, 0.0))
    image = jnp.concatenate(images, axis=0)
    image_ref[...] = image
    lane = lax.broadcasted_iota(jnp.int32, (1, 128), 1)
    sums = jnp.zeros((1, 128), F32)
    for k in range(basis_ref.shape[0] + 1):
        other = basis_ref[k] if k < basis_ref.shape[0] else image
        value = jnp.sum(jnp.sum(image * other, axis=0, keepdims=True), axis=1, keepdims=True)
        sums += jnp.where(lane == k, value, 0.0)
    sums_ref[...] = jnp.broadcast_to(sums, sums_ref.shape)


def late_fields(own, pairs, counts, slots, leaf_ids, leaf_kinds, group_ids, group_kinds, groups,
                density, near, basis, features, far, up, maps, window, devices):
    clusters, panels = density.shape
    return pl.pallas_call(
        late_kernel,
        in_specs=[SMEM] * 3 + [VMEM] * 2 + [SMEM] * 2 + [VMEM] * 4 + [ANY] + [HBM] * 3 + [ANY] * 7,
        out_specs=[VMEM, VMEM],
        out_shape=[
            jax.ShapeDtypeStruct(density.shape, F32),
            jax.ShapeDtypeStruct((devices, 128), F32),
        ],
        scratch_shapes=near_scratch(clusters, slots + 1, panels, 3)
        + [
            pltpu.SemaphoreType.DMA((3, 7)),
            pltpu.VMEM(far.shape, BF16),
            pltpu.VMEM(up.shape, BF16),
            pltpu.VMEM(maps.shape, BF16),
            pltpu.VMEM((clusters + 1, 8, panels), F32),
            pltpu.VMEM((7 * clusters, maps.shape[1]), F32),
            pltpu.SemaphoreType.DMA((4,)),
        ],
        compiler_params=pltpu.CompilerParams(vmem_limit_bytes=56 * 10**6),
        cost_estimate=pl.CostEstimate(flops=3 * 10**9, bytes_accessed=MIB, transcendentals=10**6),
    )(own, pairs, counts, leaf_ids, leaf_kinds, group_ids, group_kinds, groups, density,
      near, basis, features, far, up, maps, *window)


def close_kernel(rows, sums_ref, image_hbm, basis_ref, next_ref, column_ref, image_ref, sem):
    copy = pltpu.make_async_copy(image_hbm, image_ref, sem)
    copy.start()
    count = basis_ref.shape[0]
    means = jnp.sum(sums_ref[...], axis=0, keepdims=True) * (1.0 / rows)
    lane = lax.broadcasted_iota(jnp.int32, (1, 128), 1)
    coeffs = jnp.where(lane < count, means, 0.0)
    square = jnp.sum(jnp.where(lane == count, means, 0.0), axis=1, keepdims=True)
    energy = square - jnp.sum(coeffs * coeffs, axis=1, keepdims=True)
    height = jnp.sqrt(energy + EPSILON)
    copy.wait()
    remainder = image_ref[...]
    for k in range(count):
        remainder = remainder - coeffs[:, k : k + 1] * basis_ref[k]
        column_ref[k] = means[0, k]
    column_ref[count] = height[0, 0]
    next_ref[...] = remainder / height


def close(sums, image, basis, rows):
    return pl.pallas_call(
        functools.partial(close_kernel, rows),
        in_specs=[VMEM, HBM, VMEM],
        out_specs=[VMEM, SMEM],
        out_shape=[
            jax.ShapeDtypeStruct(image.shape, F32),
            jax.ShapeDtypeStruct((basis.shape[0] + 1,), F32),
        ],
        scratch_shapes=[pltpu.VMEM(image.shape, F32), pltpu.SemaphoreType.DMA],
        compiler_params=pltpu.CompilerParams(vmem_limit_bytes=2 * MIB),
    )(sums, image, basis)


def row_routes(rows, width):
    spot = lambda r, y: (r % rows) * width + y
    turns = {1: (1, -1, -1, -1), 2: (1, 1, -1, -1), 3: (1, 1, 1, -1)}
    return {
        k: [(spot(r, y), spot(r + turns[k][y], y)) for r in range(rows) for y in range(width)]
        for k in turns
    }


def shards(
    positions, normals, panel_areas, panel_counts, near_lists, near_counts, leaf_lists, leaf_kinds,
    group_lists, group_kinds, block_inverse, moment_maps, up_operators, far_operators, krylov_basis,
):
    clusters, _, panels = positions.shape
    coeffs = moment_maps.shape[1]
    devices = lax.axis_size(AXES)
    width = lax.axis_size(AXES[-1])
    own = jnp.full((1,), lax.axis_index(AXES), jnp.int32)
    payload, group, density, features, row_pairs, off_pairs = sources(
        own, near_lists, near_counts, panel_counts, krylov_basis, block_inverse, moment_maps, up_operators,
        positions.transpose(1, 0, 2), normals.transpose(1, 0, 2), panel_areas, devices,
    )
    row = [payload] + [
        lax.ppermute(payload, AXES[-1], [(y, (y + k) % width) for y in range(width)])
        for k in range(1, width)
    ]
    routes = row_routes(devices // width, width)
    window = row + [lax.ppermute(row[k], AXES, routes[k]) for k in range(1, width)]
    groups = lax.all_to_all(group, AXES, 0, 0, tiled=True)
    slots = near_lists.shape[1]
    near = row_fields(row_pairs, panel_counts, features, slots, row)
    image, sums = late_fields(
        own, off_pairs, panel_counts, slots, leaf_lists, leaf_kinds, group_lists, group_kinds,
        groups, density, near, krylov_basis, features, far_operators, up_operators, moment_maps, window, devices,
    )
    sums = lax.all_to_all(sums, AXES, 0, 0, tiled=True)
    return close(sums, image, krylov_basis, devices * clusters * panels)


def solution(mesh):
    finer = Mesh(mesh.devices.reshape(mesh.shape["role"], 4, 4, 4), AXES)
    split = lambda rank: P(AXES, *([None] * (rank - 1)))
    return jax.shard_map(
        shards,
        mesh=finer,
        in_specs=(
            split(3), split(3), split(2), split(1), split(2), split(1), split(2), split(2), split(2),
            split(2), split(3), split(3), P(), P(), P(None, AXES, None),
        ),
        out_specs=(split(2), P()),
        check_vma=False,
    )
```
